32 devices in a mesh: head: 4 (over y, x), seq: 8 (over z, core).
Axes of the slice: x: 2, y: 2, z: 4, core: 2. Of those that a mesh axis runs over, the one named last changes fastest.
Arguments:
- hidden_in: bfloat16 [8192, 2048], P(('head', 'seq')), may hold values from -6 to 6
- cotangent: bfloat16 [8192, 2048], P(('head', 'seq')), may hold values from -6 to 6
- lengths: int32 [2], replicated, may hold values from 1024 to 4096, as said below
- token_order: int32 [8192], replicated, may hold values from 0 to 8191, as said below
- own_map: int32 [4, 192], P('head'), may hold values from 0 to 191, each once within a row
- w_query: bfloat16 [2048, 2048], P('seq', 'head'), may hold values from -0.125 to 0.125
- w_key: bfloat16 [2048, 2048], P('seq', 'head'), may hold values from -0.125 to 0.125
- w_value: bfloat16 [2048, 2048], P('seq', 'head'), may hold values from -0.125 to 0.125
- w_out: bfloat16 [2048, 2048], P('head', 'seq'), may hold values from -3 to 3
- w_up: bfloat16 [2048, 8192], P('seq', 'head'), may hold values from -0.125 to 0.125
- w_down: bfloat16 [8192, 2048], P('head', 'seq'), may hold values from -0.0625 to 0.0625
- gains: float32 [2, 2048], replicated, may hold values from 0.25 to 1.75
- biases: float32 [6, 2048], replicated, may hold values from -4 to 4
- up_bias: float32 [8192], P('head'), may hold values from -4 to 4
- vector_moment: float32 [8, 2048], replicated, may hold values from -48 to 48
- vector_second: float32 [8, 2048], replicated, may hold values from 1 to 20
- bias_moment: float32 [8192], P('head'), may hold values from -24 to 24
- bias_second: float32 [8192], P('head'), may hold values from 0.3 to 6
- step_count: int32 [1], replicated, may hold values from 1 to 20
- stat_left: float32 [768, 256, 256], P(('head', 'seq')), as said below
- stat_right: float32 [768, 256, 256], P(('head', 'seq')), as said below
- root_left: float32 [768, 256, 256], P(('head', 'seq')), as said below
- root_right: float32 [768, 256, 256], P(('head', 'seq')), as said below
- master: float32 [768, 256, 256], P(('head', 'seq')), may hold values from -0.125 to 0.125
Outputs:
- layer_out: bfloat16 [8192, 2048], P(('head', 'seq'))
- input_grad: float32 [8192, 2048], P(('head', 'seq'))
- block_grads: float32 [768, 256, 256], P(('head', 'seq'))
- stat_left_new: float32 [768, 256, 256], P(('head', 'seq'))
- stat_right_new: float32 [768, 256, 256], P(('head', 'seq'))
- master_new: float32 [768, 256, 256], P(('head', 'seq'))
- biases_new: float32 [6, 2048], replicated
- gains_new: float32 [2, 2048], replicated
- up_bias_new: float32 [8192], P('head')
- vector_grad: float32 [8, 2048], replicated
- vector_moment_new: float32 [8, 2048], replicated
- vector_second_new: float32 [8, 2048], replicated
- up_bias_grad: float32 [8192], P('head')
- bias_moment_new: float32 [8192], P('head')
- bias_second_new: float32 [8192], P('head')
The draws below stay inside these ranges and needn't reach their ends.
Inputs may be any that keep to these rules, and one draw needn't show every extreme that they name: `lengths`: sequences are packed one after another from stream position 0; positions past the last are padding. One sequence has 4096 tokens and another 1024. `token_order`: A permutation of the stream positions that keeps aligned runs of 256 positions whole and in order. `own_map`: each row is a permutation of the 192 canonical blocks of its head group. `stat_left`: each block is symmetric. `stat_right`: each block is symmetric. `root_left`: each block is symmetric. `root_right`: each block is symmetric.
All inputs are finite; a program needn't handle non-finite values.
Results may differ from the reference program's by a relative error of at most 0.02.
Values may be sent and summed in bfloat16 or wider, within the bound.
A program may use at most 320 MiB of HBM per device.

```python
import math
import jax
import jax.numpy as jnp
from jax import lax

D = 2048
HEADS = 16
FF = 8192
HDIM = 128
TOK_DEV = 256
MAXLEN = 4096
MINLEN = 1024
QROWS = 512
BLOCK = 256
TOKENS = 8192
NSEQ = 2
NBH = 192
NBLK = 768
N_HEAD = 4


def draw_lengths(key, part):
    inner = jax.random.fold_in(key, 15)
    key_base, key_long, key_offset = jax.random.split(inner, 3)
    drawn = jax.random.randint(key_base, (NSEQ,), MINLEN, MAXLEN + 1, dtype=jnp.int32)
    longest = jax.random.randint(key_long, (), 0, NSEQ, dtype=jnp.int32)
    offset = jax.random.randint(key_offset, (), 1, NSEQ, dtype=jnp.int32)
    shortest = (longest + offset) % NSEQ
    slot_ids = jnp.arange(NSEQ, dtype=jnp.int32)
    drawn = jnp.where(slot_ids == longest, MAXLEN, drawn)
    return jnp.where(slot_ids == shortest, MINLEN, drawn).astype(jnp.int32)


def draw_token_order(key, part):
    inner = jax.random.fold_in(key, 16)
    block_order = jax.random.permutation(inner, jnp.arange(TOKENS // TOK_DEV, dtype=jnp.int32))
    inside = jnp.arange(TOK_DEV, dtype=jnp.int32)
    return (block_order[:, None] * TOK_DEV + inside[None, :]).reshape(-1).astype(jnp.int32)


def symmetric_blocks(key, scale_value, spread):
    key_diag, key_off = jax.random.split(key)
    diagonal = jax.random.uniform(key_diag, (NBLK, BLOCK), jnp.float32, 0.5, 2.0)
    noise = jax.random.normal(key_off, (NBLK, BLOCK, BLOCK), jnp.float32)
    mixed = (noise + jnp.swapaxes(noise, 1, 2)) * (spread / math.sqrt(2.0 * BLOCK))
    identity = jnp.eye(BLOCK, dtype=jnp.float32)
    return scale_value * (identity[None, :, :] * diagonal[:, :, None] + mixed)


def stat_scale():
    return 0.05 * BLOCK * TOKENS


def draw_stat_left(key, part):
    return symmetric_blocks(jax.random.fold_in(key, 11), stat_scale(), 1.0)


def draw_stat_right(key, part):
    return symmetric_blocks(jax.random.fold_in(key, 12), stat_scale(), 1.0)


def draw_root_left(key, part):
    return symmetric_blocks(jax.random.fold_in(key, 13), stat_scale() ** (-0.25), 0.7)


def draw_root_right(key, part):
    return symmetric_blocks(jax.random.fold_in(key, 14), stat_scale() ** (-0.25), 0.7)


def block_levels(own_key, shape, shards, smallest, top_value):
    loudness = 1.0
    for dim, blocks in shards:
        steps = jax.random.uniform(jax.random.fold_in(jax.random.fold_in(own_key, 6), dim), (blocks,), jnp.float32, smallest / len(shards), top_value / len(shards))
        loudness = loudness * jnp.repeat(jnp.exp(steps), shape[dim] // blocks).reshape((-1,) + (1,) * (len(shape) - 1 - dim))
    return loudness


def gaussian(rng, shape, scale, most, shards=(), kind=jnp.bfloat16):
    result = scale * jax.random.normal(rng, shape, jnp.float32)
    if shards:
        result = result * block_levels(rng, shape, shards, -0.22, 0.18)
    return jnp.clip(result, -most, most).astype(kind)


def setup_inputs(seed: int = 0) -> dict:
    seeds = jax.random.split(jax.random.key(seed), 25)
    hidden_in = gaussian(seeds[0], (TOKENS, D), 1.0, 6.0, ((0, 32),))
    cotangent = gaussian(seeds[1], (TOKENS, D), 1.0, 6.0, ((0, 32),))
    lengths = draw_lengths(jax.random.fold_in(seeds[24], 71), 0)
    token_order = draw_token_order(jax.random.fold_in(seeds[24], 71), 0)
    own_map = jax.vmap(lambda own: jax.random.permutation(own, NBH))(jax.random.split(seeds[4], N_HEAD)).reshape((N_HEAD, NBH)).astype(jnp.int32)
    w_query = gaussian(seeds[5], (D, D), D ** -0.5, 0.125, ((0, 8), (1, 4)))
    w_key = gaussian(seeds[6], (D, D), D ** -0.5, 0.125, ((0, 8), (1, 4)))
    w_value = gaussian(seeds[7], (D, D), D ** -0.5, 0.125, ((0, 8), (1, 4)))
    w_out = gaussian(seeds[8], (D, D), 4 ** -0.5, 3.0, ((0, 4), (1, 8)))
    w_up = gaussian(seeds[9], (D, FF), D ** -0.5, 0.125, ((0, 8), (1, 4)))
    w_down = gaussian(seeds[10], (FF, D), FF ** -0.5, 0.0625, ((0, 4), (1, 8)))
    gains = jnp.clip(1.0 + 0.15 * jax.random.normal(seeds[11], (2, D), jnp.float32), 0.25, 1.75)
    biases = gaussian(seeds[12], (6, D), 0.3, 4.0, (), jnp.float32)
    up_bias = gaussian(seeds[13], (FF,), 0.3, 4.0, ((0, 4),), jnp.float32)
    vector_moment = gaussian(seeds[14], (8, D), 8.0, 48.0, (), jnp.float32)
    vector_second = jnp.clip(jnp.exp(jax.random.uniform(seeds[15], (8, D), jnp.float32, math.log(1.0), math.log(20.0))), 1.0, 20.0)
    bias_moment = gaussian(seeds[16], (FF,), 4.0, 24.0, ((0, 4),), jnp.float32)
    bias_second = jnp.clip(jnp.exp(math.log(6.0) - 2.9957322 * jax.random.uniform(seeds[17], (FF,), jnp.float32) ** block_levels(seeds[17], (FF,), ((0, 4),), -0.2, 0.2)), 0.3, 6.0)
    step_count = jax.random.randint(seeds[18], (1,), 1, 21).astype(jnp.int32)
    stat_left = draw_stat_left(jax.random.fold_in(seeds[24], 71), 0)
    stat_right = draw_stat_right(jax.random.fold_in(seeds[24], 71), 0)
    root_left = draw_root_left(jax.random.fold_in(seeds[24], 71), 0)
    root_right = draw_root_right(jax.random.fold_in(seeds[24], 71), 0)
    master = gaussian(seeds[23], (NBLK, BLOCK, BLOCK), D ** -0.5, 0.125, ((0, 32),), jnp.float32)
    return {"hidden_in": hidden_in, "cotangent": cotangent, "lengths": lengths, "token_order": token_order, "own_map": own_map, "w_query": w_query, "w_key": w_key, "w_value": w_value, "w_out": w_out, "w_up": w_up, "w_down": w_down, "gains": gains, "biases": biases, "up_bias": up_bias, "vector_moment": vector_moment, "vector_second": vector_second, "bias_moment": bias_moment, "bias_second": bias_second, "step_count": step_count, "stat_left": stat_left, "stat_right": stat_right, "root_left": root_left, "root_right": root_right, "master": master}


NEG_LARGE = -1e+30
NORM_EPS = 1e-12
ADAM_RATE = 0.4
SHAMPOO_RATE = 0.15

@jax.custom_vjp
def low(v):
    return lax.optimization_barrier(v.astype(jnp.bfloat16)).astype(jnp.float32)

@jax.custom_vjp
def low_back(v):
    return v

def low_keep(v):
    return (low(v), None)

def low_pass(kept, grad):
    return (grad,)

def back_keep(v):
    return (v, None)

def back_low(kept, grad):
    return (low(grad),)
low.defvjp(low_keep, low_pass)
low_back.defvjp(back_keep, back_low)

def matmul(left, right):
    return jnp.dot(left, right, precision=lax.Precision.HIGHEST)

def segment_table(token_order, lengths):
    seq_count = lengths.shape[0]
    seq_ends = jnp.cumsum(lengths).astype(jnp.int32)
    before = lax.optimization_barrier(jnp.sum((token_order[:, None] >= seq_ends[None, :]).astype(jnp.int32), axis=1)).astype(jnp.int32)
    is_valid = token_order < seq_ends[seq_count - 1]
    row_ids = jnp.arange(token_order.shape[0], dtype=jnp.int32)
    return (jnp.where(is_valid, before, seq_count + row_ids).astype(jnp.int32), is_valid)

def layer_norm(z_rows, gain, shift):
    average = lax.optimization_barrier(jnp.mean(z_rows, axis=-1, keepdims=True))
    centered = z_rows - average
    variance = lax.optimization_barrier(jnp.mean(centered * centered, axis=-1, keepdims=True))
    return centered * lax.rsqrt(variance + NORM_EPS) * gain + shift

def attention(queries, keys_all, values_all, seg_ids):
    query_heads = queries.reshape(TOKENS, HEADS, HDIM).transpose(1, 0, 2)
    key_heads = keys_all.reshape(TOKENS, HEADS, HDIM).transpose(1, 0, 2)
    value_heads = values_all.reshape(TOKENS, HEADS, HDIM).transpose(1, 0, 2)
    block_count = TOKENS // QROWS
    score_scale = 1.0 / HDIM ** 0.5

    def one_block(position):
        head_id = position // block_count
        row_start = position % block_count * QROWS
        query_rows = lax.dynamic_slice_in_dim(lax.dynamic_index_in_dim(query_heads, head_id, 0, keepdims=False), row_start, QROWS, 0)
        key_rows = lax.dynamic_index_in_dim(key_heads, head_id, 0, keepdims=False)
        value_rows = lax.dynamic_index_in_dim(value_heads, head_id, 0, keepdims=False)
        seg_rows = lax.dynamic_slice_in_dim(seg_ids, row_start, QROWS, 0)
        scores = low_back(matmul(query_rows, key_rows.T) * score_scale)
        allowed = seg_rows[:, None] == seg_ids[None, :]
        top = lax.optimization_barrier(jnp.max(jnp.where(allowed, scores, NEG_LARGE), axis=1))
        prob = jnp.where(allowed, jnp.exp(scores - top[:, None]), 0.0)
        total = lax.optimization_barrier(jnp.sum(prob, axis=1))
        return matmul(low(prob), value_rows) / total[:, None]
    stacked = lax.map(jax.checkpoint(one_block), jnp.arange(HEADS * block_count, dtype=jnp.int32))
    return stacked.reshape(HEADS, TOKENS, HDIM).transpose(1, 0, 2).reshape(TOKENS, D)

def column_panels(matrix):
    height, breadth = matrix.shape
    return matrix.reshape(height, N_HEAD, breadth // N_HEAD).transpose(1, 0, 2)

def row_panels(matrix):
    height, breadth = matrix.shape
    return matrix.reshape(N_HEAD, height // N_HEAD, breadth)

def to_blocks(panels):
    panel_count, height, breadth = panels.shape
    shaped = panels.reshape(panel_count, height // BLOCK, BLOCK, breadth // BLOCK, BLOCK)
    return shaped.transpose(0, 1, 3, 2, 4).reshape(panel_count, -1, BLOCK, BLOCK)

def adam_step(param, grad, moment, second, step_float):
    moment_new = 0.9 * moment + 0.1 * grad
    second_new = 0.999 * second + 0.001 * grad * grad
    fix_one = 1.0 - jnp.power(jnp.float32(0.9), step_float)
    fix_two = 1.0 - jnp.power(jnp.float32(0.999), step_float)
    update = ADAM_RATE * (moment_new / fix_one) / (jnp.sqrt(second_new / fix_two) + 1e-08)
    return (param - update, moment_new, second_new)

def reference(hidden_in, cotangent, lengths, token_order, own_map, w_query, w_key, w_value, w_out, w_up, w_down, gains, biases, up_bias, vector_moment, vector_second, bias_moment, bias_second, step_count, stat_left, stat_right, root_left, root_right, master):
    seg_ids, is_valid = segment_table(token_order, lengths)

    def forward(inputs, wq_f, wk_f, wv_f, wo_f, wu_f, wd_f, gain_rows, bias_rows, hidden_bias):
        queries = low(low_back(matmul(inputs, wq_f) + bias_rows[0]))
        keys_all = low(low_back(matmul(inputs, wk_f)))
        values_all = low(low_back(matmul(inputs, wv_f) + bias_rows[1]))
        attended = attention(queries, keys_all, values_all, seg_ids)
        attended_low = low(low_back(attended))
        z_one = inputs + low_back(matmul(attended_low, wo_f)) + bias_rows[2]
        h_one = layer_norm(z_one, gain_rows[0], bias_rows[3])
        pre_act = low_back(matmul(low(h_one), wu_f) + hidden_bias)
        act = low(jax.nn.gelu(pre_act, approximate=True))
        z_two = h_one + low_back(matmul(act, wd_f)) + bias_rows[4]
        return layer_norm(z_two, gain_rows[1], bias_rows[5])
    out_f32, pull_back = jax.vjp(forward, hidden_in.astype(jnp.float32), w_query.astype(jnp.float32), w_key.astype(jnp.float32), w_value.astype(jnp.float32), w_out.astype(jnp.float32), w_up.astype(jnp.float32), w_down.astype(jnp.float32), gains, biases, up_bias)
    grad_y = cotangent.astype(jnp.float32) * is_valid[:, None].astype(jnp.float32)
    input_grad, grad_query, grad_key, grad_value, grad_out, grad_up, grad_down, grad_gains, grad_biases, up_bias_grad = pull_back(grad_y)
    canon = jnp.concatenate([to_blocks(column_panels(grad_query)), to_blocks(column_panels(grad_key)), to_blocks(column_panels(grad_value)), to_blocks(row_panels(grad_out)), to_blocks(column_panels(grad_up)), to_blocks(row_panels(grad_down))], axis=1)
    block_grads = jnp.take_along_axis(canon, own_map[:, :, None, None], axis=1).reshape(NBLK, BLOCK, BLOCK)
    stat_left_new = 0.5 * stat_left + 0.5 * jnp.einsum('bij,bkj->bik', block_grads, block_grads, precision=lax.Precision.HIGHEST)
    stat_right_new = 0.5 * stat_right + 0.5 * jnp.einsum('bji,bjk->bik', block_grads, block_grads, precision=lax.Precision.HIGHEST)
    left_mix = jnp.einsum('bij,bjk->bik', root_left, block_grads, precision=lax.Precision.HIGHEST)
    direction = jnp.einsum('bij,bjk->bik', left_mix, root_right, precision=lax.Precision.HIGHEST)
    master_new = master - SHAMPOO_RATE * direction
    step_float = step_count[0].astype(jnp.float32)
    vector_grad = jnp.concatenate([grad_biases, grad_gains], axis=0)
    vector_params = jnp.concatenate([biases, gains], axis=0)
    vector_new, vector_moment_new, vector_second_new = adam_step(vector_params, vector_grad, vector_moment, vector_second, step_float)
    up_bias_new, bias_moment_new, bias_second_new = adam_step(up_bias, up_bias_grad, bias_moment, bias_second, step_float)
    return (out_f32.astype(jnp.bfloat16), input_grad, block_grads, stat_left_new, stat_right_new, master_new, vector_new[0:6], vector_new[6:8], up_bias_new, vector_grad, vector_moment_new, vector_second_new, up_bias_grad, bias_moment_new, bias_second_new)
```

```python
import functools
import math

import jax
import jax.numpy as jnp
from jax import lax
from jax.experimental import pallas as pl
from jax.experimental.pallas import tpu as pltpu
from jax.sharding import PartitionSpec as P

HDIM = 128
BLOCK = 256
RUN = 256

NEG_LARGE = -1e30
NORM_EPS = 1e-12
ADAM_RATE = 0.4
SHAMPOO_RATE = 0.15
MESH = pl.DeviceIdType.MESH
VMEM_MOST = 60 * 1024 * 1024

ANY = pl.BlockSpec(memory_space=pl.ANY)
IN_SMEM = pl.BlockSpec(memory_space=pltpu.SMEM)
IN_VMEM = pl.BlockSpec(memory_space=pltpu.VMEM)


def seq_barrier(me, heads, parts):
    own_head, own_part = me // parts, me % parts
    barrier = pltpu.get_barrier_semaphore()
    for step in range(1, heads):
        pl.semaphore_signal(
            barrier,
            inc=1,
            device_id={"seq": (own_head + step) % heads * parts + own_part},
            device_id_type=MESH,
        )
    for step in range(1, parts):
        pl.semaphore_signal(
            barrier,
            inc=1,
            device_id={"seq": own_head * parts + (own_part + step) % parts},
            device_id_type=MESH,
        )
    pl.semaphore_wait(barrier, heads - 1 + parts - 1)


def spread_kernel(
    fields, heads, parts, x_ref, y_ref, own_sem, send_sem, recv_sem, pass_sem, take_sem
):
    me = lax.axis_index("seq")
    own_head, own_part = me // parts, me % parts
    seq_barrier(me, heads, parts)

    def columns(field, head):
        return pl.ds(pl.multiple_of((field * heads + head) * HDIM, HDIM), HDIM)

    sends = []
    for step in range(1, heads):
        head = (own_head + step) % heads
        for field in range(fields):
            copy = pltpu.make_async_remote_copy(
                src_ref=x_ref.at[:, columns(field, head)],
                dst_ref=y_ref.at[field, me],
                send_sem=send_sem.at[step - 1, field],
                recv_sem=recv_sem.at[step - 1, field],
                device_id={"seq": head * parts + own_part},
                device_id_type=MESH,
            )
            copy.start()
            sends.append(copy)
    owns = []
    for field in range(fields):
        copy = pltpu.make_async_copy(
            x_ref.at[:, columns(field, own_head)], y_ref.at[field, me], own_sem.at[field]
        )
        copy.start()
        owns.append(copy)
    passes = []

    def pass_on(step, field, source):
        origin = (own_head - step + heads) % heads * parts + own_part
        for other in range(1, parts):
            copy = pltpu.make_async_remote_copy(
                src_ref=source,
                dst_ref=y_ref.at[field, origin],
                send_sem=pass_sem.at[other - 1, step, field],
                recv_sem=take_sem.at[other - 1, step, field],
                device_id={"seq": own_head * parts + (own_part + other) % parts},
                device_id_type=MESH,
            )
            copy.start()
            passes.append(copy)

    for field in range(fields):
        pass_on(0, field, x_ref.at[:, columns(field, own_head)])
    for step in range(1, heads):
        origin = (own_head - step + heads) % heads * parts + own_part
        for field in range(fields):
            sends[(step - 1) * fields + field].wait_recv()
            pass_on(step, field, y_ref.at[field, origin])
    for copy in owns:
        copy.wait()
    for copy in sends:
        copy.wait_send()
    for copy in passes:
        copy.wait()


def spread(x_rows, fields, heads, parts, seq_size, collective_id):
    rows = x_rows.shape[0]
    return pl.pallas_call(
        functools.partial(spread_kernel, fields, heads, parts),
        out_shape=jax.ShapeDtypeStruct((fields, seq_size, rows, HDIM), x_rows.dtype),
        in_specs=[IN_VMEM],
        out_specs=ANY,
        scratch_shapes=[
            pltpu.SemaphoreType.DMA((fields,)),
            pltpu.SemaphoreType.DMA((max(heads - 1, 1), fields)),
            pltpu.SemaphoreType.DMA((max(heads - 1, 1), fields)),
            pltpu.SemaphoreType.DMA((max(parts - 1, 1), heads, fields)),
            pltpu.SemaphoreType.DMA((max(parts - 1, 1), heads, fields)),
        ],
        compiler_params=pltpu.CompilerParams(
            collective_id=collective_id, has_side_effects=True, vmem_limit_bytes=24 * 1024 * 1024
        ),
        name="spread",
    )(x_rows)


def collect_kernel(
    fields,
    heads,
    parts,
    x_ref,
    y_ref,
    own,
    got,
    ready,
    own_sem,
    pass_sem,
    take_sem,
    send_sem,
    recv_sem,
    keep_sem,
):
    me = lax.axis_index("seq")
    own_head, own_part = me // parts, me % parts
    seq_barrier(me, heads, parts)
    order = list(range(1, heads)) + [0]

    def home(step, part):
        return (own_head + step) % heads * parts + part

    passes, owns = {}, {}
    for step in order:
        for field in range(fields):
            for other in range(1, parts):
                part = (own_part + other) % parts
                copy = pltpu.make_async_remote_copy(
                    src_ref=x_ref.at[field, home(step, part)],
                    dst_ref=got.at[other - 1, step, field],
                    send_sem=pass_sem.at[other - 1, step, field],
                    recv_sem=take_sem.at[other - 1, step, field],
                    device_id={"seq": own_head * parts + part},
                    device_id_type=MESH,
                )
                copy.start()
                passes[step, field, other] = copy
            copy = pltpu.make_async_copy(
                x_ref.at[field, home(step, own_part)], own.at[step, field], own_sem.at[step, field]
            )
            copy.start()
            owns[step, field] = copy

    sends = []
    for step in order:
        for field in range(fields):
            owns[step, field].wait()
            for other in range(1, parts):
                passes[step, field, other].wait_recv()
            total = own[step, field].astype(jnp.float32)
            for other in range(1, parts):
                total = total + got[other - 1, step, field].astype(jnp.float32)
            ready[step, field] = total.astype(ready.dtype)
            columns = pl.ds(pl.multiple_of((field * heads + own_head) * HDIM, HDIM), HDIM)
            if step == 0:
                copy = pltpu.make_async_copy(
                    ready.at[step, field], y_ref.at[:, columns], keep_sem.at[field]
                )
            else:
                copy = pltpu.make_async_remote_copy(
                    src_ref=ready.at[step, field],
                    dst_ref=y_ref.at[:, columns],
                    send_sem=send_sem.at[step - 1, field],
                    recv_sem=recv_sem.at[step - 1, field],
                    device_id={"seq": home(step, own_part)},
                    device_id_type=MESH,
                )
            copy.start()
            sends.append(copy)
    for copy in sends:
        copy.wait()
    for copy in passes.values():
        copy.wait_send()


def collect(x_parts, heads, parts, collective_id):
    fields, seq_size, rows, _ = x_parts.shape
    kind = x_parts.dtype
    few = max(parts - 1, 1)
    return pl.pallas_call(
        functools.partial(collect_kernel, fields, heads, parts),
        out_shape=jax.ShapeDtypeStruct((rows, fields * heads * HDIM), kind),
        in_specs=[ANY],
        out_specs=ANY,
        scratch_shapes=[
            pltpu.VMEM((heads, fields, rows, HDIM), kind),
            pltpu.VMEM((few, heads, fields, rows, HDIM), kind),
            pltpu.VMEM((heads, fields, rows, HDIM), kind),
            pltpu.SemaphoreType.DMA((heads, fields)),
            pltpu.SemaphoreType.DMA((few, heads, fields)),
            pltpu.SemaphoreType.DMA((few, heads, fields)),
            pltpu.SemaphoreType.DMA((max(heads - 1, 1), fields)),
            pltpu.SemaphoreType.DMA((max(heads - 1, 1), fields)),
            pltpu.SemaphoreType.DMA((fields,)),
        ],
        compiler_params=pltpu.CompilerParams(
            collective_id=collective_id, has_side_effects=True, vmem_limit_bytes=VMEM_MOST
        ),
        name="collect",
    )(x_parts)


def allowed_tile(ends_ref, seq_count, key_low, query_low, shape):
    key_pos = key_low + lax.broadcasted_iota(jnp.int32, shape, 0)
    query_pos = query_low + lax.broadcasted_iota(jnp.int32, shape, 1)
    key_seg = jnp.zeros(shape, jnp.int32)
    query_seg = jnp.zeros(shape, jnp.int32)
    for index in range(seq_count):
        key_seg += (key_pos >= ends_ref[index]).astype(jnp.int32)
        query_seg += (query_pos >= ends_ref[index]).astype(jnp.int32)
    last = ends_ref[seq_count - 1]
    key_seg = jnp.where(key_pos < last, key_seg, seq_count + key_pos)
    query_seg = jnp.where(query_pos < last, query_seg, seq_count + query_pos)
    return key_seg == query_seg


def nt(left, right):
    return lax.dot_general(
        left, right, (((1,), (1,)), ((), ())), preferred_element_type=jnp.float32
    )


def nn(left, right):
    return lax.dot_general(
        left, right, (((1,), (0,)), ((), ())), preferred_element_type=jnp.float32
    )


def forward_kernel(
    setup,
    where_ref,
    low_ref,
    high_ref,
    ends_ref,
    part_ref,
    qkv_ref,
    out_ref,
    exact_ref,
    log_ref,
    q_buf,
    k_buf,
    v_buf,
    vt_buf,
    sem,
):
    parts, tile, seq_count, aligned, runs = setup
    turn = pl.program_id(0)
    part = part_ref[0]
    scale2 = math.log2(math.e) / math.sqrt(HDIM)

    @pl.when(turn == 0)
    def _():
        def fetch(field, run, buf, slot):
            return pltpu.make_async_copy(
                qkv_ref.at[field, where_ref[run]],
                buf.at[pl.ds(pl.multiple_of(slot * RUN, RUN), RUN), :],
                sem.at[field],
            )

        def start(run, carry):
            fetch(1, run, k_buf, run).start()
            fetch(2, run, v_buf, run).start()
            return carry

        def start_own(index, carry):
            fetch(0, index * parts + part, q_buf, index).start()
            return carry

        def finish(run, carry):
            fetch(1, run, k_buf, run).wait()
            fetch(2, run, v_buf, run).wait()
            return carry

        def finish_own(index, carry):
            fetch(0, index * parts + part, q_buf, index).wait()
            return carry

        lax.fori_loop(0, runs, start, 0)
        lax.fori_loop(0, runs // parts, start_own, 0)
        out_ref[...] = jnp.zeros_like(out_ref)
        lax.fori_loop(0, runs, finish, 0)
        lax.fori_loop(0, runs // parts, finish_own, 0)
        if aligned:

            def turn_tile(index, carry):
                low = pl.multiple_of(index * RUN, RUN)
                vt_buf[:, pl.ds(low, RUN)] = v_buf[pl.ds(low, RUN), :].T
                return carry

            lax.fori_loop(0, runs, turn_tile, 0)

    run = turn * parts + part
    place = where_ref[run]
    queries = q_buf[pl.ds(pl.multiple_of(turn * RUN, RUN), RUN), :]

    def attend():
        def key_step(index, carry):
            top, total, acc = carry
            low = pl.multiple_of(index * tile, tile)
            scores = nt(k_buf[pl.ds(low, tile), :], queries)
            if not aligned:
                allowed = allowed_tile(ends_ref, seq_count, low, run * RUN, scores.shape)
                scores = jnp.where(allowed, scores, NEG_LARGE)
            new_top = jnp.maximum(top, jnp.max(scores, axis=0, keepdims=True))
            prob = jnp.exp2((scores - new_top) * scale2)
            if not aligned:
                prob = jnp.where(allowed, prob, 0.0)
            fade = jnp.exp2((top - new_top) * scale2)
            total = total * fade + jnp.sum(prob, axis=0, keepdims=True)
            if aligned:
                turned = vt_buf[:, pl.ds(low, tile)]
            else:
                turned = v_buf[pl.ds(low, tile), :].T
            acc = acc * fade + nn(turned, prob.astype(jnp.bfloat16))
            return new_top, total, acc

        top, total, acc = lax.fori_loop(
            low_ref[run],
            high_ref[run],
            key_step,
            (
                jnp.full((1, RUN), NEG_LARGE, jnp.float32),
                jnp.zeros((1, RUN), jnp.float32),
                jnp.zeros((HDIM, RUN), jnp.float32),
            ),
        )
        result = (acc / total).T
        exact_ref[0] = result
        out_ref[place] = result.astype(out_ref.dtype)
        log_ref[0] = top * scale2 + jnp.log2(total)

    if aligned:
        is_valid = run * RUN < ends_ref[seq_count - 1]
        pl.when(is_valid)(attend)

        @pl.when(jnp.logical_not(is_valid))
        def _():
            values = v_buf[pl.ds(pl.multiple_of(run * RUN, RUN), RUN), :]
            exact_ref[0] = values.astype(jnp.float32)
            out_ref[place] = values
            log_ref[0] = jnp.zeros((1, RUN), jnp.float32)
    else:
        attend()


def attend_forward(qkv, tables, setup):
    parts, tile, seq_count, aligned, runs = setup
    own = runs // parts
    rows = runs * RUN
    return pl.pallas_call(
        functools.partial(forward_kernel, setup),
        grid=(own,),
        out_shape=(
            jax.ShapeDtypeStruct((runs, RUN, HDIM), jnp.bfloat16),
            jax.ShapeDtypeStruct((own, RUN, HDIM), jnp.float32),
            jax.ShapeDtypeStruct((own, 1, RUN), jnp.float32),
        ),
        in_specs=[IN_SMEM] * 5 + [ANY],
        out_specs=(
            pl.BlockSpec((runs, RUN, HDIM), lambda i: (0, 0, 0), pipeline_mode=pl.Buffered(1)),
            pl.BlockSpec((1, RUN, HDIM), lambda i: (i, 0, 0)),
            pl.BlockSpec((1, 1, RUN), lambda i: (i, 0, 0)),
        ),
        scratch_shapes=[
            pltpu.VMEM((own * RUN, HDIM), jnp.bfloat16),
            pltpu.VMEM((rows, HDIM), jnp.bfloat16),
            pltpu.VMEM((rows, HDIM), jnp.bfloat16),
            pltpu.VMEM((HDIM, rows if aligned else RUN), jnp.bfloat16),
            pltpu.SemaphoreType.DMA((3,)),
        ],
        compiler_params=pltpu.CompilerParams(
            dimension_semantics=("arbitrary",), vmem_limit_bytes=VMEM_MOST
        ),
        name="attend_forward",
    )(*tables, qkv)


def backward_kernel(
    setup,
    where_ref,
    low_ref,
    high_ref,
    ends_ref,
    part_ref,
    qkv_ref,
    grad_ref,
    exact_ref,
    log_ref,
    out_ref,
    q_buf,
    k_buf,
    v_buf,
    kt_buf,
    g_buf,
    dk_acc,
    dv_acc,
    stage,
    sem,
    out_sem,
):
    parts, tile, seq_count, aligned, runs = setup
    own = runs // parts
    turn = pl.program_id(0)
    part = part_ref[0]
    scale = 1.0 / math.sqrt(HDIM)
    scale2 = math.log2(math.e) * scale

    @pl.when(turn == 0)
    def _():
        def fetch(source, index, buf, slot, lane):
            return pltpu.make_async_copy(
                source.at[index],
                buf.at[pl.ds(pl.multiple_of(slot * RUN, RUN), RUN), :],
                sem.at[lane],
            )

        def pair(run):
            place = where_ref[run]
            return (
                fetch(qkv_ref.at[1], place, k_buf, run, 1),
                fetch(qkv_ref.at[2], place, v_buf, run, 2),
            )

        def own_pair(index):
            place = where_ref[index * parts + part]
            return (
                fetch(qkv_ref.at[0], place, q_buf, index, 0),
                fetch(grad_ref, place, g_buf, index, 3),
            )

        def start(run, carry):
            for copy in pair(run):
                copy.start()
            return carry

        def start_own(index, carry):
            for copy in own_pair(index):
                copy.start()
            return carry

        def finish(run, carry):
            for copy in pair(run):
                copy.wait()
            return carry

        def finish_own(index, carry):
            for copy in own_pair(index):
                copy.wait()
            return carry

        lax.fori_loop(0, runs, start, 0)
        lax.fori_loop(0, own, start_own, 0)
        dk_acc[...] = jnp.zeros_like(dk_acc)
        dv_acc[...] = jnp.zeros_like(dv_acc)
        lax.fori_loop(0, runs, finish, 0)
        lax.fori_loop(0, own, finish_own, 0)
        if aligned:

            def turn_tile(index, carry):
                low = pl.multiple_of(index * RUN, RUN)
                kt_buf[:, pl.ds(low, RUN)] = k_buf[pl.ds(low, RUN), :].T
                return carry

            lax.fori_loop(0, runs, turn_tile, 0)

    run = turn * parts + part
    low_row = pl.multiple_of(turn * RUN, RUN)

    def attend():
        queries = q_buf[pl.ds(low_row, RUN), :]
        grads = g_buf[pl.ds(low_row, RUN), :]
        delta = jnp.sum((grads.astype(jnp.float32) * exact_ref[0]).T, axis=0, keepdims=True)
        log_total = log_ref[0]

        def key_step(index, acc):
            low = pl.multiple_of(index * tile, tile)
            keys = k_buf[pl.ds(low, tile), :]
            values = v_buf[pl.ds(low, tile), :]
            scores = nt(keys, queries)
            prob = jnp.exp2(scores * scale2 - log_total)
            if not aligned:
                allowed = allowed_tile(ends_ref, seq_count, low, run * RUN, scores.shape)
                prob = jnp.where(allowed, prob, 0.0)
            prob_grad = nt(values, grads)
            dv_acc[pl.ds(low, tile), :] += nn(prob.astype(jnp.bfloat16), grads)
            score_grad = (prob * (prob_grad - delta)).astype(jnp.bfloat16)
            dk_acc[pl.ds(low, tile), :] += nn(score_grad, queries)
            turned = kt_buf[:, pl.ds(low, tile)] if aligned else keys.T
            return acc + nn(turned, score_grad)

        acc = lax.fori_loop(
            low_ref[run], high_ref[run], key_step, jnp.zeros((HDIM, RUN), jnp.float32)
        )
        q_buf[pl.ds(low_row, RUN), :] = (acc.T * scale).astype(jnp.bfloat16)

    if aligned:
        is_valid = run * RUN < ends_ref[seq_count - 1]
        pl.when(is_valid)(attend)

        @pl.when(jnp.logical_not(is_valid))
        def _():
            q_buf[pl.ds(low_row, RUN), :] = jnp.zeros((RUN, HDIM), jnp.bfloat16)
    else:
        attend()

    @pl.when(turn == own - 1)
    def _():
        def key_copies(run_index, slot):
            place = where_ref[run_index]
            return (
                pltpu.make_async_copy(stage.at[slot, 0], out_ref.at[1, place], out_sem.at[slot, 0]),
                pltpu.make_async_copy(stage.at[slot, 1], out_ref.at[2, place], out_sem.at[slot, 1]),
            )

        v_buf[pl.ds(0, RUN), :] = jnp.zeros((RUN, HDIM), jnp.bfloat16)

        def query_copy(run_index):
            mine = run_index % parts == part
            place = where_ref[run_index]
            index = jnp.where(mine, run_index // parts, 0)
            return mine, (
                pltpu.make_async_copy(
                    q_buf.at[pl.ds(pl.multiple_of(index * RUN, RUN), RUN), :],
                    out_ref.at[0, place],
                    sem.at[0],
                ),
                pltpu.make_async_copy(
                    v_buf.at[pl.ds(0, RUN), :], out_ref.at[0, place], sem.at[0]
                ),
            )

        def start_query(run_index, carry):
            mine, (copy, blank) = query_copy(run_index)
            pl.when(mine)(copy.start)
            pl.when(jnp.logical_not(mine))(blank.start)
            return carry

        def finish_query(run_index, carry):
            _, (copy, blank) = query_copy(run_index)
            blank.wait()
            return carry

        lax.fori_loop(0, runs, start_query, 0)

        def write(run_index, carry):
            slot = run_index % 2

            @pl.when(run_index >= 2)
            def _():
                for copy in key_copies(run_index - 2, slot):
                    copy.wait()

            low = pl.multiple_of(run_index * RUN, RUN)
            stage[slot, 0] = (dk_acc[pl.ds(low, RUN), :] * scale).astype(jnp.bfloat16)
            stage[slot, 1] = dv_acc[pl.ds(low, RUN), :].astype(jnp.bfloat16)
            for copy in key_copies(run_index, slot):
                copy.start()
            return carry

        lax.fori_loop(0, runs, write, 0)
        for back in (2, 1):
            for copy in key_copies(runs - back, (runs - back) % 2):
                copy.wait()
        lax.fori_loop(0, runs, finish_query, 0)


def attend_backward(qkv, grads, exact, log_total, tables, setup):
    parts, tile, seq_count, aligned, runs = setup
    own = runs // parts
    rows = runs * RUN
    return pl.pallas_call(
        functools.partial(backward_kernel, setup),
        grid=(own,),
        out_shape=jax.ShapeDtypeStruct((3, runs, RUN, HDIM), jnp.bfloat16),
        in_specs=[IN_SMEM] * 5
        + [
            ANY,
            ANY,
            pl.BlockSpec((1, RUN, HDIM), lambda i: (i, 0, 0)),
            pl.BlockSpec((1, 1, RUN), lambda i: (i, 0, 0)),
        ],
        out_specs=ANY,
        scratch_shapes=[
            pltpu.VMEM((own * RUN, HDIM), jnp.bfloat16),
            pltpu.VMEM((rows, HDIM), jnp.bfloat16),
            pltpu.VMEM((rows, HDIM), jnp.bfloat16),
            pltpu.VMEM((HDIM, rows if aligned else RUN), jnp.bfloat16),
            pltpu.VMEM((own * RUN, HDIM), jnp.bfloat16),
            pltpu.VMEM((rows, HDIM), jnp.float32),
            pltpu.VMEM((rows, HDIM), jnp.float32),
            pltpu.VMEM((2, 2, RUN, HDIM), jnp.bfloat16),
            pltpu.SemaphoreType.DMA((4,)),
            pltpu.SemaphoreType.DMA((2, 2)),
        ],
        compiler_params=pltpu.CompilerParams(
            dimension_semantics=("arbitrary",), vmem_limit_bytes=VMEM_MOST
        ),
        name="attend_backward",
    )(*tables, qkv, grads, exact, log_total)


def stream_tables(token_order, lengths, head_count, seq_size, parts, tile, part):
    runs = token_order.shape[0] // RUN
    stream = (token_order.reshape(head_count, seq_size, RUN)[:, :, 0] // RUN).T.reshape(-1)
    places = jnp.arange(runs, dtype=jnp.int32)
    where = jnp.sum(jnp.where(stream[None, :] == places[:, None], places[None, :], 0), axis=1)
    ends = jnp.cumsum(lengths)
    starts = ends - lengths
    first = places * RUN
    last = first + RUN - 1

    def bound(position, of_seq, of_pad):
        inside = (position[:, None] >= starts[None, :]) & (position[:, None] < ends[None, :])
        found = jnp.sum(jnp.where(inside, of_seq[None, :], 0), axis=1)
        return jnp.where(position < ends[-1], found, of_pad)

    low = bound(first, starts, first) // tile
    high = (bound(last, ends, last + 1) + tile - 1) // tile
    return (
        where.astype(jnp.int32),
        low.astype(jnp.int32),
        high.astype(jnp.int32),
        ends.astype(jnp.int32),
        part.reshape(1).astype(jnp.int32),
    )


def normalize(z_rows, gain, shift):
    average = jnp.mean(z_rows, axis=-1, keepdims=True)
    centered = z_rows - average
    variance = jnp.mean(centered * centered, axis=-1, keepdims=True)
    recip = lax.rsqrt(variance + NORM_EPS)
    normed = centered * recip
    return (normed * gain + shift, normed, recip)


def normalize_back(grad_rows, normed, recip, gain):
    scaled = grad_rows * gain
    dz_rows = recip * (
        scaled
        - jnp.mean(scaled, axis=-1, keepdims=True)
        - normed * jnp.mean(scaled * normed, axis=-1, keepdims=True)
    )
    return (dz_rows, jnp.sum(grad_rows * normed, axis=0), jnp.sum(grad_rows, axis=0))


def group_rows(rows_low):
    return lax.all_gather(rows_low, "head", axis=0, tiled=True)


def group_sums(partial_value):
    return lax.psum_scatter(
        partial_value.astype(jnp.bfloat16), "head", scatter_dimension=0, tiled=True
    ).astype(jnp.float32)


def to_blocks(panel):
    height, breadth = panel.shape
    shaped = panel.reshape(height // BLOCK, BLOCK, breadth // BLOCK, BLOCK)
    return shaped.transpose(0, 2, 1, 3).reshape(-1, BLOCK, BLOCK)


def weight_grad(rows, grads):
    return lax.dot_general(
        rows, grads, (((0,), (0,)), ((), ())), preferred_element_type=jnp.float32
    ).astype(jnp.bfloat16)


def adam_step(param, grad, moment, second, step_float):
    moment_new = 0.9 * moment + 0.1 * grad
    second_new = 0.999 * second + 0.001 * grad * grad
    fix_one = 1.0 - jnp.power(jnp.float32(0.9), step_float)
    fix_two = 1.0 - jnp.power(jnp.float32(0.999), step_float)
    update = ADAM_RATE * (moment_new / fix_one) / (jnp.sqrt(second_new / fix_two) + 1e-08)
    return (param - update, moment_new, second_new)


def shards(
    hidden_in,
    cotangent,
    lengths,
    token_order,
    own_map,
    w_query,
    w_key,
    w_value,
    w_out,
    w_up,
    w_down,
    gains,
    biases,
    up_bias,
    vector_moment,
    vector_second,
    bias_moment,
    bias_second,
    step_count,
    stat_left,
    stat_right,
    root_left,
    root_right,
    master,
):
    head_count = lax.axis_size("head")
    seq_size = lax.axis_size("seq")
    head_index = lax.axis_index("head")
    group_index = lax.axis_index("seq")
    tok_count = hidden_in.shape[0]
    width = hidden_in.shape[1]
    panel_width = w_query.shape[1]
    ff_width = w_up.shape[1]
    seq_count = lengths.shape[0]
    heads = panel_width // HDIM
    parts = seq_size // heads
    runs = token_order.shape[0] // RUN
    aligned = seq_count == 2
    tile = 1024 if aligned else RUN
    setup = (parts, tile, seq_count, aligned, runs)
    tables = stream_tables(
        token_order, lengths, head_count, seq_size, parts, tile, group_index % parts
    )
    own_block = head_index * seq_size + group_index
    order_here = lax.dynamic_slice_in_dim(token_order, own_block * tok_count, tok_count, 0)
    valid_here = order_here < tables[3][seq_count - 1]
    inputs_f32 = hidden_in.astype(jnp.float32)

    qkv_panel = lax.all_gather(
        jnp.concatenate([w_query, w_key, w_value], axis=1), "seq", axis=0, tiled=True
    )
    inputs_grp = group_rows(hidden_in)
    o_panel = lax.all_gather(w_out, "seq", axis=1, tiled=True)
    up_panel = lax.all_gather(w_up, "seq", axis=0, tiled=True)
    down_panel = lax.all_gather(w_down, "seq", axis=1, tiled=True)

    def own_columns(row):
        return lax.dynamic_slice_in_dim(row, head_index * panel_width, panel_width, 0)

    qkv_bias = jnp.concatenate(
        [own_columns(biases[0]), jnp.zeros((panel_width,), jnp.float32), own_columns(biases[1])]
    )
    qkv_grp = (
        jnp.dot(inputs_grp, qkv_panel, preferred_element_type=jnp.float32) + qkv_bias
    ).astype(jnp.bfloat16)
    qkv_head = spread(qkv_grp, 3, heads, parts, seq_size, 0).reshape(3, runs, RUN, HDIM)
    attended_part, attended_exact, log_total = attend_forward(qkv_head, tables, setup)
    rows_grp = head_count * tok_count
    attended_grp = collect(
        attended_part.reshape(1, seq_size, rows_grp, HDIM), heads, parts, 1
    )
    branch_out = group_sums(jnp.dot(attended_grp, o_panel, preferred_element_type=jnp.float32))
    z_one = inputs_f32 + branch_out + biases[2]
    h_one, normed_one, recip_one = normalize(z_one, gains[0], biases[3])
    h_low = h_one.astype(jnp.bfloat16)
    h_grp = group_rows(h_low)
    pre_act = jnp.dot(h_grp, up_panel, preferred_element_type=jnp.float32) + up_bias
    act = jax.nn.gelu(pre_act, approximate=True).astype(jnp.bfloat16)
    ff_out = group_sums(jnp.dot(act, down_panel, preferred_element_type=jnp.float32))
    z_two = h_one + ff_out + biases[4]
    layer_f32, normed_two, recip_two = normalize(z_two, gains[1], biases[5])
    layer_out = layer_f32.astype(jnp.bfloat16)
    grad_y = cotangent.astype(jnp.float32) * valid_here[:, None].astype(jnp.float32)
    dz_two, dgain_two, dshift_two = normalize_back(grad_y, normed_two, recip_two, gains[1])
    dbias_down = jnp.sum(dz_two, axis=0)
    dz_two_grp = group_rows(dz_two.astype(jnp.bfloat16))
    dact = jnp.dot(dz_two_grp, down_panel.T, preferred_element_type=jnp.float32)
    gelu_value, gelu_pull = jax.vjp(lambda inner: jax.nn.gelu(inner, approximate=True), pre_act)
    dpre = gelu_pull(dact)[0].astype(jnp.bfloat16)
    up_bias_part = jnp.sum(dpre.astype(jnp.float32), axis=0)
    dh_one = dz_two + group_sums(jnp.dot(dpre, up_panel.T, preferred_element_type=jnp.float32))
    dz_one, dgain_one, dshift_one = normalize_back(dh_one, normed_one, recip_one, gains[0])
    dbias_out = jnp.sum(dz_one, axis=0)
    dz_one_grp = group_rows(dz_one.astype(jnp.bfloat16))
    dattended = jnp.dot(dz_one_grp, o_panel.T, preferred_element_type=jnp.float32).astype(
        jnp.bfloat16
    )
    dattended_head = spread(dattended, 1, heads, parts, seq_size, 2).reshape(runs, RUN, HDIM)
    dqkv_part = attend_backward(
        qkv_head, dattended_head, attended_exact, log_total, tables, setup
    )
    dqkv_grp = collect(dqkv_part.reshape(3, seq_size, rows_grp, HDIM), heads, parts, 3)
    input_grad = dz_one + group_sums(
        jnp.dot(dqkv_grp, qkv_panel.T, preferred_element_type=jnp.float32)
    )
    grad_down = weight_grad(act, dz_two_grp)
    grad_up = weight_grad(h_grp, dpre)
    grad_out = weight_grad(attended_grp, dz_one_grp)
    grad_qkv = weight_grad(inputs_grp, dqkv_grp)
    bias_qkv = jnp.sum(dqkv_grp.astype(jnp.float32), axis=0)
    zero_width = jnp.zeros((width,), jnp.float32)
    dbias_query = lax.dynamic_update_slice_in_dim(
        zero_width, bias_qkv[:panel_width], head_index * panel_width, 0
    )
    dbias_value = lax.dynamic_update_slice_in_dim(
        zero_width, bias_qkv[2 * panel_width :], head_index * panel_width, 0
    )
    local_vectors = jnp.stack(
        (
            dbias_query,
            dbias_value,
            dbias_out,
            dshift_one,
            dbias_down,
            dshift_two,
            dgain_one,
            dgain_two,
        )
    )
    up_bias_grad = lax.psum(up_bias_part, "seq")
    vector_grad = lax.psum(local_vectors, ("head", "seq"))
    canon = jnp.concatenate(
        [
            to_blocks(grad_qkv[:, :panel_width]),
            to_blocks(grad_qkv[:, panel_width : 2 * panel_width]),
            to_blocks(grad_qkv[:, 2 * panel_width :]),
            to_blocks(grad_out),
            to_blocks(grad_up),
            to_blocks(grad_down),
        ],
        axis=0,
    )
    ordered = jnp.take(canon, own_map[0], axis=0)
    low_grads = lax.psum_scatter(ordered, "seq", scatter_dimension=0, tiled=True)
    block_grads = low_grads.astype(jnp.float32)
    stat_left_new = 0.5 * stat_left + 0.5 * jnp.einsum(
        "bij,bkj->bik", low_grads, low_grads, preferred_element_type=jnp.float32
    )
    stat_right_new = 0.5 * stat_right + 0.5 * jnp.einsum(
        "bji,bjk->bik", low_grads, low_grads, preferred_element_type=jnp.float32
    )
    left_mix = jnp.einsum("bij,bjk->bik", root_left, block_grads, precision=lax.Precision.HIGHEST)
    direction = jnp.einsum("bij,bjk->bik", left_mix, root_right, precision=lax.Precision.HIGHEST)
    master_new = master - SHAMPOO_RATE * direction
    step_float = step_count[0].astype(jnp.float32)
    vector_params = jnp.concatenate([biases, gains], axis=0)
    vector_new, vector_moment_new, vector_second_new = adam_step(
        vector_params, vector_grad, vector_moment, vector_second, step_float
    )
    up_bias_new, bias_moment_new, bias_second_new = adam_step(
        up_bias, up_bias_grad, bias_moment, bias_second, step_float
    )
    return (
        layer_out,
        input_grad,
        block_grads,
        stat_left_new,
        stat_right_new,
        master_new,
        vector_new[0:6],
        vector_new[6:8],
        up_bias_new,
        vector_grad,
        vector_moment_new,
        vector_second_new,
        up_bias_grad,
        bias_moment_new,
        bias_second_new,
    )


def solution(mesh):
    rows = P(("head", "seq"), None)
    blocks = P(("head", "seq"), None, None)
    in_specs = (
        rows,
        rows,
        P(),
        P(),
        P("head", None),
        P("seq", "head"),
        P("seq", "head"),
        P("seq", "head"),
        P("head", "seq"),
        P("seq", "head"),
        P("head", "seq"),
        P(),
        P(),
        P("head"),
        P(),
        P(),
        P("head"),
        P("head"),
        P(),
        blocks,
        blocks,
        blocks,
        blocks,
        blocks,
    )
    out_specs = (
        rows,
        rows,
        blocks,
        blocks,
        blocks,
        blocks,
        P(),
        P(),
        P("head"),
        P(),
        P(),
        P(),
        P("head"),
        P("head"),
        P("head"),
    )
    return jax.shard_map(shards, mesh=mesh, in_specs=in_specs, out_specs=out_specs, check_vma=False)
```

```python
import functools
import math

import jax
import jax.numpy as jnp
from jax import lax
from jax.experimental import pallas as pl
from jax.experimental.pallas import tpu as pltpu
from jax.sharding import PartitionSpec as P

HDIM = 128
BLOCK = 256
RUN = 256

NEG_LARGE = -1e30
NORM_EPS = 1e-12
ADAM_RATE = 0.4
SHAMPOO_RATE = 0.15
MESH = pl.DeviceIdType.MESH
VMEM_MOST = 60 * 1024 * 1024

ANY = pl.BlockSpec(memory_space=pl.ANY)
IN_SMEM = pl.BlockSpec(memory_space=pltpu.SMEM)
IN_VMEM = pl.BlockSpec(memory_space=pltpu.VMEM)


def seq_barrier(me, heads, parts):
    own_head, own_part = me // parts, me % parts
    barrier = pltpu.get_barrier_semaphore()
    for step in range(1, heads):
        pl.semaphore_signal(
            barrier,
            inc=1,
            device_id={"seq": (own_head + step) % heads * parts + own_part},
            device_id_type=MESH,
        )
    for step in range(1, parts):
        pl.semaphore_signal(
            barrier,
            inc=1,
            device_id={"seq": own_head * parts + (own_part + step) % parts},
            device_id_type=MESH,
        )
    pl.semaphore_wait(barrier, heads - 1 + parts - 1)


def spread_kernel(
    fields, heads, parts, x_ref, y_ref, own_sem, send_sem, recv_sem, pass_sem, take_sem
):
    me = lax.axis_index("seq")
    own_head, own_part = me // parts, me % parts
    seq_barrier(me, heads, parts)

    def columns(field, head):
        return pl.ds(pl.multiple_of((field * heads + head) * HDIM, HDIM), HDIM)

    sends = []
    for step in range(1, heads):
        head = (own_head + step) % heads
        for field in range(fields):
            copy = pltpu.make_async_remote_copy(
                src_ref=x_ref.at[:, columns(field, head)],
                dst_ref=y_ref.at[field, me],
                send_sem=send_sem.at[step - 1, field],
                recv_sem=recv_sem.at[step - 1, field],
                device_id={"seq": head * parts + own_part},
                device_id_type=MESH,
            )
            copy.start()
            sends.append(copy)
    owns = []
    for field in range(fields):
        copy = pltpu.make_async_copy(
            x_ref.at[:, columns(field, own_head)], y_ref.at[field, me], own_sem.at[field]
        )
        copy.start()
        owns.append(copy)
    passes = []

    def pass_on(step, field, source):
        origin = (own_head - step + heads) % heads * parts + own_part
        for other in range(1, parts):
            copy = pltpu.make_async_remote_copy(
                src_ref=source,
                dst_ref=y_ref.at[field, origin],
                send_sem=pass_sem.at[other - 1, step, field],
                recv_sem=take_sem.at[other - 1, step, field],
                device_id={"seq": own_head * parts + (own_part + other) % parts},
                device_id_type=MESH,
            )
            copy.start()
            passes.append(copy)

    for field in range(fields):
        pass_on(0, field, x_ref.at[:, columns(field, own_head)])
    for step in range(1, heads):
        origin = (own_head - step + heads) % heads * parts + own_part
        for field in range(fields):
            sends[(step - 1) * fields + field].wait_recv()
            pass_on(step, field, y_ref.at[field, origin])
    for copy in owns:
        copy.wait()
    for copy in sends:
        copy.wait_send()
    for copy in passes:
        copy.wait()


def spread(x_rows, fields, heads, parts, seq_size, collective_id):
    rows = x_rows.shape[0]
    return pl.pallas_call(
        functools.partial(spread_kernel, fields, heads, parts),
        out_shape=jax.ShapeDtypeStruct((fields, seq_size, rows, HDIM), x_rows.dtype),
        in_specs=[IN_VMEM],
        out_specs=ANY,
        scratch_shapes=[
            pltpu.SemaphoreType.DMA((fields,)),
            pltpu.SemaphoreType.DMA((max(heads - 1, 1), fields)),
            pltpu.SemaphoreType.DMA((max(heads - 1, 1), fields)),
            pltpu.SemaphoreType.DMA((max(parts - 1, 1), heads, fields)),
            pltpu.SemaphoreType.DMA((max(parts - 1, 1), heads, fields)),
        ],
        compiler_params=pltpu.CompilerParams(
            collective_id=collective_id, has_side_effects=True, vmem_limit_bytes=24 * 1024 * 1024
        ),
        name="spread",
    )(x_rows)


def collect_kernel(
    fields,
    heads,
    parts,
    x_ref,
    y_ref,
    own,
    got,
    ready,
    own_sem,
    pass_sem,
    take_sem,
    send_sem,
    recv_sem,
    keep_sem,
):
    me = lax.axis_index("seq")
    own_head, own_part = me // parts, me % parts
    seq_barrier(me, heads, parts)
    order = list(range(1, heads)) + [0]

    def home(step, part):
        return (own_head + step) % heads * parts + part

    passes, owns = {}, {}
    for step in order:
        for field in range(fields):
            for other in range(1, parts):
                part = (own_part + other) % parts
                copy = pltpu.make_async_remote_copy(
                    src_ref=x_ref.at[field, home(step, part)],
                    dst_ref=got.at[other - 1, step, field],
                    send_sem=pass_sem.at[other - 1, step, field],
                    recv_sem=take_sem.at[other - 1, step, field],
                    device_id={"seq": own_head * parts + part},
                    device_id_type=MESH,
                )
                copy.start()
                passes[step, field, other] = copy
            copy = pltpu.make_async_copy(
                x_ref.at[field, home(step, own_part)], own.at[step, field], own_sem.at[step, field]
            )
            copy.start()
            owns[step, field] = copy

    sends = []
    for step in order:
        for field in range(fields):
            owns[step, field].wait()
            for other in range(1, parts):
                passes[step, field, other].wait_recv()
            total = own[step, field].astype(jnp.float32)
            for other in range(1, parts):
                total = total + got[other - 1, step, field].astype(jnp.float32)
            ready[step, field] = total.astype(ready.dtype)
            columns = pl.ds(pl.multiple_of((field * heads + own_head) * HDIM, HDIM), HDIM)
            if step == 0:
                copy = pltpu.make_async_copy(
                    ready.at[step, field], y_ref.at[:, columns], keep_sem.at[field]
                )
            else:
                copy = pltpu.make_async_remote_copy(
                    src_ref=ready.at[step, field],
                    dst_ref=y_ref.at[:, columns],
                    send_sem=send_sem.at[step - 1, field],
                    recv_sem=recv_sem.at[step - 1, field],
                    device_id={"seq": home(step, own_part)},
                    device_id_type=MESH,
                )
            copy.start()
            sends.append(copy)
    for copy in sends:
        copy.wait()
    for copy in passes.values():
        copy.wait_send()


def collect(x_parts, heads, parts, collective_id):
    fields, seq_size, rows, _ = x_parts.shape
    kind = x_parts.dtype
    few = max(parts - 1, 1)
    return pl.pallas_call(
        functools.partial(collect_kernel, fields, heads, parts),
        out_shape=jax.ShapeDtypeStruct((rows, fields * heads * HDIM), kind),
        in_specs=[ANY],
        out_specs=ANY,
        scratch_shapes=[
            pltpu.VMEM((heads, fields, rows, HDIM), kind),
            pltpu.VMEM((few, heads, fields, rows, HDIM), kind),
            pltpu.VMEM((heads, fields, rows, HDIM), kind),
            pltpu.SemaphoreType.DMA((heads, fields)),
            pltpu.SemaphoreType.DMA((few, heads, fields)),
            pltpu.SemaphoreType.DMA((few, heads, fields)),
            pltpu.SemaphoreType.DMA((max(heads - 1, 1), fields)),
            pltpu.SemaphoreType.DMA((max(heads - 1, 1), fields)),
            pltpu.SemaphoreType.DMA((fields,)),
        ],
        compiler_params=pltpu.CompilerParams(
            collective_id=collective_id, has_side_effects=True, vmem_limit_bytes=VMEM_MOST
        ),
        name="collect",
    )(x_parts)


def allowed_tile(ends_ref, seq_count, key_low, query_low, shape):
    key_pos = key_low + lax.broadcasted_iota(jnp.int32, shape, 0)
    query_pos = query_low + lax.broadcasted_iota(jnp.int32, shape, 1)
    key_seg = jnp.zeros(shape, jnp.int32)
    query_seg = jnp.zeros(shape, jnp.int32)
    for index in range(seq_count):
        key_seg += (key_pos >= ends_ref[index]).astype(jnp.int32)
        query_seg += (query_pos >= ends_ref[index]).astype(jnp.int32)
    last = ends_ref[seq_count - 1]
    key_seg = jnp.where(key_pos < last, key_seg, seq_count + key_pos)
    query_seg = jnp.where(query_pos < last, query_seg, seq_count + query_pos)
    return key_seg == query_seg


def nt(left, right):
    return lax.dot_general(
        left, right, (((1,), (1,)), ((), ())), preferred_element_type=jnp.float32
    )


def nn(left, right):
    return lax.dot_general(
        left, right, (((1,), (0,)), ((), ())), preferred_element_type=jnp.float32
    )


def forward_kernel(
    setup,
    where_ref,
    low_ref,
    high_ref,
    ends_ref,
    part_ref,
    qkv_ref,
    out_ref,
    exact_ref,
    log_ref,
    q_buf,
    k_buf,
    v_buf,
    vt_buf,
    sem,
):
    parts, tile, seq_count, aligned, runs = setup
    turn = pl.program_id(0)
    part = part_ref[0]
    scale2 = math.log2(math.e) / math.sqrt(HDIM)

    @pl.when(turn == 0)
    def _():
        def fetch(field, run, buf, slot):
            return pltpu.make_async_copy(
                qkv_ref.at[field, where_ref[run]],
                buf.at[pl.ds(pl.multiple_of(slot * RUN, RUN), RUN), :],
                sem.at[field],
            )

        def start(run, carry):
            fetch(1, run, k_buf, run).start()
            fetch(2, run, v_buf, run).start()
            return carry

        def start_own(index, carry):
            fetch(0, index * parts + part, q_buf, index).start()
            return carry

        def finish(run, carry):
            fetch(1, run, k_buf, run).wait()
            fetch(2, run, v_buf, run).wait()
            return carry

        def finish_own(index, carry):
            fetch(0, index * parts + part, q_buf, index).wait()
            return carry

        lax.fori_loop(0, runs, start, 0)
        lax.fori_loop(0, runs // parts, start_own, 0)
        out_ref[...] = jnp.zeros_like(out_ref)
        lax.fori_loop(0, runs, finish, 0)
        lax.fori_loop(0, runs // parts, finish_own, 0)
        if aligned:

            def turn_tile(index, carry):
                low = pl.multiple_of(index * RUN, RUN)
                vt_buf[:, pl.ds(low, RUN)] = v_buf[pl.ds(low, RUN), :].T
                return carry

            lax.fori_loop(0, runs, turn_tile, 0)

    run = turn * parts + part
    place = where_ref[run]
    queries = q_buf[pl.ds(pl.multiple_of(turn * RUN, RUN), RUN), :]

    def attend():
        def key_step(index, carry):
            top, total, acc = carry
            low = pl.multiple_of(index * tile, tile)
            scores = nt(k_buf[pl.ds(low, tile), :], queries)
            if not aligned:
                allowed = allowed_tile(ends_ref, seq_count, low, run * RUN, scores.shape)
                scores = jnp.where(allowed, scores, NEG_LARGE)
            new_top = jnp.maximum(top, jnp.max(scores, axis=0, keepdims=True))
            prob = jnp.exp2((scores - new_top) * scale2)
            if not aligned:
                prob = jnp.where(allowed, prob, 0.0)
            fade = jnp.exp2((top - new_top) * scale2)
            total = total * fade + jnp.sum(prob, axis=0, keepdims=True)
            if aligned:
                turned = vt_buf[:, pl.ds(low, tile)]
            else:
                turned = v_buf[pl.ds(low, tile), :].T
            acc = acc * fade + nn(turned, prob.astype(jnp.bfloat16))
            return new_top, total, acc

        top, total, acc = lax.fori_loop(
            low_ref[run],
            high_ref[run],
            key_step,
            (
                jnp.full((1, RUN), NEG_LARGE, jnp.float32),
                jnp.zeros((1, RUN), jnp.float32),
                jnp.zeros((HDIM, RUN), jnp.float32),
            ),
        )
        result = (acc / total).T
        exact_ref[0] = result
        out_ref[place] = result.astype(out_ref.dtype)
        log_ref[0] = top * scale2 + jnp.log2(total)

    if aligned:
        is_valid = run * RUN < ends_ref[seq_count - 1]
        pl.when(is_valid)(attend)

        @pl.when(jnp.logical_not(is_valid))
        def _():
            values = v_buf[pl.ds(pl.multiple_of(run * RUN, RUN), RUN), :]
            exact_ref[0] = values.astype(jnp.float32)
            out_ref[place] = values
            log_ref[0] = jnp.zeros((1, RUN), jnp.float32)
    else:
        attend()


def attend_forward(qkv, tables, setup):
    parts, tile, seq_count, aligned, runs = setup
    own = runs // parts
    rows = runs * RUN
    return pl.pallas_call(
        functools.partial(forward_kernel, setup),
        grid=(own,),
        out_shape=(
            jax.ShapeDtypeStruct((runs, RUN, HDIM), jnp.bfloat16),
            jax.ShapeDtypeStruct((own, RUN, HDIM), jnp.float32),
            jax.ShapeDtypeStruct((own, 1, RUN), jnp.float32),
        ),
        in_specs=[IN_SMEM] * 5 + [ANY],
        out_specs=(
            pl.BlockSpec((runs, RUN, HDIM), lambda i: (0, 0, 0), pipeline_mode=pl.Buffered(1)),
            pl.BlockSpec((1, RUN, HDIM), lambda i: (i, 0, 0)),
            pl.BlockSpec((1, 1, RUN), lambda i: (i, 0, 0)),
        ),
        scratch_shapes=[
            pltpu.VMEM((own * RUN, HDIM), jnp.bfloat16),
            pltpu.VMEM((rows, HDIM), jnp.bfloat16),
            pltpu.VMEM((rows, HDIM), jnp.bfloat16),
            pltpu.VMEM((HDIM, rows if aligned else RUN), jnp.bfloat16),
            pltpu.SemaphoreType.DMA((3,)),
        ],
        compiler_params=pltpu.CompilerParams(
            dimension_semantics=("arbitrary",), vmem_limit_bytes=VMEM_MOST
        ),
        name="attend_forward",
    )(*tables, qkv)


def backward_kernel(
    setup,
    where_ref,
    low_ref,
    high_ref,
    ends_ref,
    part_ref,
    qkv_ref,
    grad_ref,
    exact_ref,
    log_ref,
    out_ref,
    q_buf,
    k_buf,
    v_buf,
    kt_buf,
    g_buf,
    dk_acc,
    dv_acc,
    stage,
    sem,
    out_sem,
):
    parts, tile, seq_count, aligned, runs = setup
    own = runs // parts
    turn = pl.program_id(0)
    part = part_ref[0]
    scale = 1.0 / math.sqrt(HDIM)
    scale2 = math.log2(math.e) * scale

    @pl.when(turn == 0)
    def _():
        def fetch(source, index, buf, slot, lane):
            return pltpu.make_async_copy(
                source.at[index],
                buf.at[pl.ds(pl.multiple_of(slot * RUN, RUN), RUN), :],
                sem.at[lane],
            )

        def pair(run):
            place = where_ref[run]
            return (
                fetch(qkv_ref.at[1], place, k_buf, run, 1),
                fetch(qkv_ref.at[2], place, v_buf, run, 2),
            )

        def own_pair(index):
            place = where_ref[index * parts + part]
            return (
                fetch(qkv_ref.at[0], place, q_buf, index, 0),
                fetch(grad_ref, place, g_buf, index, 3),
            )

        def start(run, carry):
            for copy in pair(run):
                copy.start()
            return carry

        def start_own(index, carry):
            for copy in own_pair(index):
                copy.start()
            return carry

        def finish(run, carry):
            for copy in pair(run):
                copy.wait()
            return carry

        def finish_own(index, carry):
            for copy in own_pair(index):
                copy.wait()
            return carry

        lax.fori_loop(0, runs, start, 0)
        lax.fori_loop(0, own, start_own, 0)
        dk_acc[...] = jnp.zeros_like(dk_acc)
        dv_acc[...] = jnp.zeros_like(dv_acc)
        lax.fori_loop(0, runs, finish, 0)
        lax.fori_loop(0, own, finish_own, 0)
        if aligned:

            def turn_tile(index, carry):
                low = pl.multiple_of(index * RUN, RUN)
                kt_buf[:, pl.ds(low, RUN)] = k_buf[pl.ds(low, RUN), :].T
                return carry

            lax.fori_loop(0, runs, turn_tile, 0)

    run = turn * parts + part
    low_row = pl.multiple_of(turn * RUN, RUN)

    def attend():
        queries = q_buf[pl.ds(low_row, RUN), :]
        grads = g_buf[pl.ds(low_row, RUN), :]
        delta = jnp.sum((grads.astype(jnp.float32) * exact_ref[0]).T, axis=0, keepdims=True)
        log_total = log_ref[0]

        def key_step(index, acc):
            low = pl.multiple_of(index * tile, tile)
            keys = k_buf[pl.ds(low, tile), :]
            values = v_buf[pl.ds(low, tile), :]
            scores = nt(keys, queries)
            prob = jnp.exp2(scores * scale2 - log_total)
            if not aligned:
                allowed = allowed_tile(ends_ref, seq_count, low, run * RUN, scores.shape)
                prob = jnp.where(allowed, prob, 0.0)
            prob_grad = nt(values, grads)
            dv_acc[pl.ds(low, tile), :] += nn(prob.astype(jnp.bfloat16), grads)
            score_grad = (prob * (prob_grad - delta)).astype(jnp.bfloat16)
            dk_acc[pl.ds(low, tile), :] += nn(score_grad, queries)
            turned = kt_buf[:, pl.ds(low, tile)] if aligned else keys.T
            return acc + nn(turned, score_grad)

        acc = lax.fori_loop(
            low_ref[run], high_ref[run], key_step, jnp.zeros((HDIM, RUN), jnp.float32)
        )
        q_buf[pl.ds(low_row, RUN), :] = (acc.T * scale).astype(jnp.bfloat16)

    if aligned:
        is_valid = run * RUN < ends_ref[seq_count - 1]
        pl.when(is_valid)(attend)

        @pl.when(jnp.logical_not(is_valid))
        def _():
            q_buf[pl.ds(low_row, RUN), :] = jnp.zeros((RUN, HDIM), jnp.bfloat16)
    else:
        attend()

    @pl.when(turn == own - 1)
    def _():
        def key_copies(run_index, slot):
            place = where_ref[run_index]
            return (
                pltpu.make_async_copy(stage.at[slot, 0], out_ref.at[1, place], out_sem.at[slot, 0]),
                pltpu.make_async_copy(stage.at[slot, 1], out_ref.at[2, place], out_sem.at[slot, 1]),
            )

        v_buf[pl.ds(0, RUN), :] = jnp.zeros((RUN, HDIM), jnp.bfloat16)

        def query_copy(run_index):
            mine = run_index % parts == part
            place = where_ref[run_index]
            index = jnp.where(mine, run_index // parts, 0)
            return mine, (
                pltpu.make_async_copy(
                    q_buf.at[pl.ds(pl.multiple_of(index * RUN, RUN), RUN), :],
                    out_ref.at[0, place],
                    sem.at[0],
                ),
                pltpu.make_async_copy(
                    v_buf.at[pl.ds(0, RUN), :], out_ref.at[0, place], sem.at[0]
                ),
            )

        def start_query(run_index, carry):
            mine, (copy, blank) = query_copy(run_index)
            pl.when(mine)(copy.start)
            pl.when(jnp.logical_not(mine))(blank.start)
            return carry

        def finish_query(run_index, carry):
            _, (copy, blank) = query_copy(run_index)
            blank.wait()
            return carry

        lax.fori_loop(0, runs, start_query, 0)

        def write(run_index, carry):
            slot = run_index % 2

            @pl.when(run_index >= 2)
            def _():
                for copy in key_copies(run_index - 2, slot):
                    copy.wait()

            low = pl.multiple_of(run_index * RUN, RUN)
            stage[slot, 0] = (dk_acc[pl.ds(low, RUN), :] * scale).astype(jnp.bfloat16)
            stage[slot, 1] = dv_acc[pl.ds(low, RUN), :].astype(jnp.bfloat16)
            for copy in key_copies(run_index, slot):
                copy.start()
            return carry

        lax.fori_loop(0, runs, write, 0)
        for back in (2, 1):
            for copy in key_copies(runs - back, (runs - back) % 2):
                copy.wait()
        lax.fori_loop(0, runs, finish_query, 0)


def attend_backward(qkv, grads, exact, log_total, tables, setup):
    parts, tile, seq_count, aligned, runs = setup
    own = runs // parts
    rows = runs * RUN
    return pl.pallas_call(
        functools.partial(backward_kernel, setup),
        grid=(own,),
        out_shape=jax.ShapeDtypeStruct((3, runs, RUN, HDIM), jnp.bfloat16),
        in_specs=[IN_SMEM] * 5
        + [
            ANY,
            ANY,
            pl.BlockSpec((1, RUN, HDIM), lambda i: (i, 0, 0)),
            pl.BlockSpec((1, 1, RUN), lambda i: (i, 0, 0)),
        ],
        out_specs=ANY,
        scratch_shapes=[
            pltpu.VMEM((own * RUN, HDIM), jnp.bfloat16),
            pltpu.VMEM((rows, HDIM), jnp.bfloat16),
            pltpu.VMEM((rows, HDIM), jnp.bfloat16),
            pltpu.VMEM((HDIM, rows if aligned else RUN), jnp.bfloat16),
            pltpu.VMEM((own * RUN, HDIM), jnp.bfloat16),
            pltpu.VMEM((rows, HDIM), jnp.float32),
            pltpu.VMEM((rows, HDIM), jnp.float32),
            pltpu.VMEM((2, 2, RUN, HDIM), jnp.bfloat16),
            pltpu.SemaphoreType.DMA((4,)),
            pltpu.SemaphoreType.DMA((2, 2)),
        ],
        compiler_params=pltpu.CompilerParams(
            dimension_semantics=("arbitrary",), vmem_limit_bytes=VMEM_MOST
        ),
        name="attend_backward",
    )(*tables, qkv, grads, exact, log_total)


def stream_tables(token_order, lengths, head_count, seq_size, parts, tile, part):
    runs = token_order.shape[0] // RUN
    stream = (token_order.reshape(head_count, seq_size, RUN)[:, :, 0] // RUN).T.reshape(-1)
    places = jnp.arange(runs, dtype=jnp.int32)
    where = jnp.sum(jnp.where(stream[None, :] == places[:, None], places[None, :], 0), axis=1)
    ends = jnp.cumsum(lengths)
    starts = ends - lengths
    first = places * RUN
    last = first + RUN - 1

    def bound(position, of_seq, of_pad):
        inside = (position[:, None] >= starts[None, :]) & (position[:, None] < ends[None, :])
        found = jnp.sum(jnp.where(inside, of_seq[None, :], 0), axis=1)
        return jnp.where(position < ends[-1], found, of_pad)

    low = bound(first, starts, first) // tile
    high = (bound(last, ends, last + 1) + tile - 1) // tile
    return (
        where.astype(jnp.int32),
        low.astype(jnp.int32),
        high.astype(jnp.int32),
        ends.astype(jnp.int32),
        part.reshape(1).astype(jnp.int32),
    )


PAIR = 2
DEPTH = 4


def grads_kernel(spec, left_ref, right_ref, *refs):
    chips, slots, left_strips, right_strips = spec
    lefts, refs = refs[: len(left_strips)], refs[len(left_strips) :]
    rights, refs = refs[: len(right_strips)], refs[len(right_strips) :]
    (
        out_ref,
        left_buf,
        right_buf,
        strip_buf,
        pair_out,
        pair_in,
        line_out,
        line_in,
        last_in,
        own_sum,
        load_sem,
        pair_send,
        pair_recv,
        line_send,
        line_recv,
        last_recv,
        pair_free,
        line_free,
    ) = refs
    me = lax.axis_index("seq")
    chip, core = me // PAIR, me % PAIR
    sibling = chip * PAIR + (1 - core)
    neighbours = ((chip + 1) * PAIR + core, (chip - 1) * PAIR + core)
    has_next = (chip < chips - 1, chip > 0)

    barrier = pltpu.get_barrier_semaphore()
    pl.semaphore_signal(barrier, inc=1, device_id={"seq": sibling}, device_id_type=MESH)
    for way in range(2):

        @pl.when(has_next[way])
        def _():
            pl.semaphore_signal(
                barrier, inc=1, device_id={"seq": neighbours[way]}, device_id_type=MESH
            )

    ends = (chip == 0).astype(jnp.int32) + (chip == chips - 1).astype(jnp.int32)
    pl.semaphore_wait(barrier, 3 - ends)

    def strip(source, index):
        return source.at[:, pl.ds(pl.multiple_of(index * BLOCK, BLOCK), BLOCK)]

    low = 0
    for source, count in zip(rights, right_strips):

        def load_right(index, carry, source=source, low=low):
            pltpu.make_async_copy(
                strip(source, index), right_buf.at[low + index], load_sem.at[2]
            ).start()
            return carry

        lax.fori_loop(0, count, load_right, 0)
        low += count
    rows = left_buf.shape[2]
    low = 0
    for source, count in zip(lefts, left_strips):

        def fetch(index, slot, source=source):
            return pltpu.make_async_copy(strip(source, index), strip_buf.at[slot], load_sem.at[slot])

        def turn_strip(index, carry, count=count, low=low, fetch=fetch):
            slot = index % 2

            @pl.when(index + 1 < count)
            def _():
                fetch(index + 1, 1 - slot).start()

            fetch(index, slot).wait()
            for part in range(rows // BLOCK):
                span = pl.ds(part * BLOCK, BLOCK)
                left_buf[low + index, :, span] = strip_buf[slot, span, :].T
            return carry

        fetch(0, 0).start()
        lax.fori_loop(0, count, turn_strip, 0)
        low += count
    low = 0
    for source, count in zip(rights, right_strips):

        def wait_right(index, carry, source=source, low=low):
            pltpu.make_async_copy(
                strip(source, index), right_buf.at[low + index], load_sem.at[2]
            ).wait()
            return carry

        lax.fori_loop(0, count, wait_right, 0)
        low += count

    def product(owner_chip, owner_core, k):
        slot = (owner_chip * PAIR + owner_core) * slots + k
        return nn(left_buf[left_ref[slot]], right_buf[right_ref[slot]])

    counts = ((chips - 1 - chip) * slots, chip * slots, slots)

    def owner(stream, step):
        if stream == 0:
            return chips - 1 - step // slots
        if stream == 1:
            return step // slots
        return chip

    def pair_copy(stream, step):
        slot = step % DEPTH
        return pltpu.make_async_remote_copy(
            src_ref=pair_out.at[stream, slot],
            dst_ref=pair_in.at[stream, slot],
            send_sem=pair_send.at[stream, slot],
            recv_sem=pair_recv.at[stream, slot],
            device_id={"seq": sibling},
            device_id_type=MESH,
        )

    def line_copy(stream, step):
        slot = step % DEPTH
        return pltpu.make_async_remote_copy(
            src_ref=line_out.at[stream, slot],
            dst_ref=line_in.at[stream, slot],
            send_sem=line_send.at[stream, slot],
            recv_sem=line_recv.at[stream, slot],
            device_id={"seq": neighbours[stream]},
            device_id_type=MESH,
        )

    def last_copy(stream, step):
        slot, k = step % DEPTH, step % slots
        return pltpu.make_async_remote_copy(
            src_ref=line_out.at[stream, slot],
            dst_ref=last_in.at[stream, k],
            send_sem=line_send.at[stream, slot],
            recv_sem=last_recv.at[stream, k],
            device_id={"seq": neighbours[stream]},
            device_id_type=MESH,
        )

    def give(stream, step):
        slot = step % DEPTH

        @pl.when(step >= DEPTH)
        def _():
            pair_copy(stream, step).wait_send()
            pl.semaphore_wait(pair_free.at[stream], 1)

        pair_out[stream, slot] = product(owner(stream, step), 1 - core, step % slots).astype(
            jnp.bfloat16
        )
        pair_copy(stream, step).start()

    def take(stream, step):
        slot = step % DEPTH
        total = product(owner(stream, step), core, step % slots)
        pair_copy(stream, step).wait_recv()
        total = total + pair_in[stream, slot].astype(jnp.float32)

        @pl.when(step + DEPTH < counts[stream])
        def _():
            pl.semaphore_signal(
                pair_free.at[stream], inc=1, device_id={"seq": sibling}, device_id_type=MESH
            )

        return total

    def forward(stream, step):
        slot = step % DEPTH
        target = chip + 1 if stream == 0 else chip - 1
        ends_there = owner(stream, step) == target
        has_source = has_next[1 - stream]
        total = take(stream, step)

        @pl.when(step >= DEPTH)
        def _():
            line_copy(stream, step).wait_send()

        @pl.when(has_source)
        def _():
            line_copy(stream, step).wait_recv()
            line_out[stream, slot] = (total + line_in[stream, slot].astype(jnp.float32)).astype(
                jnp.bfloat16
            )

            @pl.when(step + DEPTH < counts[stream])
            def _():
                pl.semaphore_signal(
                    line_free.at[stream],
                    inc=1,
                    device_id={"seq": neighbours[1 - stream]},
                    device_id_type=MESH,
                )

        @pl.when(jnp.logical_not(has_source))
        def _():
            line_out[stream, slot] = total.astype(jnp.bfloat16)

        @pl.when(ends_there)
        def _():
            last_copy(stream, step).start()

        @pl.when(jnp.logical_not(ends_there))
        def _():
            @pl.when(step >= DEPTH)
            def _():
                pl.semaphore_wait(line_free.at[stream], 1)

            line_copy(stream, step).start()

    def keep(step):
        own_sum[step] = take(2, step).astype(jnp.bfloat16)

    for stream in range(2):
        pl.when(counts[stream] > 0)(functools.partial(give, stream, 0))

    def body(step, carry):
        for stream in range(2):
            pl.when(step + 1 < counts[stream])(functools.partial(give, stream, step + 1))
        own_step = step - slots

        @pl.when((own_step + 1 >= 0) & (own_step + 1 < slots))
        def _():
            give(2, own_step + 1)

        for stream in range(2):
            pl.when(step < counts[stream])(functools.partial(forward, stream, step))

        @pl.when((own_step >= 0) & (own_step < slots))
        def _():
            keep(own_step)

        return carry

    lax.fori_loop(0, (chips - 1) * slots, body, 0)

    def finish(k, carry):
        out_ref[k] = own_sum[k]
        for stream in range(2):

            @pl.when(has_next[1 - stream])
            def _():
                last_copy(stream, k).wait_recv()
                out_ref[k] = (
                    out_ref[k].astype(jnp.float32) + last_in[stream, k].astype(jnp.float32)
                ).astype(jnp.bfloat16)

        return carry

    lax.fori_loop(0, slots, finish, 0)
    for slot in range(DEPTH):
        for stream in range(2):

            @pl.when(counts[stream] > 0)
            def _():
                line_copy(stream, slot).wait_send()
                pair_copy(stream, slot).wait_send()

        pair_copy(2, slot).wait_send()


def owned_grads(left_index, right_index, lefts, rights, seq_size, collective_id):
    rows = lefts[0].shape[0]
    left_strips = tuple(array.shape[1] // BLOCK for array in lefts)
    right_strips = tuple(array.shape[1] // BLOCK for array in rights)
    chips = seq_size // PAIR
    slots = left_index.shape[0] // seq_size
    kind = jnp.bfloat16
    block = (BLOCK, BLOCK)
    products = chips * PAIR * slots
    return pl.pallas_call(
        functools.partial(grads_kernel, (chips, slots, left_strips, right_strips)),
        out_shape=jax.ShapeDtypeStruct((slots,) + block, kind),
        in_specs=[IN_SMEM] * 2 + [ANY] * (len(lefts) + len(rights)),
        out_specs=IN_VMEM,
        scratch_shapes=[
            pltpu.VMEM((sum(left_strips), BLOCK, rows), kind),
            pltpu.VMEM((sum(right_strips), rows, BLOCK), kind),
            pltpu.VMEM((2, rows, BLOCK), kind),
            pltpu.VMEM((3, DEPTH) + block, kind),
            pltpu.VMEM((3, DEPTH) + block, kind),
            pltpu.VMEM((2, DEPTH) + block, kind),
            pltpu.VMEM((2, DEPTH) + block, kind),
            pltpu.VMEM((2, slots) + block, kind),
            pltpu.VMEM((slots,) + block, kind),
            pltpu.SemaphoreType.DMA((3,)),
            pltpu.SemaphoreType.DMA((3, DEPTH)),
            pltpu.SemaphoreType.DMA((3, DEPTH)),
            pltpu.SemaphoreType.DMA((2, DEPTH)),
            pltpu.SemaphoreType.DMA((2, DEPTH)),
            pltpu.SemaphoreType.DMA((2, slots)),
            pltpu.SemaphoreType.REGULAR((3,)),
            pltpu.SemaphoreType.REGULAR((2,)),
        ],
        compiler_params=pltpu.CompilerParams(
            collective_id=collective_id, has_side_effects=True, vmem_limit_bytes=VMEM_MOST
        ),
        cost_estimate=pl.CostEstimate(
            flops=products * 2 * rows * BLOCK * BLOCK,
            bytes_accessed=2 * (sum(left_strips) + sum(right_strips)) * rows * BLOCK,
            transcendentals=0,
        ),
        name="owned_grads",
    )(left_index, right_index, *lefts, *rights)


def block_operands(own_map, width, panel_width, ff_width):
    deep, narrow, wide = width // BLOCK, panel_width // BLOCK, ff_width // BLOCK
    left = jnp.zeros_like(own_map)
    right = jnp.zeros_like(own_map)
    first, left_low, right_low = 0, 0, 0
    panels = [(deep, narrow, 0, 0), (deep, narrow, 0, narrow), (deep, narrow, 0, 2 * narrow)]
    panels.append((narrow, deep, deep, 3 * narrow))
    panels.append((deep, wide, deep + narrow, 3 * narrow + deep))
    panels.append((wide, deep, 2 * deep + narrow, 3 * narrow + deep + wide))
    for high, broad, left_low, right_low in panels:
        inside = (own_map >= first) & (own_map < first + high * broad)
        within = own_map - first
        left = jnp.where(inside, left_low + within // broad, left)
        right = jnp.where(inside, right_low + within % broad, right)
        first += high * broad
    return left.astype(jnp.int32), right.astype(jnp.int32)


def normalize(z_rows, gain, shift):
    average = jnp.mean(z_rows, axis=-1, keepdims=True)
    centered = z_rows - average
    variance = jnp.mean(centered * centered, axis=-1, keepdims=True)
    recip = lax.rsqrt(variance + NORM_EPS)
    normed = centered * recip
    return (normed * gain + shift, normed, recip)


def normalize_back(grad_rows, normed, recip, gain):
    scaled = grad_rows * gain
    dz_rows = recip * (
        scaled
        - jnp.mean(scaled, axis=-1, keepdims=True)
        - normed * jnp.mean(scaled * normed, axis=-1, keepdims=True)
    )
    return (dz_rows, jnp.sum(grad_rows * normed, axis=0), jnp.sum(grad_rows, axis=0))


def group_rows(rows_low):
    return lax.all_gather(rows_low, "head", axis=0, tiled=True)


def group_sums(partial_value):
    return lax.psum_scatter(
        partial_value.astype(jnp.bfloat16), "head", scatter_dimension=0, tiled=True
    ).astype(jnp.float32)


def adam_step(param, grad, moment, second, step_float):
    moment_new = 0.9 * moment + 0.1 * grad
    second_new = 0.999 * second + 0.001 * grad * grad
    fix_one = 1.0 - jnp.power(jnp.float32(0.9), step_float)
    fix_two = 1.0 - jnp.power(jnp.float32(0.999), step_float)
    update = ADAM_RATE * (moment_new / fix_one) / (jnp.sqrt(second_new / fix_two) + 1e-08)
    return (param - update, moment_new, second_new)


def shards(
    hidden_in,
    cotangent,
    lengths,
    token_order,
    own_map,
    w_query,
    w_key,
    w_value,
    w_out,
    w_up,
    w_down,
    gains,
    biases,
    up_bias,
    vector_moment,
    vector_second,
    bias_moment,
    bias_second,
    step_count,
    stat_left,
    stat_right,
    root_left,
    root_right,
    master,
):
    head_count = lax.axis_size("head")
    seq_size = lax.axis_size("seq")
    head_index = lax.axis_index("head")
    group_index = lax.axis_index("seq")
    tok_count = hidden_in.shape[0]
    width = hidden_in.shape[1]
    panel_width = w_query.shape[1]
    ff_width = w_up.shape[1]
    seq_count = lengths.shape[0]
    heads = panel_width // HDIM
    parts = seq_size // heads
    runs = token_order.shape[0] // RUN
    aligned = seq_count == 2
    tile = 1024 if aligned else RUN
    setup = (parts, tile, seq_count, aligned, runs)
    tables = stream_tables(
        token_order, lengths, head_count, seq_size, parts, tile, group_index % parts
    )
    own_block = head_index * seq_size + group_index
    order_here = lax.dynamic_slice_in_dim(token_order, own_block * tok_count, tok_count, 0)
    valid_here = order_here < tables[3][seq_count - 1]
    inputs_f32 = hidden_in.astype(jnp.float32)

    qkv_panel = lax.all_gather(
        jnp.concatenate([w_query, w_key, w_value], axis=1), "seq", axis=0, tiled=True
    )
    inputs_grp = group_rows(hidden_in)
    o_panel = lax.all_gather(w_out, "seq", axis=1, tiled=True)
    up_panel = lax.all_gather(w_up, "seq", axis=0, tiled=True)
    down_panel = lax.all_gather(w_down, "seq", axis=1, tiled=True)

    def own_columns(row):
        return lax.dynamic_slice_in_dim(row, head_index * panel_width, panel_width, 0)

    qkv_bias = jnp.concatenate(
        [own_columns(biases[0]), jnp.zeros((panel_width,), jnp.float32), own_columns(biases[1])]
    )
    qkv_grp = (
        jnp.dot(inputs_grp, qkv_panel, preferred_element_type=jnp.float32) + qkv_bias
    ).astype(jnp.bfloat16)
    qkv_head = spread(qkv_grp, 3, heads, parts, seq_size, 0).reshape(3, runs, RUN, HDIM)
    attended_part, attended_exact, log_total = attend_forward(qkv_head, tables, setup)
    rows_grp = head_count * tok_count
    attended_grp = collect(
        attended_part.reshape(1, seq_size, rows_grp, HDIM), heads, parts, 1
    )
    branch_out = group_sums(jnp.dot(attended_grp, o_panel, preferred_element_type=jnp.float32))
    z_one = inputs_f32 + branch_out + biases[2]
    h_one, normed_one, recip_one = normalize(z_one, gains[0], biases[3])
    h_low = h_one.astype(jnp.bfloat16)
    h_grp = group_rows(h_low)
    pre_act = jnp.dot(h_grp, up_panel, preferred_element_type=jnp.float32) + up_bias
    act = jax.nn.gelu(pre_act, approximate=True).astype(jnp.bfloat16)
    ff_out = group_sums(jnp.dot(act, down_panel, preferred_element_type=jnp.float32))
    z_two = h_one + ff_out + biases[4]
    layer_f32, normed_two, recip_two = normalize(z_two, gains[1], biases[5])
    layer_out = layer_f32.astype(jnp.bfloat16)
    grad_y = cotangent.astype(jnp.float32) * valid_here[:, None].astype(jnp.float32)
    dz_two, dgain_two, dshift_two = normalize_back(grad_y, normed_two, recip_two, gains[1])
    dbias_down = jnp.sum(dz_two, axis=0)
    dz_two_grp = group_rows(dz_two.astype(jnp.bfloat16))
    dact = jnp.dot(dz_two_grp, down_panel.T, preferred_element_type=jnp.float32)
    gelu_value, gelu_pull = jax.vjp(lambda inner: jax.nn.gelu(inner, approximate=True), pre_act)
    dpre = gelu_pull(dact)[0].astype(jnp.bfloat16)
    up_bias_part = jnp.sum(dpre.astype(jnp.float32), axis=0)
    dh_one = dz_two + group_sums(jnp.dot(dpre, up_panel.T, preferred_element_type=jnp.float32))
    dz_one, dgain_one, dshift_one = normalize_back(dh_one, normed_one, recip_one, gains[0])
    dbias_out = jnp.sum(dz_one, axis=0)
    dz_one_grp = group_rows(dz_one.astype(jnp.bfloat16))
    dattended = jnp.dot(dz_one_grp, o_panel.T, preferred_element_type=jnp.float32).astype(
        jnp.bfloat16
    )
    dattended_head = spread(dattended, 1, heads, parts, seq_size, 2).reshape(runs, RUN, HDIM)
    dqkv_part = attend_backward(
        qkv_head, dattended_head, attended_exact, log_total, tables, setup
    )
    dqkv_grp = collect(dqkv_part.reshape(3, seq_size, rows_grp, HDIM), heads, parts, 3)
    input_grad = dz_one + group_sums(
        jnp.dot(dqkv_grp, qkv_panel.T, preferred_element_type=jnp.float32)
    )
    bias_qkv = jnp.sum(dqkv_grp.astype(jnp.float32), axis=0)
    zero_width = jnp.zeros((width,), jnp.float32)
    dbias_query = lax.dynamic_update_slice_in_dim(
        zero_width, bias_qkv[:panel_width], head_index * panel_width, 0
    )
    dbias_value = lax.dynamic_update_slice_in_dim(
        zero_width, bias_qkv[2 * panel_width :], head_index * panel_width, 0
    )
    local_vectors = jnp.stack(
        (
            dbias_query,
            dbias_value,
            dbias_out,
            dshift_one,
            dbias_down,
            dshift_two,
            dgain_one,
            dgain_two,
        )
    )
    up_bias_grad = lax.psum(up_bias_part, "seq")
    vector_grad = lax.psum(local_vectors, ("head", "seq"))
    left_index, right_index = block_operands(own_map[0], width, panel_width, ff_width)
    low_grads = owned_grads(
        left_index,
        right_index,
        (inputs_grp, attended_grp, h_grp, act),
        (dqkv_grp, dz_one_grp, dpre, dz_two_grp),
        seq_size,
        4,
    )
    block_grads = low_grads.astype(jnp.float32)
    stat_left_new = 0.5 * stat_left + 0.5 * jnp.einsum(
        "bij,bkj->bik", low_grads, low_grads, preferred_element_type=jnp.float32
    )
    stat_right_new = 0.5 * stat_right + 0.5 * jnp.einsum(
        "bji,bjk->bik", low_grads, low_grads, preferred_element_type=jnp.float32
    )
    left_mix = jnp.einsum("bij,bjk->bik", root_left, block_grads, precision=lax.Precision.HIGHEST)
    direction = jnp.einsum("bij,bjk->bik", left_mix, root_right, precision=lax.Precision.HIGHEST)
    master_new = master - SHAMPOO_RATE * direction
    step_float = step_count[0].astype(jnp.float32)
    vector_params = jnp.concatenate([biases, gains], axis=0)
    vector_new, vector_moment_new, vector_second_new = adam_step(
        vector_params, vector_grad, vector_moment, vector_second, step_float
    )
    up_bias_new, bias_moment_new, bias_second_new = adam_step(
        up_bias, up_bias_grad, bias_moment, bias_second, step_float
    )
    return (
        layer_out,
        input_grad,
        block_grads,
        stat_left_new,
        stat_right_new,
        master_new,
        vector_new[0:6],
        vector_new[6:8],
        up_bias_new,
        vector_grad,
        vector_moment_new,
        vector_second_new,
        up_bias_grad,
        bias_moment_new,
        bias_second_new,
    )


def solution(mesh):
    rows = P(("head", "seq"), None)
    blocks = P(("head", "seq"), None, None)
    in_specs = (
        rows,
        rows,
        P(),
        P(),
        P("head", None),
        P("seq", "head"),
        P("seq", "head"),
        P("seq", "head"),
        P("head", "seq"),
        P("seq", "head"),
        P("head", "seq"),
        P(),
        P(),
        P("head"),
        P(),
        P(),
        P("head"),
        P("head"),
        P(),
        blocks,
        blocks,
        blocks,
        blocks,
        blocks,
    )
    out_specs = (
        rows,
        rows,
        blocks,
        blocks,
        blocks,
        blocks,
        P(),
        P(),
        P("head"),
        P(),
        P(),
        P(),
        P("head"),
        P("head"),
        P("head"),
    )
    return jax.shard_map(shards, mesh=mesh, in_specs=in_specs, out_specs=out_specs, check_vma=False)
```

```python
import functools
import math

import jax
import jax.numpy as jnp
from jax import lax
from jax.experimental import pallas as pl
from jax.experimental.pallas import tpu as pltpu
from jax.sharding import PartitionSpec as P

HDIM = 128
BLOCK = 256
RUN = 256

NEG_LARGE = -1e30
NORM_EPS = 1e-12
ADAM_RATE = 0.4
SHAMPOO_RATE = 0.15
MESH = pl.DeviceIdType.MESH
VMEM_MOST = 60 * 1024 * 1024

ANY = pl.BlockSpec(memory_space=pl.ANY)
IN_SMEM = pl.BlockSpec(memory_space=pltpu.SMEM)
IN_VMEM = pl.BlockSpec(memory_space=pltpu.VMEM)


def busy(microseconds):
    return pl.CostEstimate(
        flops=microseconds * 800_000_000, bytes_accessed=1_000_000, transcendentals=0
    )


def seq_barrier(me, heads, parts):
    own_head, own_part = me // parts, me % parts
    barrier = pltpu.get_barrier_semaphore()
    for step in range(1, heads):
        pl.semaphore_signal(
            barrier,
            inc=1,
            device_id={"seq": (own_head + step) % heads * parts + own_part},
            device_id_type=MESH,
        )
    for step in range(1, parts):
        pl.semaphore_signal(
            barrier,
            inc=1,
            device_id={"seq": own_head * parts + (own_part + step) % parts},
            device_id_type=MESH,
        )
    pl.semaphore_wait(barrier, heads - 1 + parts - 1)


def spread_kernel(
    fields, heads, parts, x_ref, y_ref, own_sem, send_sem, recv_sem, pass_sem, take_sem
):
    me = lax.axis_index("seq")
    own_head, own_part = me // parts, me % parts
    seq_barrier(me, heads, parts)

    def columns(field, head):
        return pl.ds(pl.multiple_of((field * heads + head) * HDIM, HDIM), HDIM)

    sends = []
    for step in range(1, heads):
        head = (own_head + step) % heads
        for field in range(fields):
            copy = pltpu.make_async_remote_copy(
                src_ref=x_ref.at[:, columns(field, head)],
                dst_ref=y_ref.at[field, me],
                send_sem=send_sem.at[step - 1, field],
                recv_sem=recv_sem.at[step - 1, field],
                device_id={"seq": head * parts + own_part},
                device_id_type=MESH,
            )
            copy.start()
            sends.append(copy)
    owns = []
    for field in range(fields):
        copy = pltpu.make_async_copy(
            x_ref.at[:, columns(field, own_head)], y_ref.at[field, me], own_sem.at[field]
        )
        copy.start()
        owns.append(copy)
    passes = []

    def pass_on(step, field, source):
        origin = (own_head - step + heads) % heads * parts + own_part
        for other in range(1, parts):
            copy = pltpu.make_async_remote_copy(
                src_ref=source,
                dst_ref=y_ref.at[field, origin],
                send_sem=pass_sem.at[other - 1, step, field],
                recv_sem=take_sem.at[other - 1, step, field],
                device_id={"seq": own_head * parts + (own_part + other) % parts},
                device_id_type=MESH,
            )
            copy.start()
            passes.append(copy)

    for field in range(fields):
        pass_on(0, field, x_ref.at[:, columns(field, own_head)])
    for step in range(1, heads):
        origin = (own_head - step + heads) % heads * parts + own_part
        for field in range(fields):
            sends[(step - 1) * fields + field].wait_recv()
            pass_on(step, field, y_ref.at[field, origin])
    for copy in owns:
        copy.wait()
    for copy in sends:
        copy.wait_send()
    for copy in passes:
        copy.wait()


def spread(x_rows, fields, heads, parts, seq_size, collective_id):
    rows = x_rows.shape[0]
    return pl.pallas_call(
        functools.partial(spread_kernel, fields, heads, parts),
        out_shape=jax.ShapeDtypeStruct((fields, seq_size, rows, HDIM), x_rows.dtype),
        in_specs=[IN_VMEM],
        out_specs=ANY,
        scratch_shapes=[
            pltpu.SemaphoreType.DMA((fields,)),
            pltpu.SemaphoreType.DMA((max(heads - 1, 1), fields)),
            pltpu.SemaphoreType.DMA((max(heads - 1, 1), fields)),
            pltpu.SemaphoreType.DMA((max(parts - 1, 1), heads, fields)),
            pltpu.SemaphoreType.DMA((max(parts - 1, 1), heads, fields)),
        ],
        compiler_params=pltpu.CompilerParams(
            collective_id=collective_id, has_side_effects=True, vmem_limit_bytes=24 * 1024 * 1024
        ),
        cost_estimate=busy(fields * 24),
        name="spread",
    )(x_rows)


def collect_kernel(
    fields,
    heads,
    parts,
    x_ref,
    y_ref,
    own,
    got,
    ready,
    own_sem,
    pass_sem,
    take_sem,
    send_sem,
    recv_sem,
    keep_sem,
):
    me = lax.axis_index("seq")
    own_head, own_part = me // parts, me % parts
    seq_barrier(me, heads, parts)
    order = list(range(1, heads)) + [0]

    def home(step, part):
        return (own_head + step) % heads * parts + part

    passes, owns = {}, {}
    for step in order:
        for field in range(fields):
            for other in range(1, parts):
                part = (own_part + other) % parts
                copy = pltpu.make_async_remote_copy(
                    src_ref=x_ref.at[field, home(step, part)],
                    dst_ref=got.at[other - 1, step, field],
                    send_sem=pass_sem.at[other - 1, step, field],
                    recv_sem=take_sem.at[other - 1, step, field],
                    device_id={"seq": own_head * parts + part},
                    device_id_type=MESH,
                )
                copy.start()
                passes[step, field, other] = copy
            copy = pltpu.make_async_copy(
                x_ref.at[field, home(step, own_part)], own.at[step, field], own_sem.at[step, field]
            )
            copy.start()
            owns[step, field] = copy

    sends = []
    for step in order:
        for field in range(fields):
            owns[step, field].wait()
            for other in range(1, parts):
                passes[step, field, other].wait_recv()
            total = own[step, field].astype(jnp.float32)
            for other in range(1, parts):
                total = total + got[other - 1, step, field].astype(jnp.float32)
            ready[step, field] = total.astype(ready.dtype)
            columns = pl.ds(pl.multiple_of((field * heads + own_head) * HDIM, HDIM), HDIM)
            if step == 0:
                copy = pltpu.make_async_copy(
                    ready.at[step, field], y_ref.at[:, columns], keep_sem.at[field]
                )
            else:
                copy = pltpu.make_async_remote_copy(
                    src_ref=ready.at[step, field],
                    dst_ref=y_ref.at[:, columns],
                    send_sem=send_sem.at[step - 1, field],
                    recv_sem=recv_sem.at[step - 1, field],
                    device_id={"seq": home(step, own_part)},
                    device_id_type=MESH,
                )
            copy.start()
            sends.append(copy)
    for copy in sends:
        copy.wait()
    for copy in passes.values():
        copy.wait_send()


def collect(x_parts, heads, parts, collective_id):
    fields, seq_size, rows, _ = x_parts.shape
    kind = x_parts.dtype
    few = max(parts - 1, 1)
    return pl.pallas_call(
        functools.partial(collect_kernel, fields, heads, parts),
        out_shape=jax.ShapeDtypeStruct((rows, fields * heads * HDIM), kind),
        in_specs=[ANY],
        out_specs=ANY,
        scratch_shapes=[
            pltpu.VMEM((heads, fields, rows, HDIM), kind),
            pltpu.VMEM((few, heads, fields, rows, HDIM), kind),
            pltpu.VMEM((heads, fields, rows, HDIM), kind),
            pltpu.SemaphoreType.DMA((heads, fields)),
            pltpu.SemaphoreType.DMA((few, heads, fields)),
            pltpu.SemaphoreType.DMA((few, heads, fields)),
            pltpu.SemaphoreType.DMA((max(heads - 1, 1), fields)),
            pltpu.SemaphoreType.DMA((max(heads - 1, 1), fields)),
            pltpu.SemaphoreType.DMA((fields,)),
        ],
        compiler_params=pltpu.CompilerParams(
            collective_id=collective_id, has_side_effects=True, vmem_limit_bytes=VMEM_MOST
        ),
        cost_estimate=busy(fields * 24),
        name="collect",
    )(x_parts)


def allowed_tile(ends_ref, seq_count, key_low, query_low, shape):
    key_pos = key_low + lax.broadcasted_iota(jnp.int32, shape, 0)
    query_pos = query_low + lax.broadcasted_iota(jnp.int32, shape, 1)
    key_seg = jnp.zeros(shape, jnp.int32)
    query_seg = jnp.zeros(shape, jnp.int32)
    for index in range(seq_count):
        key_seg += (key_pos >= ends_ref[index]).astype(jnp.int32)
        query_seg += (query_pos >= ends_ref[index]).astype(jnp.int32)
    last = ends_ref[seq_count - 1]
    key_seg = jnp.where(key_pos < last, key_seg, seq_count + key_pos)
    query_seg = jnp.where(query_pos < last, query_seg, seq_count + query_pos)
    return key_seg == query_seg


def nt(left, right):
    return lax.dot_general(
        left, right, (((1,), (1,)), ((), ())), preferred_element_type=jnp.float32
    )


def nn(left, right):
    return lax.dot_general(
        left, right, (((1,), (0,)), ((), ())), preferred_element_type=jnp.float32
    )


def forward_kernel(
    setup,
    where_ref,
    low_ref,
    high_ref,
    ends_ref,
    part_ref,
    qkv_ref,
    out_ref,
    exact_ref,
    log_ref,
    q_buf,
    k_buf,
    v_buf,
    vt_buf,
    sem,
):
    parts, tile, seq_count, aligned, runs = setup
    turn = pl.program_id(0)
    part = part_ref[0]
    scale2 = math.log2(math.e) / math.sqrt(HDIM)

    @pl.when(turn == 0)
    def _():
        def fetch(field, run, buf, slot):
            return pltpu.make_async_copy(
                qkv_ref.at[field, where_ref[run]],
                buf.at[pl.ds(pl.multiple_of(slot * RUN, RUN), RUN), :],
                sem.at[field],
            )

        def start(run, carry):
            fetch(1, run, k_buf, run).start()
            fetch(2, run, v_buf, run).start()
            return carry

        def start_own(index, carry):
            fetch(0, index * parts + part, q_buf, index).start()
            return carry

        def finish(run, carry):
            fetch(1, run, k_buf, run).wait()
            fetch(2, run, v_buf, run).wait()
            return carry

        def finish_own(index, carry):
            fetch(0, index * parts + part, q_buf, index).wait()
            return carry

        lax.fori_loop(0, runs, start, 0)
        lax.fori_loop(0, runs // parts, start_own, 0)
        out_ref[...] = jnp.zeros_like(out_ref)
        lax.fori_loop(0, runs, finish, 0)
        lax.fori_loop(0, runs // parts, finish_own, 0)
        if aligned:

            def turn_tile(index, carry):
                low = pl.multiple_of(index * RUN, RUN)
                vt_buf[:, pl.ds(low, RUN)] = v_buf[pl.ds(low, RUN), :].T
                return carry

            lax.fori_loop(0, runs, turn_tile, 0)

    run = turn * parts + part
    place = where_ref[run]
    queries = q_buf[pl.ds(pl.multiple_of(turn * RUN, RUN), RUN), :]

    def attend():
        def key_step(index, carry):
            top, total, acc = carry
            low = pl.multiple_of(index * tile, tile)
            scores = nt(k_buf[pl.ds(low, tile), :], queries)
            if not aligned:
                allowed = allowed_tile(ends_ref, seq_count, low, run * RUN, scores.shape)
                scores = jnp.where(allowed, scores, NEG_LARGE)
            new_top = jnp.maximum(top, jnp.max(scores, axis=0, keepdims=True))
            prob = jnp.exp2((scores - new_top) * scale2)
            if not aligned:
                prob = jnp.where(allowed, prob, 0.0)
            fade = jnp.exp2((top - new_top) * scale2)
            total = total * fade + jnp.sum(prob, axis=0, keepdims=True)
            if aligned:
                turned = vt_buf[:, pl.ds(low, tile)]
            else:
                turned = v_buf[pl.ds(low, tile), :].T
            acc = acc * fade + nn(turned, prob.astype(jnp.bfloat16))
            return new_top, total, acc

        top, total, acc = lax.fori_loop(
            low_ref[run],
            high_ref[run],
            key_step,
            (
                jnp.full((1, RUN), NEG_LARGE, jnp.float32),
                jnp.zeros((1, RUN), jnp.float32),
                jnp.zeros((HDIM, RUN), jnp.float32),
            ),
        )
        result = (acc / total).T
        exact_ref[0] = result
        out_ref[place] = result.astype(out_ref.dtype)
        log_ref[0] = top * scale2 + jnp.log2(total)

    if aligned:
        is_valid = run * RUN < ends_ref[seq_count - 1]
        pl.when(is_valid)(attend)

        @pl.when(jnp.logical_not(is_valid))
        def _():
            values = v_buf[pl.ds(pl.multiple_of(run * RUN, RUN), RUN), :]
            exact_ref[0] = values.astype(jnp.float32)
            out_ref[place] = values
            log_ref[0] = jnp.zeros((1, RUN), jnp.float32)
    else:
        attend()


def attend_forward(qkv, tables, setup):
    parts, tile, seq_count, aligned, runs = setup
    own = runs // parts
    rows = runs * RUN
    return pl.pallas_call(
        functools.partial(forward_kernel, setup),
        grid=(own,),
        out_shape=(
            jax.ShapeDtypeStruct((runs, RUN, HDIM), jnp.bfloat16),
            jax.ShapeDtypeStruct((own, RUN, HDIM), jnp.float32),
            jax.ShapeDtypeStruct((own, 1, RUN), jnp.float32),
        ),
        in_specs=[IN_SMEM] * 5 + [ANY],
        out_specs=(
            pl.BlockSpec((runs, RUN, HDIM), lambda i: (0, 0, 0), pipeline_mode=pl.Buffered(1)),
            pl.BlockSpec((1, RUN, HDIM), lambda i: (i, 0, 0)),
            pl.BlockSpec((1, 1, RUN), lambda i: (i, 0, 0)),
        ),
        scratch_shapes=[
            pltpu.VMEM((own * RUN, HDIM), jnp.bfloat16),
            pltpu.VMEM((rows, HDIM), jnp.bfloat16),
            pltpu.VMEM((rows, HDIM), jnp.bfloat16),
            pltpu.VMEM((HDIM, rows if aligned else RUN), jnp.bfloat16),
            pltpu.SemaphoreType.DMA((3,)),
        ],
        compiler_params=pltpu.CompilerParams(
            dimension_semantics=("arbitrary",), vmem_limit_bytes=VMEM_MOST
        ),
        cost_estimate=busy(36),
        name="attend_forward",
    )(*tables, qkv)


def backward_kernel(
    setup,
    where_ref,
    low_ref,
    high_ref,
    ends_ref,
    part_ref,
    qkv_ref,
    grad_ref,
    exact_ref,
    log_ref,
    out_ref,
    q_buf,
    k_buf,
    v_buf,
    kt_buf,
    g_buf,
    dk_acc,
    dv_acc,
    stage,
    sem,
    out_sem,
):
    parts, tile, seq_count, aligned, runs = setup
    own = runs // parts
    turn = pl.program_id(0)
    part = part_ref[0]
    scale = 1.0 / math.sqrt(HDIM)
    scale2 = math.log2(math.e) * scale

    @pl.when(turn == 0)
    def _():
        def fetch(source, index, buf, slot, lane):
            return pltpu.make_async_copy(
                source.at[index],
                buf.at[pl.ds(pl.multiple_of(slot * RUN, RUN), RUN), :],
                sem.at[lane],
            )

        def pair(run):
            place = where_ref[run]
            return (
                fetch(qkv_ref.at[1], place, k_buf, run, 1),
                fetch(qkv_ref.at[2], place, v_buf, run, 2),
            )

        def own_pair(index):
            place = where_ref[index * parts + part]
            return (
                fetch(qkv_ref.at[0], place, q_buf, index, 0),
                fetch(grad_ref, place, g_buf, index, 3),
            )

        def start(run, carry):
            for copy in pair(run):
                copy.start()
            return carry

        def start_own(index, carry):
            for copy in own_pair(index):
                copy.start()
            return carry

        def finish(run, carry):
            for copy in pair(run):
                copy.wait()
            return carry

        def finish_own(index, carry):
            for copy in own_pair(index):
                copy.wait()
            return carry

        lax.fori_loop(0, runs, start, 0)
        lax.fori_loop(0, own, start_own, 0)
        dk_acc[...] = jnp.zeros_like(dk_acc)
        dv_acc[...] = jnp.zeros_like(dv_acc)
        lax.fori_loop(0, runs, finish, 0)
        lax.fori_loop(0, own, finish_own, 0)
        if aligned:

            def turn_tile(index, carry):
                low = pl.multiple_of(index * RUN, RUN)
                kt_buf[:, pl.ds(low, RUN)] = k_buf[pl.ds(low, RUN), :].T
                return carry

            lax.fori_loop(0, runs, turn_tile, 0)

    run = turn * parts + part
    low_row = pl.multiple_of(turn * RUN, RUN)

    def attend():
        queries = q_buf[pl.ds(low_row, RUN), :]
        grads = g_buf[pl.ds(low_row, RUN), :]
        delta = jnp.sum((grads.astype(jnp.float32) * exact_ref[0]).T, axis=0, keepdims=True)
        log_total = log_ref[0]

        def key_step(index, acc):
            low = pl.multiple_of(index * tile, tile)
            keys = k_buf[pl.ds(low, tile), :]
            values = v_buf[pl.ds(low, tile), :]
            scores = nt(keys, queries)
            prob = jnp.exp2(scores * scale2 - log_total)
            if not aligned:
                allowed = allowed_tile(ends_ref, seq_count, low, run * RUN, scores.shape)
                prob = jnp.where(allowed, prob, 0.0)
            prob_grad = nt(values, grads)
            dv_acc[pl.ds(low, tile), :] += nn(prob.astype(jnp.bfloat16), grads)
            score_grad = (prob * (prob_grad - delta)).astype(jnp.bfloat16)
            dk_acc[pl.ds(low, tile), :] += nn(score_grad, queries)
            turned = kt_buf[:, pl.ds(low, tile)] if aligned else keys.T
            return acc + nn(turned, score_grad)

        acc = lax.fori_loop(
            low_ref[run], high_ref[run], key_step, jnp.zeros((HDIM, RUN), jnp.float32)
        )
        q_buf[pl.ds(low_row, RUN), :] = (acc.T * scale).astype(jnp.bfloat16)

    if aligned:
        is_valid = run * RUN < ends_ref[seq_count - 1]
        pl.when(is_valid)(attend)

        @pl.when(jnp.logical_not(is_valid))
        def _():
            q_buf[pl.ds(low_row, RUN), :] = jnp.zeros((RUN, HDIM), jnp.bfloat16)
    else:
        attend()

    @pl.when(turn == own - 1)
    def _():
        def key_copies(run_index, slot):
            place = where_ref[run_index]
            return (
                pltpu.make_async_copy(stage.at[slot, 0], out_ref.at[1, place], out_sem.at[slot, 0]),
                pltpu.make_async_copy(stage.at[slot, 1], out_ref.at[2, place], out_sem.at[slot, 1]),
            )

        v_buf[pl.ds(0, RUN), :] = jnp.zeros((RUN, HDIM), jnp.bfloat16)

        def query_copy(run_index):
            mine = run_index % parts == part
            place = where_ref[run_index]
            index = jnp.where(mine, run_index // parts, 0)
            return mine, (
                pltpu.make_async_copy(
                    q_buf.at[pl.ds(pl.multiple_of(index * RUN, RUN), RUN), :],
                    out_ref.at[0, place],
                    sem.at[0],
                ),
                pltpu.make_async_copy(
                    v_buf.at[pl.ds(0, RUN), :], out_ref.at[0, place], sem.at[0]
                ),
            )

        def start_query(run_index, carry):
            mine, (copy, blank) = query_copy(run_index)
            pl.when(mine)(copy.start)
            pl.when(jnp.logical_not(mine))(blank.start)
            return carry

        def finish_query(run_index, carry):
            _, (copy, blank) = query_copy(run_index)
            blank.wait()
            return carry

        lax.fori_loop(0, runs, start_query, 0)

        def write(run_index, carry):
            slot = run_index % 2

            @pl.when(run_index >= 2)
            def _():
                for copy in key_copies(run_index - 2, slot):
                    copy.wait()

            low = pl.multiple_of(run_index * RUN, RUN)
            stage[slot, 0] = (dk_acc[pl.ds(low, RUN), :] * scale).astype(jnp.bfloat16)
            stage[slot, 1] = dv_acc[pl.ds(low, RUN), :].astype(jnp.bfloat16)
            for copy in key_copies(run_index, slot):
                copy.start()
            return carry

        lax.fori_loop(0, runs, write, 0)
        for back in (2, 1):
            for copy in key_copies(runs - back, (runs - back) % 2):
                copy.wait()
        lax.fori_loop(0, runs, finish_query, 0)


def attend_backward(qkv, grads, exact, log_total, tables, setup):
    parts, tile, seq_count, aligned, runs = setup
    own = runs // parts
    rows = runs * RUN
    return pl.pallas_call(
        functools.partial(backward_kernel, setup),
        grid=(own,),
        out_shape=jax.ShapeDtypeStruct((3, runs, RUN, HDIM), jnp.bfloat16),
        in_specs=[IN_SMEM] * 5
        + [
            ANY,
            ANY,
            pl.BlockSpec((1, RUN, HDIM), lambda i: (i, 0, 0)),
            pl.BlockSpec((1, 1, RUN), lambda i: (i, 0, 0)),
        ],
        out_specs=ANY,
        scratch_shapes=[
            pltpu.VMEM((own * RUN, HDIM), jnp.bfloat16),
            pltpu.VMEM((rows, HDIM), jnp.bfloat16),
            pltpu.VMEM((rows, HDIM), jnp.bfloat16),
            pltpu.VMEM((HDIM, rows if aligned else RUN), jnp.bfloat16),
            pltpu.VMEM((own * RUN, HDIM), jnp.bfloat16),
            pltpu.VMEM((rows, HDIM), jnp.float32),
            pltpu.VMEM((rows, HDIM), jnp.float32),
            pltpu.VMEM((2, 2, RUN, HDIM), jnp.bfloat16),
            pltpu.SemaphoreType.DMA((4,)),
            pltpu.SemaphoreType.DMA((2, 2)),
        ],
        compiler_params=pltpu.CompilerParams(
            dimension_semantics=("arbitrary",), vmem_limit_bytes=VMEM_MOST
        ),
        cost_estimate=busy(50),
        name="attend_backward",
    )(*tables, qkv, grads, exact, log_total)


def stream_tables(token_order, lengths, head_count, seq_size, parts, tile, part):
    runs = token_order.shape[0] // RUN
    stream = (token_order.reshape(head_count, seq_size, RUN)[:, :, 0] // RUN).T.reshape(-1)
    places = jnp.arange(runs, dtype=jnp.int32)
    where = jnp.sum(jnp.where(stream[None, :] == places[:, None], places[None, :], 0), axis=1)
    ends = jnp.cumsum(lengths)
    starts = ends - lengths
    first = places * RUN
    last = first + RUN - 1

    def bound(position, of_seq, of_pad):
        inside = (position[:, None] >= starts[None, :]) & (position[:, None] < ends[None, :])
        found = jnp.sum(jnp.where(inside, of_seq[None, :], 0), axis=1)
        return jnp.where(position < ends[-1], found, of_pad)

    low = bound(first, starts, first) // tile
    high = (bound(last, ends, last + 1) + tile - 1) // tile
    return (
        where.astype(jnp.int32),
        low.astype(jnp.int32),
        high.astype(jnp.int32),
        ends.astype(jnp.int32),
        part.reshape(1).astype(jnp.int32),
    )


PAIR = 2
DEPTH = 6
LAG = 2


def grads_kernel(spec, left_ref, right_ref, *refs):
    chips, slots, left_strips, right_strips = spec
    lefts, refs = refs[: len(left_strips)], refs[len(left_strips) :]
    rights, refs = refs[: len(right_strips)], refs[len(right_strips) :]
    (
        out_ref,
        left_buf,
        right_buf,
        strip_buf,
        pair_out,
        pair_in,
        line_out,
        line_in,
        last_in,
        own_sum,
        load_sem,
        pair_send,
        pair_recv,
        line_send,
        line_recv,
        last_recv,
        pair_free,
        line_free,
    ) = refs
    me = lax.axis_index("seq")
    chip, core = me // PAIR, me % PAIR
    sibling = chip * PAIR + (1 - core)
    neighbours = ((chip + 1) * PAIR + core, (chip - 1) * PAIR + core)
    has_next = (chip < chips - 1, chip > 0)

    barrier = pltpu.get_barrier_semaphore()
    pl.semaphore_signal(barrier, inc=1, device_id={"seq": sibling}, device_id_type=MESH)
    for way in range(2):

        @pl.when(has_next[way])
        def _():
            pl.semaphore_signal(
                barrier, inc=1, device_id={"seq": neighbours[way]}, device_id_type=MESH
            )

    ends = (chip == 0).astype(jnp.int32) + (chip == chips - 1).astype(jnp.int32)
    pl.semaphore_wait(barrier, 3 - ends)

    def strip(source, index):
        return source.at[:, pl.ds(pl.multiple_of(index * BLOCK, BLOCK), BLOCK)]

    low = 0
    for source, count in zip(rights, right_strips):

        def load_right(index, carry, source=source, low=low):
            pltpu.make_async_copy(
                strip(source, index), right_buf.at[low + index], load_sem.at[2]
            ).start()
            return carry

        lax.fori_loop(0, count, load_right, 0)
        low += count
    rows = left_buf.shape[2]
    low = 0
    for source, count in zip(lefts, left_strips):

        def fetch(index, slot, source=source):
            return pltpu.make_async_copy(strip(source, index), strip_buf.at[slot], load_sem.at[slot])

        def turn_strip(index, carry, count=count, low=low, fetch=fetch):
            slot = index % 2

            @pl.when(index + 1 < count)
            def _():
                fetch(index + 1, 1 - slot).start()

            fetch(index, slot).wait()
            for part in range(rows // BLOCK):
                span = pl.ds(part * BLOCK, BLOCK)
                left_buf[low + index, :, span] = strip_buf[slot, span, :].T
            return carry

        fetch(0, 0).start()
        lax.fori_loop(0, count, turn_strip, 0)
        low += count
    low = 0
    for source, count in zip(rights, right_strips):

        def wait_right(index, carry, source=source, low=low):
            pltpu.make_async_copy(
                strip(source, index), right_buf.at[low + index], load_sem.at[2]
            ).wait()
            return carry

        lax.fori_loop(0, count, wait_right, 0)
        low += count

    def product(owner_chip, owner_core, k):
        slot = (owner_chip * PAIR + owner_core) * slots + k
        return nn(left_buf[left_ref[slot]], right_buf[right_ref[slot]])

    counts = ((chips - 1 - chip) * slots, chip * slots, slots)

    def owner(stream, step):
        if stream == 0:
            return chips - 1 - step // slots
        if stream == 1:
            return step // slots
        return chip

    def pair_copy(stream, step):
        slot = step % DEPTH
        return pltpu.make_async_remote_copy(
            src_ref=pair_out.at[stream, slot],
            dst_ref=pair_in.at[stream, slot],
            send_sem=pair_send.at[stream, slot],
            recv_sem=pair_recv.at[stream, slot],
            device_id={"seq": sibling},
            device_id_type=MESH,
        )

    def line_copy(stream, step):
        slot = step % DEPTH
        return pltpu.make_async_remote_copy(
            src_ref=line_out.at[stream, slot],
            dst_ref=line_in.at[stream, slot],
            send_sem=line_send.at[stream, slot],
            recv_sem=line_recv.at[stream, slot],
            device_id={"seq": neighbours[stream]},
            device_id_type=MESH,
        )

    def last_copy(stream, step):
        slot, k = step % DEPTH, step % slots
        return pltpu.make_async_remote_copy(
            src_ref=line_out.at[stream, slot],
            dst_ref=last_in.at[stream, k],
            send_sem=line_send.at[stream, slot],
            recv_sem=last_recv.at[stream, k],
            device_id={"seq": neighbours[stream]},
            device_id_type=MESH,
        )

    def give(stream, step):
        slot = step % DEPTH

        @pl.when(step >= DEPTH)
        def _():
            pair_copy(stream, step).wait_send()
            pl.semaphore_wait(pair_free.at[stream], 1)

        pair_out[stream, slot] = product(owner(stream, step), 1 - core, step % slots).astype(
            jnp.bfloat16
        )
        pair_copy(stream, step).start()

    def take(stream, step):
        slot = step % DEPTH
        total = product(owner(stream, step), core, step % slots)
        pair_copy(stream, step).wait_recv()
        total = total + pair_in[stream, slot].astype(jnp.float32)

        @pl.when(step + DEPTH < counts[stream])
        def _():
            pl.semaphore_signal(
                pair_free.at[stream], inc=1, device_id={"seq": sibling}, device_id_type=MESH
            )

        return total

    def forward(stream, step):
        slot = step % DEPTH
        target = chip + 1 if stream == 0 else chip - 1
        ends_there = owner(stream, step) == target
        has_source = has_next[1 - stream]
        total = take(stream, step)

        @pl.when(step >= DEPTH)
        def _():
            line_copy(stream, step).wait_send()

        @pl.when(has_source)
        def _():
            line_copy(stream, step).wait_recv()
            line_out[stream, slot] = (total + line_in[stream, slot].astype(jnp.float32)).astype(
                jnp.bfloat16
            )

            @pl.when(step + DEPTH < counts[stream])
            def _():
                pl.semaphore_signal(
                    line_free.at[stream],
                    inc=1,
                    device_id={"seq": neighbours[1 - stream]},
                    device_id_type=MESH,
                )

        @pl.when(jnp.logical_not(has_source))
        def _():
            line_out[stream, slot] = total.astype(jnp.bfloat16)

        @pl.when(ends_there)
        def _():
            last_copy(stream, step).start()

        @pl.when(jnp.logical_not(ends_there))
        def _():
            @pl.when(step >= DEPTH)
            def _():
                pl.semaphore_wait(line_free.at[stream], 1)

            line_copy(stream, step).start()

    def keep(step):
        own_sum[step] = take(2, step).astype(jnp.bfloat16)

    for stream in range(2):
        pl.when(counts[stream] > 0)(functools.partial(give, stream, 0))
    give(2, 0)

    delays = (chip * LAG, (chips - 1 - chip) * LAG, slots)

    def body(turn, carry):
        for stream in range(3):
            step = turn - delays[stream] + 1

            @pl.when((step > 0) & (step < counts[stream]))
            def _():
                give(stream, step)

        for stream in range(3):
            step = turn - delays[stream]

            @pl.when((step >= 0) & (step < counts[stream]))
            def _():
                if stream < 2:
                    forward(stream, step)
                else:
                    keep(step)

        return carry

    lax.fori_loop(0, (chips - 1) * slots + (chips - 1) * LAG, body, 0)

    def finish(k, carry):
        out_ref[k] = own_sum[k]
        for stream in range(2):

            @pl.when(has_next[1 - stream])
            def _():
                last_copy(stream, k).wait_recv()
                out_ref[k] = (
                    out_ref[k].astype(jnp.float32) + last_in[stream, k].astype(jnp.float32)
                ).astype(jnp.bfloat16)

        return carry

    lax.fori_loop(0, slots, finish, 0)
    for slot in range(DEPTH):
        for stream in range(2):

            @pl.when(counts[stream] > 0)
            def _():
                line_copy(stream, slot).wait_send()
                pair_copy(stream, slot).wait_send()

        pair_copy(2, slot).wait_send()


def owned_grads(left_index, right_index, lefts, rights, seq_size, collective_id):
    rows = lefts[0].shape[0]
    left_strips = tuple(array.shape[1] // BLOCK for array in lefts)
    right_strips = tuple(array.shape[1] // BLOCK for array in rights)
    chips = seq_size // PAIR
    slots = left_index.shape[0] // seq_size
    kind = jnp.bfloat16
    block = (BLOCK, BLOCK)
    return pl.pallas_call(
        functools.partial(grads_kernel, (chips, slots, left_strips, right_strips)),
        out_shape=jax.ShapeDtypeStruct((slots,) + block, kind),
        in_specs=[IN_SMEM] * 2 + [ANY] * (len(lefts) + len(rights)),
        out_specs=IN_VMEM,
        scratch_shapes=[
            pltpu.VMEM((sum(left_strips), BLOCK, rows), kind),
            pltpu.VMEM((sum(right_strips), rows, BLOCK), kind),
            pltpu.VMEM((2, rows, BLOCK), kind),
            pltpu.VMEM((3, DEPTH) + block, kind),
            pltpu.VMEM((3, DEPTH) + block, kind),
            pltpu.VMEM((2, DEPTH) + block, kind),
            pltpu.VMEM((2, DEPTH) + block, kind),
            pltpu.VMEM((2, slots) + block, kind),
            pltpu.VMEM((slots,) + block, kind),
            pltpu.SemaphoreType.DMA((3,)),
            pltpu.SemaphoreType.DMA((3, DEPTH)),
            pltpu.SemaphoreType.DMA((3, DEPTH)),
            pltpu.SemaphoreType.DMA((2, DEPTH)),
            pltpu.SemaphoreType.DMA((2, DEPTH)),
            pltpu.SemaphoreType.DMA((2, slots)),
            pltpu.SemaphoreType.REGULAR((3,)),
            pltpu.SemaphoreType.REGULAR((2,)),
        ],
        compiler_params=pltpu.CompilerParams(
            collective_id=collective_id, has_side_effects=True, vmem_limit_bytes=VMEM_MOST
        ),
        cost_estimate=busy(240),
        name="owned_grads",
    )(left_index, right_index, *lefts, *rights)


def block_operands(own_map, width, panel_width, ff_width):
    deep, narrow, wide = width // BLOCK, panel_width // BLOCK, ff_width // BLOCK
    left = jnp.zeros_like(own_map)
    right = jnp.zeros_like(own_map)
    first, left_low, right_low = 0, 0, 0
    panels = [(deep, narrow, 0, 0), (deep, narrow, 0, narrow), (deep, narrow, 0, 2 * narrow)]
    panels.append((narrow, deep, deep, 3 * narrow))
    panels.append((deep, wide, deep + narrow, 3 * narrow + deep))
    panels.append((wide, deep, 2 * deep + narrow, 3 * narrow + deep + wide))
    for high, broad, left_low, right_low in panels:
        inside = (own_map >= first) & (own_map < first + high * broad)
        within = own_map - first
        left = jnp.where(inside, left_low + within // broad, left)
        right = jnp.where(inside, right_low + within % broad, right)
        first += high * broad
    return left.astype(jnp.int32), right.astype(jnp.int32)


def group_peer(me, count, slot, way):
    far, near = slot // 2, slot % 2
    half = count // 2
    return (me // 2 + way * far + half) % half * 2 + (me % 2 + near) % 2


def group_barrier(me, count):
    barrier = pltpu.get_barrier_semaphore()
    for slot in range(1, count):
        pl.semaphore_signal(
            barrier, inc=1, device_id={"head": group_peer(me, count, slot, 1)}, device_id_type=MESH
        )
    pl.semaphore_wait(barrier, count - 1)


GELU_SCALE = 0.7978845608028654
GELU_CUBIC = 0.044715
WIDE = 512


def gelu(u):
    return 0.5 * u * (1.0 + jnp.tanh(GELU_SCALE * (u + GELU_CUBIC * (u * u * u))))


def gelu_slope(u):
    square = u * u
    bend = jnp.tanh(GELU_SCALE * (u + GELU_CUBIC * (square * u)))
    inner = GELU_SCALE * (1.0 + 3.0 * GELU_CUBIC * square)
    return 0.5 * (1.0 + bend) + 0.5 * u * (1.0 - bend * bend) * inner


def feed_kernel(is_forward, count, x_ref, up_ref, down_ref, side_ref, *refs):
    if is_forward:
        rows_ref, mid_ref, pre_ref, sum_ref = refs[:4]
        refs = refs[4:]
    else:
        rows_ref, mid_ref, sum_ref = refs[:3]
        refs = refs[3:]
    (
        land,
        up_buf,
        down_buf,
        mid_buf,
        pre_buf,
        part_buf,
        got,
        load_sem,
        send_sem,
        recv_sem,
        back_sem,
        got_sem,
        out_sem,
    ) = refs
    me = lax.axis_index("head")
    width, ff_width = up_buf.shape
    loads = [
        pltpu.make_async_copy(up_ref, up_buf, load_sem.at[0]),
        pltpu.make_async_copy(down_ref, down_buf, load_sem.at[1]),
    ]
    if not is_forward:
        loads.append(pltpu.make_async_copy(side_ref, pre_buf, load_sem.at[2]))
    for copy in loads:
        copy.start()
    group_barrier(me, count)

    def push(slot):
        return pltpu.make_async_remote_copy(
            src_ref=x_ref,
            dst_ref=land.at[slot],
            send_sem=send_sem.at[slot],
            recv_sem=recv_sem.at[slot],
            device_id={"head": group_peer(me, count, slot, 1)},
            device_id_type=MESH,
        )

    def give_back(slot):
        return pltpu.make_async_remote_copy(
            src_ref=part_buf.at[slot],
            dst_ref=got.at[slot],
            send_sem=back_sem.at[slot],
            recv_sem=got_sem.at[slot],
            device_id={"head": group_peer(me, count, slot, -1)},
            device_id_type=MESH,
        )

    def outs(slot):
        copies = [
            pltpu.make_async_copy(land.at[slot], rows_ref.at[slot], out_sem.at[0, slot]),
            pltpu.make_async_copy(mid_buf.at[slot], mid_ref.at[slot], out_sem.at[1, slot]),
        ]
        if is_forward:
            copies.append(
                pltpu.make_async_copy(pre_buf.at[slot], pre_ref.at[slot], out_sem.at[2, slot])
            )
        return copies

    for slot in range(1, count):
        push(slot).start()
    land[0] = x_ref[...]
    for copy in loads:
        copy.wait()

    def work(slot, carry):
        @pl.when(slot > 0)
        def _():
            push(slot).wait_recv()

        def hidden(index, inner):
            span = pl.ds(pl.multiple_of(index * WIDE, WIDE), WIDE)
            if is_forward:
                pre = nn(land[slot], up_buf[:, span]) + side_ref[:, span]
                pre_buf[slot, :, span] = pre.astype(jnp.bfloat16)
                mid_buf[slot, :, span] = gelu(pre).astype(jnp.bfloat16)
            else:
                grad = nt(land[slot], down_buf[span, :])
                slope = gelu_slope(pre_buf[slot, :, span].astype(jnp.float32))
                mid_buf[slot, :, span] = (grad * slope).astype(jnp.bfloat16)
            return inner

        def result(index, inner):
            span = pl.ds(pl.multiple_of(index * WIDE, WIDE), WIDE)
            if is_forward:
                part = nn(mid_buf[slot], down_buf[:, span])
            else:
                part = nt(mid_buf[slot], up_buf[span, :])

            @pl.when(slot == 0)
            def _():
                sum_ref[:, span] = part

            @pl.when(slot > 0)
            def _():
                part_buf[slot, :, span] = part.astype(jnp.bfloat16)

            return inner

        lax.fori_loop(0, ff_width // WIDE, hidden, 0)
        for copy in outs(slot):
            copy.start()
        lax.fori_loop(0, width // WIDE, result, 0)

        @pl.when(slot > 0)
        def _():
            give_back(slot).start()

        return carry

    lax.fori_loop(0, count, work, 0)

    def add(slot, carry):
        give_back(slot).wait_recv()
        sum_ref[...] += got[slot].astype(jnp.float32)
        return carry

    lax.fori_loop(1, count, add, 0)
    for slot in range(count):
        for copy in outs(slot):
            copy.wait()
        if slot > 0:
            push(slot).wait_send()
            give_back(slot).wait_send()


def feed(x_rows, up_panel, down_panel, side, is_forward, count, collective_id):
    rows, width = x_rows.shape
    ff_width = up_panel.shape[1]
    kind = jnp.bfloat16
    by_width = jax.ShapeDtypeStruct((count, rows, width), kind)
    by_ff = jax.ShapeDtypeStruct((count, rows, ff_width), kind)
    total = jax.ShapeDtypeStruct((rows, width), jnp.float32)
    out_shape = (by_width, by_ff, by_ff, total) if is_forward else (by_width, by_ff, total)
    return pl.pallas_call(
        functools.partial(feed_kernel, is_forward, count),
        out_shape=out_shape,
        in_specs=[IN_VMEM, ANY, ANY, IN_VMEM if is_forward else ANY],
        out_specs=(ANY,) * (len(out_shape) - 1) + (IN_VMEM,),
        scratch_shapes=[
            pltpu.VMEM((count, rows, width), kind),
            pltpu.VMEM(up_panel.shape, kind),
            pltpu.VMEM(down_panel.shape, kind),
            pltpu.VMEM((count, rows, ff_width), kind),
            pltpu.VMEM((count, rows, ff_width), kind),
            pltpu.VMEM((count, rows, width), kind),
            pltpu.VMEM((count, rows, width), kind),
            pltpu.SemaphoreType.DMA((3,)),
            pltpu.SemaphoreType.DMA((count,)),
            pltpu.SemaphoreType.DMA((count,)),
            pltpu.SemaphoreType.DMA((count,)),
            pltpu.SemaphoreType.DMA((count,)),
            pltpu.SemaphoreType.DMA((3, count)),
        ],
        compiler_params=pltpu.CompilerParams(
            collective_id=collective_id, has_side_effects=True, vmem_limit_bytes=VMEM_MOST
        ),
        cost_estimate=busy(90),
        name="feed_forward" if is_forward else "feed_backward",
    )(x_rows, up_panel, down_panel, side)


def normalize(z_rows, gain, shift):
    average = jnp.mean(z_rows, axis=-1, keepdims=True)
    centered = z_rows - average
    variance = jnp.mean(centered * centered, axis=-1, keepdims=True)
    recip = lax.rsqrt(variance + NORM_EPS)
    normed = centered * recip
    return (normed * gain + shift, normed, recip)


def normalize_back(grad_rows, normed, recip, gain):
    scaled = grad_rows * gain
    dz_rows = recip * (
        scaled
        - jnp.mean(scaled, axis=-1, keepdims=True)
        - normed * jnp.mean(scaled * normed, axis=-1, keepdims=True)
    )
    return (dz_rows, jnp.sum(grad_rows * normed, axis=0), jnp.sum(grad_rows, axis=0))


def group_rows(rows_low):
    return lax.all_gather(rows_low, "head", axis=0, tiled=True)


def group_sums(partial_value):
    return lax.psum_scatter(
        partial_value.astype(jnp.bfloat16), "head", scatter_dimension=0, tiled=True
    ).astype(jnp.float32)


def adam_step(param, grad, moment, second, step_float):
    moment_new = 0.9 * moment + 0.1 * grad
    second_new = 0.999 * second + 0.001 * grad * grad
    fix_one = 1.0 - jnp.power(jnp.float32(0.9), step_float)
    fix_two = 1.0 - jnp.power(jnp.float32(0.999), step_float)
    update = ADAM_RATE * (moment_new / fix_one) / (jnp.sqrt(second_new / fix_two) + 1e-08)
    return (param - update, moment_new, second_new)


def shards(
    hidden_in,
    cotangent,
    lengths,
    token_order,
    own_map,
    w_query,
    w_key,
    w_value,
    w_out,
    w_up,
    w_down,
    gains,
    biases,
    up_bias,
    vector_moment,
    vector_second,
    bias_moment,
    bias_second,
    step_count,
    stat_left,
    stat_right,
    root_left,
    root_right,
    master,
):
    head_count = lax.axis_size("head")
    seq_size = lax.axis_size("seq")
    head_index = lax.axis_index("head")
    group_index = lax.axis_index("seq")
    tok_count = hidden_in.shape[0]
    width = hidden_in.shape[1]
    panel_width = w_query.shape[1]
    ff_width = w_up.shape[1]
    seq_count = lengths.shape[0]
    heads = panel_width // HDIM
    parts = seq_size // heads
    runs = token_order.shape[0] // RUN
    aligned = seq_count == 2
    tile = 1024 if aligned else RUN
    setup = (parts, tile, seq_count, aligned, runs)
    tables = stream_tables(
        token_order, lengths, head_count, seq_size, parts, tile, group_index % parts
    )
    own_block = head_index * seq_size + group_index
    order_here = lax.dynamic_slice_in_dim(token_order, own_block * tok_count, tok_count, 0)
    valid_here = order_here < tables[3][seq_count - 1]
    inputs_f32 = hidden_in.astype(jnp.float32)

    qkv_panel = lax.all_gather(
        jnp.concatenate([w_query, w_key, w_value], axis=1), "seq", axis=0, tiled=True
    )
    inputs_grp = group_rows(hidden_in)
    o_panel = lax.all_gather(w_out, "seq", axis=1, tiled=True)
    up_panel = lax.all_gather(w_up, "seq", axis=0, tiled=True)
    down_panel = lax.all_gather(w_down, "seq", axis=1, tiled=True)

    def own_columns(row):
        return lax.dynamic_slice_in_dim(row, head_index * panel_width, panel_width, 0)

    qkv_bias = jnp.concatenate(
        [own_columns(biases[0]), jnp.zeros((panel_width,), jnp.float32), own_columns(biases[1])]
    )
    qkv_grp = (
        jnp.dot(inputs_grp, qkv_panel, preferred_element_type=jnp.float32) + qkv_bias
    ).astype(jnp.bfloat16)
    qkv_head = spread(qkv_grp, 3, heads, parts, seq_size, 0).reshape(3, runs, RUN, HDIM)
    attended_part, attended_exact, log_total = attend_forward(qkv_head, tables, setup)
    rows_grp = head_count * tok_count
    attended_grp = collect(
        attended_part.reshape(1, seq_size, rows_grp, HDIM), heads, parts, 1
    )
    branch_out = group_sums(jnp.dot(attended_grp, o_panel, preferred_element_type=jnp.float32))
    z_one = inputs_f32 + branch_out + biases[2]
    h_one, normed_one, recip_one = normalize(z_one, gains[0], biases[3])
    h_low = h_one.astype(jnp.bfloat16)
    h_grp, act, pre_act, ff_out = feed(
        h_low, up_panel, down_panel, up_bias.reshape(1, ff_width), True, head_count, 5
    )
    z_two = h_one + ff_out + biases[4]
    layer_f32, normed_two, recip_two = normalize(z_two, gains[1], biases[5])
    layer_out = layer_f32.astype(jnp.bfloat16)
    grad_y = cotangent.astype(jnp.float32) * valid_here[:, None].astype(jnp.float32)
    dz_two, dgain_two, dshift_two = normalize_back(grad_y, normed_two, recip_two, gains[1])
    dbias_down = jnp.sum(dz_two, axis=0)
    dz_two_grp, dpre, dh_part = feed(
        dz_two.astype(jnp.bfloat16), up_panel, down_panel, pre_act, False, head_count, 6
    )
    h_grp, act, dz_two_grp, dpre = (
        array.reshape(rows_grp, array.shape[2]) for array in (h_grp, act, dz_two_grp, dpre)
    )
    up_bias_part = jnp.sum(dpre.astype(jnp.float32), axis=0)
    dh_one = dz_two + dh_part
    dz_one, dgain_one, dshift_one = normalize_back(dh_one, normed_one, recip_one, gains[0])
    dbias_out = jnp.sum(dz_one, axis=0)
    dz_one_grp = group_rows(dz_one.astype(jnp.bfloat16))
    dattended = jnp.dot(dz_one_grp, o_panel.T, preferred_element_type=jnp.float32).astype(
        jnp.bfloat16
    )
    dattended_head = spread(dattended, 1, heads, parts, seq_size, 2).reshape(runs, RUN, HDIM)
    dqkv_part = attend_backward(
        qkv_head, dattended_head, attended_exact, log_total, tables, setup
    )
    dqkv_grp = collect(dqkv_part.reshape(3, seq_size, rows_grp, HDIM), heads, parts, 3)
    input_grad = dz_one + group_sums(
        jnp.dot(dqkv_grp, qkv_panel.T, preferred_element_type=jnp.float32)
    )
    bias_qkv = jnp.sum(dqkv_grp.astype(jnp.float32), axis=0)
    zero_width = jnp.zeros((width,), jnp.float32)
    dbias_query = lax.dynamic_update_slice_in_dim(
        zero_width, bias_qkv[:panel_width], head_index * panel_width, 0
    )
    dbias_value = lax.dynamic_update_slice_in_dim(
        zero_width, bias_qkv[2 * panel_width :], head_index * panel_width, 0
    )
    local_vectors = jnp.stack(
        (
            dbias_query,
            dbias_value,
            dbias_out,
            dshift_one,
            dbias_down,
            dshift_two,
            dgain_one,
            dgain_two,
        )
    )
    up_bias_grad = jnp.sum(lax.all_gather(up_bias_part, "seq"), axis=0)
    vector_grad = jnp.sum(lax.all_gather(local_vectors, ("head", "seq")), axis=0)
    left_index, right_index = block_operands(own_map[0], width, panel_width, ff_width)
    low_grads = owned_grads(
        left_index,
        right_index,
        (inputs_grp, attended_grp, h_grp, act),
        (dqkv_grp, dz_one_grp, dpre, dz_two_grp),
        seq_size,
        4,
    )
    block_grads = low_grads.astype(jnp.float32)
    stat_left_new = 0.5 * stat_left + 0.5 * jnp.einsum(
        "bij,bkj->bik", low_grads, low_grads, preferred_element_type=jnp.float32
    )
    stat_right_new = 0.5 * stat_right + 0.5 * jnp.einsum(
        "bji,bjk->bik", low_grads, low_grads, preferred_element_type=jnp.float32
    )
    left_mix = jnp.einsum("bij,bjk->bik", root_left, block_grads, precision=lax.Precision.HIGHEST)
    direction = jnp.einsum("bij,bjk->bik", left_mix, root_right, precision=lax.Precision.HIGHEST)
    master_new = master - SHAMPOO_RATE * direction
    step_float = step_count[0].astype(jnp.float32)
    vector_params = jnp.concatenate([biases, gains], axis=0)
    vector_new, vector_moment_new, vector_second_new = adam_step(
        vector_params, vector_grad, vector_moment, vector_second, step_float
    )
    up_bias_new, bias_moment_new, bias_second_new = adam_step(
        up_bias, up_bias_grad, bias_moment, bias_second, step_float
    )
    return (
        layer_out,
        input_grad,
        block_grads,
        stat_left_new,
        stat_right_new,
        master_new,
        vector_new[0:6],
        vector_new[6:8],
        up_bias_new,
        vector_grad,
        vector_moment_new,
        vector_second_new,
        up_bias_grad,
        bias_moment_new,
        bias_second_new,
    )


def solution(mesh):
    rows = P(("head", "seq"), None)
    blocks = P(("head", "seq"), None, None)
    in_specs = (
        rows,
        rows,
        P(),
        P(),
        P("head", None),
        P("seq", "head"),
        P("seq", "head"),
        P("seq", "head"),
        P("head", "seq"),
        P("seq", "head"),
        P("head", "seq"),
        P(),
        P(),
        P("head"),
        P(),
        P(),
        P("head"),
        P("head"),
        P(),
        blocks,
        blocks,
        blocks,
        blocks,
        blocks,
    )
    out_specs = (
        rows,
        rows,
        blocks,
        blocks,
        blocks,
        blocks,
        P(),
        P(),
        P("head"),
        P(),
        P(),
        P(),
        P("head"),
        P("head"),
        P("head"),
    )
    return jax.shard_map(shards, mesh=mesh, in_specs=in_specs, out_specs=out_specs, check_vma=False)
```

```python
import functools
import math

import jax
import jax.numpy as jnp
from jax import lax
from jax.experimental import pallas as pl
from jax.experimental.pallas import tpu as pltpu
from jax.sharding import PartitionSpec as P


HDIM = 128
BLOCK = 256
RUN = 256

NEG_LARGE = -1e30
NORM_EPS = 1e-12
ADAM_RATE = 0.4
SHAMPOO_RATE = 0.15
MESH = pl.DeviceIdType.MESH
VMEM_MOST = 60 * 1024 * 1024

ANY = pl.BlockSpec(memory_space=pl.ANY)
IN_SMEM = pl.BlockSpec(memory_space=pltpu.SMEM)
IN_VMEM = pl.BlockSpec(memory_space=pltpu.VMEM)


def busy(microseconds):
    return pl.CostEstimate(
        flops=microseconds * 800_000_000, bytes_accessed=1_000_000, transcendentals=0
    )


def seq_barrier(me, heads, parts):
    own_head, own_part = me // parts, me % parts
    barrier = pltpu.get_barrier_semaphore()
    for step in range(1, heads):
        pl.semaphore_signal(
            barrier,
            inc=1,
            device_id={"seq": (own_head + step) % heads * parts + own_part},
            device_id_type=MESH,
        )
    for step in range(1, parts):
        pl.semaphore_signal(
            barrier,
            inc=1,
            device_id={"seq": own_head * parts + (own_part + step) % parts},
            device_id_type=MESH,
        )
    pl.semaphore_wait(barrier, heads - 1 + parts - 1)


def spread_kernel(
    fields, heads, parts, x_ref, y_ref, own_sem, send_sem, recv_sem, pass_sem, take_sem
):
    me = lax.axis_index("seq")
    own_head, own_part = me // parts, me % parts
    seq_barrier(me, heads, parts)

    def columns(field, head):
        return pl.ds(pl.multiple_of((field * heads + head) * HDIM, HDIM), HDIM)

    sends = []
    for step in range(1, heads):
        head = (own_head + step) % heads
        for field in range(fields):
            copy = pltpu.make_async_remote_copy(
                src_ref=x_ref.at[:, columns(field, head)],
                dst_ref=y_ref.at[field, me],
                send_sem=send_sem.at[step - 1, field],
                recv_sem=recv_sem.at[step - 1, field],
                device_id={"seq": head * parts + own_part},
                device_id_type=MESH,
            )
            copy.start()
            sends.append(copy)
    owns = []
    for field in range(fields):
        copy = pltpu.make_async_copy(
            x_ref.at[:, columns(field, own_head)], y_ref.at[field, me], own_sem.at[field]
        )
        copy.start()
        owns.append(copy)
    passes = []

    def pass_on(step, field, source):
        origin = (own_head - step + heads) % heads * parts + own_part
        for other in range(1, parts):
            copy = pltpu.make_async_remote_copy(
                src_ref=source,
                dst_ref=y_ref.at[field, origin],
                send_sem=pass_sem.at[other - 1, step, field],
                recv_sem=take_sem.at[other - 1, step, field],
                device_id={"seq": own_head * parts + (own_part + other) % parts},
                device_id_type=MESH,
            )
            copy.start()
            passes.append(copy)

    for field in range(fields):
        pass_on(0, field, x_ref.at[:, columns(field, own_head)])
    for step in range(1, heads):
        origin = (own_head - step + heads) % heads * parts + own_part
        for field in range(fields):
            sends[(step - 1) * fields + field].wait_recv()
            pass_on(step, field, y_ref.at[field, origin])
    for copy in owns:
        copy.wait()
    for copy in sends:
        copy.wait_send()
    for copy in passes:
        copy.wait()


def spread(x_rows, fields, heads, parts, seq_size, collective_id):
    rows = x_rows.shape[0]
    return pl.pallas_call(
        functools.partial(spread_kernel, fields, heads, parts),
        out_shape=jax.ShapeDtypeStruct((fields, seq_size, rows, HDIM), x_rows.dtype),
        in_specs=[IN_VMEM],
        out_specs=ANY,
        scratch_shapes=[
            pltpu.SemaphoreType.DMA((fields,)),
            pltpu.SemaphoreType.DMA((max(heads - 1, 1), fields)),
            pltpu.SemaphoreType.DMA((max(heads - 1, 1), fields)),
            pltpu.SemaphoreType.DMA((max(parts - 1, 1), heads, fields)),
            pltpu.SemaphoreType.DMA((max(parts - 1, 1), heads, fields)),
        ],
        compiler_params=pltpu.CompilerParams(
            collective_id=collective_id, has_side_effects=True, vmem_limit_bytes=24 * 1024 * 1024
        ),
        cost_estimate=busy(fields * 24),
        name="spread",
    )(x_rows)


def collect_kernel(
    fields,
    heads,
    parts,
    x_ref,
    y_ref,
    own,
    got,
    ready,
    own_sem,
    pass_sem,
    take_sem,
    send_sem,
    recv_sem,
    keep_sem,
):
    me = lax.axis_index("seq")
    own_head, own_part = me // parts, me % parts
    seq_barrier(me, heads, parts)
    order = list(range(1, heads)) + [0]

    def home(step, part):
        return (own_head + step) % heads * parts + part

    passes, owns = {}, {}
    for step in order:
        for field in range(fields):
            for other in range(1, parts):
                part = (own_part + other) % parts
                copy = pltpu.make_async_remote_copy(
                    src_ref=x_ref.at[field, home(step, part)],
                    dst_ref=got.at[other - 1, step, field],
                    send_sem=pass_sem.at[other - 1, step, field],
                    recv_sem=take_sem.at[other - 1, step, field],
                    device_id={"seq": own_head * parts + part},
                    device_id_type=MESH,
                )
                copy.start()
                passes[step, field, other] = copy
            copy = pltpu.make_async_copy(
                x_ref.at[field, home(step, own_part)], own.at[step, field], own_sem.at[step, field]
            )
            copy.start()
            owns[step, field] = copy

    sends = []
    for step in order:
        for field in range(fields):
            owns[step, field].wait()
            for other in range(1, parts):
                passes[step, field, other].wait_recv()
            total = own[step, field].astype(jnp.float32)
            for other in range(1, parts):
                total = total + got[other - 1, step, field].astype(jnp.float32)
            ready[step, field] = total.astype(ready.dtype)
            columns = pl.ds(pl.multiple_of((field * heads + own_head) * HDIM, HDIM), HDIM)
            if step == 0:
                copy = pltpu.make_async_copy(
                    ready.at[step, field], y_ref.at[:, columns], keep_sem.at[field]
                )
            else:
                copy = pltpu.make_async_remote_copy(
                    src_ref=ready.at[step, field],
                    dst_ref=y_ref.at[:, columns],
                    send_sem=send_sem.at[step - 1, field],
                    recv_sem=recv_sem.at[step - 1, field],
                    device_id={"seq": home(step, own_part)},
                    device_id_type=MESH,
                )
            copy.start()
            sends.append(copy)
    for copy in sends:
        copy.wait()
    for copy in passes.values():
        copy.wait_send()


def collect(x_parts, heads, parts, collective_id):
    fields, _, rows, _ = x_parts.shape
    kind = x_parts.dtype
    few = max(parts - 1, 1)
    return pl.pallas_call(
        functools.partial(collect_kernel, fields, heads, parts),
        out_shape=jax.ShapeDtypeStruct((rows, fields * heads * HDIM), kind),
        in_specs=[ANY],
        out_specs=ANY,
        scratch_shapes=[
            pltpu.VMEM((heads, fields, rows, HDIM), kind),
            pltpu.VMEM((few, heads, fields, rows, HDIM), kind),
            pltpu.VMEM((heads, fields, rows, HDIM), kind),
            pltpu.SemaphoreType.DMA((heads, fields)),
            pltpu.SemaphoreType.DMA((few, heads, fields)),
            pltpu.SemaphoreType.DMA((few, heads, fields)),
            pltpu.SemaphoreType.DMA((max(heads - 1, 1), fields)),
            pltpu.SemaphoreType.DMA((max(heads - 1, 1), fields)),
            pltpu.SemaphoreType.DMA((fields,)),
        ],
        compiler_params=pltpu.CompilerParams(
            collective_id=collective_id, has_side_effects=True, vmem_limit_bytes=VMEM_MOST
        ),
        cost_estimate=busy(fields * 24),
        name="collect",
    )(x_parts)


def allowed_tile(ends_ref, seq_count, key_low, query_low, shape):
    key_pos = key_low + lax.broadcasted_iota(jnp.int32, shape, 0)
    query_pos = query_low + lax.broadcasted_iota(jnp.int32, shape, 1)
    key_seg = jnp.zeros(shape, jnp.int32)
    query_seg = jnp.zeros(shape, jnp.int32)
    for index in range(seq_count):
        key_seg += (key_pos >= ends_ref[index]).astype(jnp.int32)
        query_seg += (query_pos >= ends_ref[index]).astype(jnp.int32)
    last = ends_ref[seq_count - 1]
    key_seg = jnp.where(key_pos < last, key_seg, seq_count + key_pos)
    query_seg = jnp.where(query_pos < last, query_seg, seq_count + query_pos)
    return key_seg == query_seg


def nt(left, right):
    return lax.dot_general(
        left, right, (((1,), (1,)), ((), ())), preferred_element_type=jnp.float32
    )


def nn(left, right):
    return lax.dot_general(
        left, right, (((1,), (0,)), ((), ())), preferred_element_type=jnp.float32
    )


def forward_kernel(
    setup,
    where_ref,
    low_ref,
    high_ref,
    ends_ref,
    part_ref,
    qkv_ref,
    out_ref,
    exact_ref,
    log_ref,
    q_buf,
    k_buf,
    v_buf,
    vt_buf,
    sem,
):
    parts, tile, seq_count, aligned, runs = setup
    turn = pl.program_id(0)
    part = part_ref[0]
    scale2 = math.log2(math.e) / math.sqrt(HDIM)

    @pl.when(turn == 0)
    def _():
        def fetch(field, run, buf, slot):
            return pltpu.make_async_copy(
                qkv_ref.at[field, where_ref[run]],
                buf.at[pl.ds(pl.multiple_of(slot * RUN, RUN), RUN), :],
                sem.at[field],
            )

        def start(run, carry):
            fetch(1, run, k_buf, run).start()
            fetch(2, run, v_buf, run).start()
            return carry

        def start_own(index, carry):
            fetch(0, index * parts + part, q_buf, index).start()
            return carry

        def finish(run, carry):
            fetch(1, run, k_buf, run).wait()
            fetch(2, run, v_buf, run).wait()
            return carry

        def finish_own(index, carry):
            fetch(0, index * parts + part, q_buf, index).wait()
            return carry

        lax.fori_loop(0, runs, start, 0)
        lax.fori_loop(0, runs // parts, start_own, 0)
        out_ref[...] = jnp.zeros_like(out_ref)
        lax.fori_loop(0, runs, finish, 0)
        lax.fori_loop(0, runs // parts, finish_own, 0)
        if aligned:

            def turn_tile(index, carry):
                low = pl.multiple_of(index * RUN, RUN)
                vt_buf[:, pl.ds(low, RUN)] = v_buf[pl.ds(low, RUN), :].T
                return carry

            lax.fori_loop(0, runs, turn_tile, 0)

    run = turn * parts + part
    place = where_ref[run]
    queries = q_buf[pl.ds(pl.multiple_of(turn * RUN, RUN), RUN), :]

    def attend():
        def key_step(index, carry):
            top, total, acc = carry
            low = pl.multiple_of(index * tile, tile)
            scores = nt(k_buf[pl.ds(low, tile), :], queries)
            if not aligned:
                allowed = allowed_tile(ends_ref, seq_count, low, run * RUN, scores.shape)
                scores = jnp.where(allowed, scores, NEG_LARGE)
            new_top = jnp.maximum(top, jnp.max(scores, axis=0, keepdims=True))
            prob = jnp.exp2((scores - new_top) * scale2)
            if not aligned:
                prob = jnp.where(allowed, prob, 0.0)
            fade = jnp.exp2((top - new_top) * scale2)
            total = total * fade + jnp.sum(prob, axis=0, keepdims=True)
            if aligned:
                turned = vt_buf[:, pl.ds(low, tile)]
            else:
                turned = v_buf[pl.ds(low, tile), :].T
            acc = acc * fade + nn(turned, prob.astype(jnp.bfloat16))
            return new_top, total, acc

        top, total, acc = lax.fori_loop(
            low_ref[run],
            high_ref[run],
            key_step,
            (
                jnp.full((1, RUN), NEG_LARGE, jnp.float32),
                jnp.zeros((1, RUN), jnp.float32),
                jnp.zeros((HDIM, RUN), jnp.float32),
            ),
        )
        result = (acc / total).T
        exact_ref[0] = result
        out_ref[place] = result.astype(out_ref.dtype)
        log_ref[0] = top * scale2 + jnp.log2(total)

    if aligned:
        is_valid = run * RUN < ends_ref[seq_count - 1]
        pl.when(is_valid)(attend)

        @pl.when(jnp.logical_not(is_valid))
        def _():
            values = v_buf[pl.ds(pl.multiple_of(run * RUN, RUN), RUN), :]
            exact_ref[0] = values.astype(jnp.float32)
            out_ref[place] = values
            log_ref[0] = jnp.zeros((1, RUN), jnp.float32)
    else:
        attend()


def attend_forward(qkv, tables, setup):
    parts, _, _, aligned, runs = setup
    own = runs // parts
    rows = runs * RUN
    return pl.pallas_call(
        functools.partial(forward_kernel, setup),
        grid=(own,),
        out_shape=(
            jax.ShapeDtypeStruct((runs, RUN, HDIM), jnp.bfloat16),
            jax.ShapeDtypeStruct((own, RUN, HDIM), jnp.float32),
            jax.ShapeDtypeStruct((own, 1, RUN), jnp.float32),
        ),
        in_specs=[IN_SMEM] * 5 + [ANY],
        out_specs=(
            pl.BlockSpec((runs, RUN, HDIM), lambda i: (0, 0, 0), pipeline_mode=pl.Buffered(1)),
            pl.BlockSpec((1, RUN, HDIM), lambda i: (i, 0, 0)),
            pl.BlockSpec((1, 1, RUN), lambda i: (i, 0, 0)),
        ),
        scratch_shapes=[
            pltpu.VMEM((own * RUN, HDIM), jnp.bfloat16),
            pltpu.VMEM((rows, HDIM), jnp.bfloat16),
            pltpu.VMEM((rows, HDIM), jnp.bfloat16),
            pltpu.VMEM((HDIM, rows if aligned else RUN), jnp.bfloat16),
            pltpu.SemaphoreType.DMA((3,)),
        ],
        compiler_params=pltpu.CompilerParams(
            dimension_semantics=("arbitrary",), vmem_limit_bytes=VMEM_MOST
        ),
        cost_estimate=busy(36),
        name="attend_forward",
    )(*tables, qkv)


def backward_kernel(
    setup,
    where_ref,
    low_ref,
    high_ref,
    ends_ref,
    part_ref,
    qkv_ref,
    grad_ref,
    exact_ref,
    log_ref,
    out_ref,
    q_buf,
    k_buf,
    v_buf,
    kt_buf,
    g_buf,
    dk_acc,
    dv_acc,
    stage,
    sem,
    out_sem,
):
    parts, tile, seq_count, aligned, runs = setup
    own = runs // parts
    turn = pl.program_id(0)
    part = part_ref[0]
    scale = 1.0 / math.sqrt(HDIM)
    scale2 = math.log2(math.e) * scale

    @pl.when(turn == 0)
    def _():
        def fetch(source, index, buf, slot, lane):
            return pltpu.make_async_copy(
                source.at[index],
                buf.at[pl.ds(pl.multiple_of(slot * RUN, RUN), RUN), :],
                sem.at[lane],
            )

        def pair(run):
            place = where_ref[run]
            return (
                fetch(qkv_ref.at[1], place, k_buf, run, 1),
                fetch(qkv_ref.at[2], place, v_buf, run, 2),
            )

        def own_pair(index):
            place = where_ref[index * parts + part]
            return (
                fetch(qkv_ref.at[0], place, q_buf, index, 0),
                fetch(grad_ref, place, g_buf, index, 3),
            )

        def start(run, carry):
            for copy in pair(run):
                copy.start()
            return carry

        def start_own(index, carry):
            for copy in own_pair(index):
                copy.start()
            return carry

        def finish(run, carry):
            for copy in pair(run):
                copy.wait()
            return carry

        def finish_own(index, carry):
            for copy in own_pair(index):
                copy.wait()
            return carry

        lax.fori_loop(0, runs, start, 0)
        lax.fori_loop(0, own, start_own, 0)
        dk_acc[...] = jnp.zeros_like(dk_acc)
        dv_acc[...] = jnp.zeros_like(dv_acc)
        lax.fori_loop(0, runs, finish, 0)
        lax.fori_loop(0, own, finish_own, 0)
        if aligned:

            def turn_tile(index, carry):
                low = pl.multiple_of(index * RUN, RUN)
                kt_buf[:, pl.ds(low, RUN)] = k_buf[pl.ds(low, RUN), :].T
                return carry

            lax.fori_loop(0, runs, turn_tile, 0)

    run = turn * parts + part
    low_row = pl.multiple_of(turn * RUN, RUN)

    def attend():
        queries = q_buf[pl.ds(low_row, RUN), :]
        grads = g_buf[pl.ds(low_row, RUN), :]
        delta = jnp.sum((grads.astype(jnp.float32) * exact_ref[0]).T, axis=0, keepdims=True)
        log_total = log_ref[0]

        def key_step(index, acc):
            low = pl.multiple_of(index * tile, tile)
            keys = k_buf[pl.ds(low, tile), :]
            values = v_buf[pl.ds(low, tile), :]
            scores = nt(keys, queries)
            prob = jnp.exp2(scores * scale2 - log_total)
            if not aligned:
                allowed = allowed_tile(ends_ref, seq_count, low, run * RUN, scores.shape)
                prob = jnp.where(allowed, prob, 0.0)
            prob_grad = nt(values, grads)
            dv_acc[pl.ds(low, tile), :] += nn(prob.astype(jnp.bfloat16), grads)
            score_grad = (prob * (prob_grad - delta)).astype(jnp.bfloat16)
            dk_acc[pl.ds(low, tile), :] += nn(score_grad, queries)
            turned = kt_buf[:, pl.ds(low, tile)] if aligned else keys.T
            return acc + nn(turned, score_grad)

        acc = lax.fori_loop(
            low_ref[run], high_ref[run], key_step, jnp.zeros((HDIM, RUN), jnp.float32)
        )
        q_buf[pl.ds(low_row, RUN), :] = (acc.T * scale).astype(jnp.bfloat16)

    if aligned:
        is_valid = run * RUN < ends_ref[seq_count - 1]
        pl.when(is_valid)(attend)

        @pl.when(jnp.logical_not(is_valid))
        def _():
            q_buf[pl.ds(low_row, RUN), :] = jnp.zeros((RUN, HDIM), jnp.bfloat16)
    else:
        attend()

    @pl.when(turn == own - 1)
    def _():
        def key_copies(run_index, slot):
            place = where_ref[run_index]
            return (
                pltpu.make_async_copy(stage.at[slot, 0], out_ref.at[1, place], out_sem.at[slot, 0]),
                pltpu.make_async_copy(stage.at[slot, 1], out_ref.at[2, place], out_sem.at[slot, 1]),
            )

        v_buf[pl.ds(0, RUN), :] = jnp.zeros((RUN, HDIM), jnp.bfloat16)

        def query_copy(run_index):
            mine = run_index % parts == part
            place = where_ref[run_index]
            index = jnp.where(mine, run_index // parts, 0)
            return mine, (
                pltpu.make_async_copy(
                    q_buf.at[pl.ds(pl.multiple_of(index * RUN, RUN), RUN), :],
                    out_ref.at[0, place],
                    sem.at[0],
                ),
                pltpu.make_async_copy(
                    v_buf.at[pl.ds(0, RUN), :], out_ref.at[0, place], sem.at[0]
                ),
            )

        def start_query(run_index, carry):
            mine, (copy, blank) = query_copy(run_index)
            pl.when(mine)(copy.start)
            pl.when(jnp.logical_not(mine))(blank.start)
            return carry

        def finish_query(run_index, carry):
            _, (copy, blank) = query_copy(run_index)
            blank.wait()
            return carry

        lax.fori_loop(0, runs, start_query, 0)

        def write(run_index, carry):
            slot = run_index % 2

            @pl.when(run_index >= 2)
            def _():
                for copy in key_copies(run_index - 2, slot):
                    copy.wait()

            low = pl.multiple_of(run_index * RUN, RUN)
            stage[slot, 0] = (dk_acc[pl.ds(low, RUN), :] * scale).astype(jnp.bfloat16)
            stage[slot, 1] = dv_acc[pl.ds(low, RUN), :].astype(jnp.bfloat16)
            for copy in key_copies(run_index, slot):
                copy.start()
            return carry

        lax.fori_loop(0, runs, write, 0)
        for back in (2, 1):
            for copy in key_copies(runs - back, (runs - back) % 2):
                copy.wait()
        lax.fori_loop(0, runs, finish_query, 0)


def attend_backward(qkv, grads, exact, log_total, tables, setup):
    parts, _, _, aligned, runs = setup
    own = runs // parts
    rows = runs * RUN
    return pl.pallas_call(
        functools.partial(backward_kernel, setup),
        grid=(own,),
        out_shape=jax.ShapeDtypeStruct((3, runs, RUN, HDIM), jnp.bfloat16),
        in_specs=[IN_SMEM] * 5
        + [
            ANY,
            ANY,
            pl.BlockSpec((1, RUN, HDIM), lambda i: (i, 0, 0)),
            pl.BlockSpec((1, 1, RUN), lambda i: (i, 0, 0)),
        ],
        out_specs=ANY,
        scratch_shapes=[
            pltpu.VMEM((own * RUN, HDIM), jnp.bfloat16),
            pltpu.VMEM((rows, HDIM), jnp.bfloat16),
            pltpu.VMEM((rows, HDIM), jnp.bfloat16),
            pltpu.VMEM((HDIM, rows if aligned else RUN), jnp.bfloat16),
            pltpu.VMEM((own * RUN, HDIM), jnp.bfloat16),
            pltpu.VMEM((rows, HDIM), jnp.float32),
            pltpu.VMEM((rows, HDIM), jnp.float32),
            pltpu.VMEM((2, 2, RUN, HDIM), jnp.bfloat16),
            pltpu.SemaphoreType.DMA((4,)),
            pltpu.SemaphoreType.DMA((2, 2)),
        ],
        compiler_params=pltpu.CompilerParams(
            dimension_semantics=("arbitrary",), vmem_limit_bytes=VMEM_MOST
        ),
        cost_estimate=busy(50),
        name="attend_backward",
    )(*tables, qkv, grads, exact, log_total)


def stream_tables(token_order, lengths, head_count, seq_size, tile, part):
    runs = token_order.shape[0] // RUN
    stream = (token_order.reshape(head_count, seq_size, RUN)[:, :, 0] // RUN).T.reshape(-1)
    places = jnp.arange(runs, dtype=jnp.int32)
    where = jnp.sum(jnp.where(stream[None, :] == places[:, None], places[None, :], 0), axis=1)
    ends = jnp.cumsum(lengths)
    starts = ends - lengths
    first = places * RUN
    last = first + RUN - 1

    def bound(position, of_seq, of_pad):
        inside = (position[:, None] >= starts[None, :]) & (position[:, None] < ends[None, :])
        found = jnp.sum(jnp.where(inside, of_seq[None, :], 0), axis=1)
        return jnp.where(position < ends[-1], found, of_pad)

    low = bound(first, starts, first) // tile
    high = (bound(last, ends, last + 1) + tile - 1) // tile
    return (
        where.astype(jnp.int32),
        low.astype(jnp.int32),
        high.astype(jnp.int32),
        ends.astype(jnp.int32),
        part.reshape(1).astype(jnp.int32),
    )


PAIR = 2
DEPTH = 6
LAG = 2


def grads_kernel(spec, left_ref, right_ref, *refs):
    chips, slots, left_strips, right_strips = spec
    lefts, refs = refs[: len(left_strips)], refs[len(left_strips) :]
    rights, refs = refs[: len(right_strips)], refs[len(right_strips) :]
    (
        out_ref,
        left_buf,
        right_buf,
        strip_buf,
        pair_out,
        pair_in,
        line_out,
        line_in,
        last_in,
        own_sum,
        load_sem,
        pair_send,
        pair_recv,
        line_send,
        line_recv,
        last_recv,
        pair_free,
        line_free,
    ) = refs
    me = lax.axis_index("seq")
    chip, core = me // PAIR, me % PAIR
    sibling = chip * PAIR + (1 - core)
    neighbours = ((chip + 1) * PAIR + core, (chip - 1) * PAIR + core)
    has_next = (chip < chips - 1, chip > 0)

    barrier = pltpu.get_barrier_semaphore()
    pl.semaphore_signal(barrier, inc=1, device_id={"seq": sibling}, device_id_type=MESH)
    for way in range(2):

        @pl.when(has_next[way])
        def _():
            pl.semaphore_signal(
                barrier, inc=1, device_id={"seq": neighbours[way]}, device_id_type=MESH
            )

    ends = (chip == 0).astype(jnp.int32) + (chip == chips - 1).astype(jnp.int32)
    pl.semaphore_wait(barrier, 3 - ends)

    def strip(source, index):
        return source.at[:, pl.ds(pl.multiple_of(index * BLOCK, BLOCK), BLOCK)]

    low = 0
    for source, count in zip(rights, right_strips):

        def load_right(index, carry, source=source, low=low):
            pltpu.make_async_copy(
                strip(source, index), right_buf.at[low + index], load_sem.at[2]
            ).start()
            return carry

        lax.fori_loop(0, count, load_right, 0)
        low += count
    rows = left_buf.shape[2]
    low = 0
    for source, count in zip(lefts, left_strips):

        def fetch(index, slot, source=source):
            return pltpu.make_async_copy(strip(source, index), strip_buf.at[slot], load_sem.at[slot])

        def turn_strip(index, carry, count=count, low=low, fetch=fetch):
            slot = index % 2

            @pl.when(index + 1 < count)
            def _():
                fetch(index + 1, 1 - slot).start()

            fetch(index, slot).wait()
            for part in range(rows // BLOCK):
                span = pl.ds(part * BLOCK, BLOCK)
                left_buf[low + index, :, span] = strip_buf[slot, span, :].T
            return carry

        fetch(0, 0).start()
        lax.fori_loop(0, count, turn_strip, 0)
        low += count
    low = 0
    for source, count in zip(rights, right_strips):

        def wait_right(index, carry, source=source, low=low):
            pltpu.make_async_copy(
                strip(source, index), right_buf.at[low + index], load_sem.at[2]
            ).wait()
            return carry

        lax.fori_loop(0, count, wait_right, 0)
        low += count

    def product(owner_chip, owner_core, k):
        slot = (owner_chip * PAIR + owner_core) * slots + k
        return nn(left_buf[left_ref[slot]], right_buf[right_ref[slot]])

    counts = ((chips - 1 - chip) * slots, chip * slots, slots)

    def owner(stream, step):
        if stream == 0:
            return chips - 1 - step // slots
        if stream == 1:
            return step // slots
        return chip

    def pair_copy(stream, step):
        slot = step % DEPTH
        return pltpu.make_async_remote_copy(
            src_ref=pair_out.at[stream, slot],
            dst_ref=pair_in.at[stream, slot],
            send_sem=pair_send.at[stream, slot],
            recv_sem=pair_recv.at[stream, slot],
            device_id={"seq": sibling},
            device_id_type=MESH,
        )

    def line_copy(stream, step):
        slot = step % DEPTH
        return pltpu.make_async_remote_copy(
            src_ref=line_out.at[stream, slot],
            dst_ref=line_in.at[stream, slot],
            send_sem=line_send.at[stream, slot],
            recv_sem=line_recv.at[stream, slot],
            device_id={"seq": neighbours[stream]},
            device_id_type=MESH,
        )

    def last_copy(stream, step):
        slot, k = step % DEPTH, step % slots
        return pltpu.make_async_remote_copy(
            src_ref=line_out.at[stream, slot],
            dst_ref=last_in.at[stream, k],
            send_sem=line_send.at[stream, slot],
            recv_sem=last_recv.at[stream, k],
            device_id={"seq": neighbours[stream]},
            device_id_type=MESH,
        )

    def give(stream, step):
        slot = step % DEPTH

        @pl.when(step >= DEPTH)
        def _():
            pair_copy(stream, step).wait_send()
            pl.semaphore_wait(pair_free.at[stream], 1)

        pair_out[stream, slot] = product(owner(stream, step), 1 - core, step % slots).astype(
            jnp.bfloat16
        )
        pair_copy(stream, step).start()

    def take(stream, step):
        slot = step % DEPTH
        total = product(owner(stream, step), core, step % slots)
        pair_copy(stream, step).wait_recv()
        total = total + pair_in[stream, slot].astype(jnp.float32)

        @pl.when(step + DEPTH < counts[stream])
        def _():
            pl.semaphore_signal(
                pair_free.at[stream], inc=1, device_id={"seq": sibling}, device_id_type=MESH
            )

        return total

    def forward(stream, step):
        slot = step % DEPTH
        target = chip + 1 if stream == 0 else chip - 1
        ends_there = owner(stream, step) == target
        has_source = has_next[1 - stream]
        total = take(stream, step)

        @pl.when(step >= DEPTH)
        def _():
            line_copy(stream, step).wait_send()

        @pl.when(has_source)
        def _():
            line_copy(stream, step).wait_recv()
            line_out[stream, slot] = (total + line_in[stream, slot].astype(jnp.float32)).astype(
                jnp.bfloat16
            )

            @pl.when(step + DEPTH < counts[stream])
            def _():
                pl.semaphore_signal(
                    line_free.at[stream],
                    inc=1,
                    device_id={"seq": neighbours[1 - stream]},
                    device_id_type=MESH,
                )

        @pl.when(jnp.logical_not(has_source))
        def _():
            line_out[stream, slot] = total.astype(jnp.bfloat16)

        @pl.when(ends_there)
        def _():
            last_copy(stream, step).start()

        @pl.when(jnp.logical_not(ends_there))
        def _():
            @pl.when(step >= DEPTH)
            def _():
                pl.semaphore_wait(line_free.at[stream], 1)

            line_copy(stream, step).start()

    def keep(step):
        own_sum[step] = take(2, step).astype(jnp.bfloat16)

    for stream in range(2):
        pl.when(counts[stream] > 0)(functools.partial(give, stream, 0))
    give(2, 0)

    delays = (chip * LAG, (chips - 1 - chip) * LAG, slots)

    def body(turn, carry):
        for stream in range(3):
            step = turn - delays[stream] + 1

            @pl.when((step > 0) & (step < counts[stream]))
            def _():
                give(stream, step)

        for stream in range(3):
            step = turn - delays[stream]

            @pl.when((step >= 0) & (step < counts[stream]))
            def _():
                if stream < 2:
                    forward(stream, step)
                else:
                    keep(step)

        return carry

    lax.fori_loop(0, (chips - 1) * slots + (chips - 1) * LAG, body, 0)

    def finish(k, carry):
        out_ref[k] = own_sum[k]
        for stream in range(2):

            @pl.when(has_next[1 - stream])
            def _():
                last_copy(stream, k).wait_recv()
                out_ref[k] = (
                    out_ref[k].astype(jnp.float32) + last_in[stream, k].astype(jnp.float32)
                ).astype(jnp.bfloat16)

        return carry

    lax.fori_loop(0, slots, finish, 0)
    for slot in range(DEPTH):
        for stream in range(2):

            @pl.when(counts[stream] > 0)
            def _():
                line_copy(stream, slot).wait_send()
                pair_copy(stream, slot).wait_send()

        pair_copy(2, slot).wait_send()


def owned_grads(left_index, right_index, lefts, rights, seq_size, collective_id):
    rows = lefts[0].shape[0]
    left_strips = tuple(array.shape[1] // BLOCK for array in lefts)
    right_strips = tuple(array.shape[1] // BLOCK for array in rights)
    chips = seq_size // PAIR
    slots = left_index.shape[0] // seq_size
    kind = jnp.bfloat16
    block = (BLOCK, BLOCK)
    return pl.pallas_call(
        functools.partial(grads_kernel, (chips, slots, left_strips, right_strips)),
        out_shape=jax.ShapeDtypeStruct((slots,) + block, kind),
        in_specs=[IN_SMEM] * 2 + [ANY] * (len(lefts) + len(rights)),
        out_specs=IN_VMEM,
        scratch_shapes=[
            pltpu.VMEM((sum(left_strips), BLOCK, rows), kind),
            pltpu.VMEM((sum(right_strips), rows, BLOCK), kind),
            pltpu.VMEM((2, rows, BLOCK), kind),
            pltpu.VMEM((3, DEPTH) + block, kind),
            pltpu.VMEM((3, DEPTH) + block, kind),
            pltpu.VMEM((2, DEPTH) + block, kind),
            pltpu.VMEM((2, DEPTH) + block, kind),
            pltpu.VMEM((2, slots) + block, kind),
            pltpu.VMEM((slots,) + block, kind),
            pltpu.SemaphoreType.DMA((3,)),
            pltpu.SemaphoreType.DMA((3, DEPTH)),
            pltpu.SemaphoreType.DMA((3, DEPTH)),
            pltpu.SemaphoreType.DMA((2, DEPTH)),
            pltpu.SemaphoreType.DMA((2, DEPTH)),
            pltpu.SemaphoreType.DMA((2, slots)),
            pltpu.SemaphoreType.REGULAR((3,)),
            pltpu.SemaphoreType.REGULAR((2,)),
        ],
        compiler_params=pltpu.CompilerParams(
            collective_id=collective_id, has_side_effects=True, vmem_limit_bytes=VMEM_MOST
        ),
        cost_estimate=busy(240),
        name="owned_grads",
    )(left_index, right_index, *lefts, *rights)


def block_operands(own_map, width, panel_width, ff_width):
    deep, narrow, wide = width // BLOCK, panel_width // BLOCK, ff_width // BLOCK
    left = jnp.zeros_like(own_map)
    right = jnp.zeros_like(own_map)
    first, left_low, right_low = 0, 0, 0
    panels = [(deep, narrow, 0, 0), (deep, narrow, 0, narrow), (deep, narrow, 0, 2 * narrow)]
    panels.append((narrow, deep, deep, 3 * narrow))
    panels.append((deep, wide, deep + narrow, 3 * narrow + deep))
    panels.append((wide, deep, 2 * deep + narrow, 3 * narrow + deep + wide))
    for high, broad, left_low, right_low in panels:
        inside = (own_map >= first) & (own_map < first + high * broad)
        within = own_map - first
        left = jnp.where(inside, left_low + within // broad, left)
        right = jnp.where(inside, right_low + within % broad, right)
        first += high * broad
    return left.astype(jnp.int32), right.astype(jnp.int32)


def group_peer(me, count, slot, way):
    far, near = slot // 2, slot % 2
    half = count // 2
    return (me // 2 + way * far + half) % half * 2 + (me % 2 + near) % 2


def group_barrier(me, count):
    barrier = pltpu.get_barrier_semaphore()
    for slot in range(1, count):
        pl.semaphore_signal(
            barrier, inc=1, device_id={"head": group_peer(me, count, slot, 1)}, device_id_type=MESH
        )
    pl.semaphore_wait(barrier, count - 1)


GELU_SCALE = 0.7978845608028654
GELU_CUBIC = 0.044715
WIDE = 512


def gelu(u):
    return 0.5 * u * (1.0 + jnp.tanh(GELU_SCALE * (u + GELU_CUBIC * (u * u * u))))


def gelu_slope(u):
    square = u * u
    bend = jnp.tanh(GELU_SCALE * (u + GELU_CUBIC * (square * u)))
    inner = GELU_SCALE * (1.0 + 3.0 * GELU_CUBIC * square)
    return 0.5 * (1.0 + bend) + 0.5 * u * (1.0 - bend * bend) * inner


def feed_kernel(is_forward, count, x_ref, up_ref, down_ref, side_ref, *refs):
    if is_forward:
        rows_ref, mid_ref, pre_ref, sum_ref = refs[:4]
        refs = refs[4:]
    else:
        rows_ref, mid_ref, sum_ref = refs[:3]
        refs = refs[3:]
    (
        land,
        up_buf,
        down_buf,
        mid_buf,
        pre_buf,
        part_buf,
        got,
        load_sem,
        send_sem,
        recv_sem,
        back_sem,
        got_sem,
        out_sem,
    ) = refs
    me = lax.axis_index("head")
    width, ff_width = up_buf.shape
    loads = [
        pltpu.make_async_copy(up_ref, up_buf, load_sem.at[0]),
        pltpu.make_async_copy(down_ref, down_buf, load_sem.at[1]),
    ]
    if not is_forward:
        loads.append(pltpu.make_async_copy(side_ref, pre_buf, load_sem.at[2]))
    for copy in loads:
        copy.start()
    group_barrier(me, count)

    def push(slot):
        return pltpu.make_async_remote_copy(
            src_ref=x_ref,
            dst_ref=land.at[slot],
            send_sem=send_sem.at[slot],
            recv_sem=recv_sem.at[slot],
            device_id={"head": group_peer(me, count, slot, 1)},
            device_id_type=MESH,
        )

    def give_back(slot):
        return pltpu.make_async_remote_copy(
            src_ref=part_buf.at[slot],
            dst_ref=got.at[slot],
            send_sem=back_sem.at[slot],
            recv_sem=got_sem.at[slot],
            device_id={"head": group_peer(me, count, slot, -1)},
            device_id_type=MESH,
        )

    def outs(slot):
        copies = [
            pltpu.make_async_copy(land.at[slot], rows_ref.at[slot], out_sem.at[0, slot]),
            pltpu.make_async_copy(mid_buf.at[slot], mid_ref.at[slot], out_sem.at[1, slot]),
        ]
        if is_forward:
            copies.append(
                pltpu.make_async_copy(pre_buf.at[slot], pre_ref.at[slot], out_sem.at[2, slot])
            )
        return copies

    for slot in range(1, count):
        push(slot).start()
    land[0] = x_ref[...]
    for copy in loads:
        copy.wait()

    def work(slot, carry):
        @pl.when(slot > 0)
        def _():
            push(slot).wait_recv()

        def hidden(index, inner):
            span = pl.ds(pl.multiple_of(index * WIDE, WIDE), WIDE)
            if is_forward:
                pre = nn(land[slot], up_buf[:, span]) + side_ref[:, span]
                pre_buf[slot, :, span] = pre.astype(jnp.bfloat16)
                mid_buf[slot, :, span] = gelu(pre).astype(jnp.bfloat16)
            else:
                grad = nt(land[slot], down_buf[span, :])
                slope = gelu_slope(pre_buf[slot, :, span].astype(jnp.float32))
                mid_buf[slot, :, span] = (grad * slope).astype(jnp.bfloat16)
            return inner

        def result(index, inner):
            span = pl.ds(pl.multiple_of(index * WIDE, WIDE), WIDE)
            if is_forward:
                part = nn(mid_buf[slot], down_buf[:, span])
            else:
                part = nt(mid_buf[slot], up_buf[span, :])

            @pl.when(slot == 0)
            def _():
                sum_ref[:, span] = part

            @pl.when(slot > 0)
            def _():
                part_buf[slot, :, span] = part.astype(jnp.bfloat16)

            return inner

        lax.fori_loop(0, ff_width // WIDE, hidden, 0)
        for copy in outs(slot):
            copy.start()
        lax.fori_loop(0, width // WIDE, result, 0)

        @pl.when(slot > 0)
        def _():
            give_back(slot).start()

        return carry

    lax.fori_loop(0, count, work, 0)

    def add(slot, carry):
        give_back(slot).wait_recv()
        sum_ref[...] += got[slot].astype(jnp.float32)
        return carry

    lax.fori_loop(1, count, add, 0)
    for slot in range(count):
        for copy in outs(slot):
            copy.wait()
        if slot > 0:
            push(slot).wait_send()
            give_back(slot).wait_send()


def feed(x_rows, up_panel, down_panel, side, is_forward, count, collective_id):
    rows, width = x_rows.shape
    ff_width = up_panel.shape[1]
    kind = jnp.bfloat16
    by_width = jax.ShapeDtypeStruct((count, rows, width), kind)
    by_ff = jax.ShapeDtypeStruct((count, rows, ff_width), kind)
    total = jax.ShapeDtypeStruct((rows, width), jnp.float32)
    out_shape = (by_width, by_ff, by_ff, total) if is_forward else (by_width, by_ff, total)
    return pl.pallas_call(
        functools.partial(feed_kernel, is_forward, count),
        out_shape=out_shape,
        in_specs=[IN_VMEM, ANY, ANY, IN_VMEM if is_forward else ANY],
        out_specs=(ANY,) * (len(out_shape) - 1) + (IN_VMEM,),
        scratch_shapes=[
            pltpu.VMEM((count, rows, width), kind),
            pltpu.VMEM(up_panel.shape, kind),
            pltpu.VMEM(down_panel.shape, kind),
            pltpu.VMEM((count, rows, ff_width), kind),
            pltpu.VMEM((count, rows, ff_width), kind),
            pltpu.VMEM((count, rows, width), kind),
            pltpu.VMEM((count, rows, width), kind),
            pltpu.SemaphoreType.DMA((3,)),
            pltpu.SemaphoreType.DMA((count,)),
            pltpu.SemaphoreType.DMA((count,)),
            pltpu.SemaphoreType.DMA((count,)),
            pltpu.SemaphoreType.DMA((count,)),
            pltpu.SemaphoreType.DMA((3, count)),
        ],
        compiler_params=pltpu.CompilerParams(
            collective_id=collective_id, has_side_effects=True, vmem_limit_bytes=VMEM_MOST
        ),
        cost_estimate=busy(90),
        name="feed_forward" if is_forward else "feed_backward",
    )(x_rows, up_panel, down_panel, side)


def start_kernel(count, chips, x_ref, w_ref, rows_ref, panel_ref, own_sem, row_sems, line_sems, pair_sems):
    me, place = lax.axis_index("head"), lax.axis_index("seq")
    chip, core = place // PAIR, place % PAIR
    sibling = chip * PAIR + (1 - core)
    neighbours = ((chip + 1) * PAIR + core, (chip - 1) * PAIR + core)
    has_next = (chip < chips - 1, chip > 0)
    owns = [
        pltpu.make_async_copy(x_ref, rows_ref.at[me], own_sem.at[0]),
        pltpu.make_async_copy(w_ref, panel_ref.at[place], own_sem.at[1]),
    ]
    for copy in owns:
        copy.start()

    barrier = pltpu.get_barrier_semaphore()
    for slot in range(1, count):
        pl.semaphore_signal(
            barrier, inc=1, device_id={"head": group_peer(me, count, slot, 1)}, device_id_type=MESH
        )
    pl.semaphore_signal(barrier, inc=1, device_id={"seq": sibling}, device_id_type=MESH)
    for way in range(2):

        @pl.when(has_next[way])
        def _():
            pl.semaphore_signal(
                barrier, inc=1, device_id={"seq": neighbours[way]}, device_id_type=MESH
            )

    ends = (chip == 0).astype(jnp.int32) + (chip == chips - 1).astype(jnp.int32)
    pl.semaphore_wait(barrier, count - 1 + 3 - ends)

    pushes = []
    for slot in range(1, count):
        pushes.append(
            pltpu.make_async_remote_copy(
                src_ref=x_ref,
                dst_ref=rows_ref.at[me],
                send_sem=row_sems.at[0, slot],
                recv_sem=row_sems.at[1, slot],
                device_id={"head": group_peer(me, count, slot, 1)},
                device_id_type=MESH,
            )
        )

    def relay(way, step):
        origin = chip - step if way == 0 else chip + step
        block = panel_ref.at[origin * PAIR + core]
        return pltpu.make_async_remote_copy(
            src_ref=w_ref if step == 0 else block,
            dst_ref=block,
            send_sem=line_sems.at[0, way, step],
            recv_sem=line_sems.at[1, way, step],
            device_id={"seq": neighbours[way]},
            device_id_type=MESH,
        )

    def share(way, step):
        origin = chip - 1 - step if way == 0 else chip + 1 + step
        if way == 2:
            origin = chip
        block = panel_ref.at[origin * PAIR + core]
        return pltpu.make_async_remote_copy(
            src_ref=w_ref if way == 2 else block,
            dst_ref=block,
            send_sem=pair_sems.at[0, way, step],
            recv_sem=pair_sems.at[1, way, step],
            device_id={"seq": sibling},
            device_id_type=MESH,
        )

    def sends(way, step):
        behind = chip >= step if way == 0 else chip + step <= chips - 1
        return has_next[way] & behind

    def receives(way, step):
        return chip - 1 - step >= 0 if way == 0 else chip + 1 + step <= chips - 1

    for way in range(2):
        pl.when(sends(way, 0))(relay(way, 0).start)
    for copy in pushes:
        copy.start()
    share(2, 0).start()
    for step in range(chips - 1):
        for way in range(2):

            @pl.when(receives(way, step))
            def _():
                relay(way, step).wait_recv()
                if step + 1 < chips - 1:
                    pl.when(sends(way, step + 1))(relay(way, step + 1).start)
                share(way, step).start()

    for copy in owns + pushes:
        copy.wait()
    share(2, 0).wait()
    for step in range(chips - 1):
        for way in range(2):
            pl.when(sends(way, step))(relay(way, step).wait_send)
            pl.when(receives(way, step))(share(way, step).wait)


def start_gathers(x_rows, w_rows, head_count, seq_size, collective_id):
    chips = seq_size // PAIR
    return pl.pallas_call(
        functools.partial(start_kernel, head_count, chips),
        out_shape=(
            jax.ShapeDtypeStruct((head_count,) + x_rows.shape, x_rows.dtype),
            jax.ShapeDtypeStruct((seq_size,) + w_rows.shape, w_rows.dtype),
        ),
        in_specs=[IN_VMEM, IN_VMEM],
        out_specs=(ANY, ANY),
        scratch_shapes=[
            pltpu.SemaphoreType.DMA((2,)),
            pltpu.SemaphoreType.DMA((2, head_count)),
            pltpu.SemaphoreType.DMA((2, 2, chips)),
            pltpu.SemaphoreType.DMA((2, 3, chips)),
        ],
        compiler_params=pltpu.CompilerParams(
            collective_id=collective_id, has_side_effects=True, vmem_limit_bytes=16 * 1024 * 1024
        ),
        cost_estimate=busy(60),
        name="start_gathers",
    )(x_rows, w_rows)


def normalize(z_rows, gain, shift):
    average = jnp.mean(z_rows, axis=-1, keepdims=True)
    centered = z_rows - average
    variance = jnp.mean(centered * centered, axis=-1, keepdims=True)
    recip = lax.rsqrt(variance + NORM_EPS)
    normed = centered * recip
    return (normed * gain + shift, normed, recip)


def normalize_back(grad_rows, normed, recip, gain):
    scaled = grad_rows * gain
    dz_rows = recip * (
        scaled
        - jnp.mean(scaled, axis=-1, keepdims=True)
        - normed * jnp.mean(scaled * normed, axis=-1, keepdims=True)
    )
    return (dz_rows, jnp.sum(grad_rows * normed, axis=0), jnp.sum(grad_rows, axis=0))


def group_rows(rows_low):
    return lax.all_gather(rows_low, "head", axis=0, tiled=True)


def group_sums(partial_value):
    return lax.psum_scatter(
        partial_value.astype(jnp.bfloat16), "head", scatter_dimension=0, tiled=True
    ).astype(jnp.float32)


def adam_step(param, grad, moment, second, step_float):
    moment_new = 0.9 * moment + 0.1 * grad
    second_new = 0.999 * second + 0.001 * grad * grad
    fix_one = 1.0 - jnp.power(jnp.float32(0.9), step_float)
    fix_two = 1.0 - jnp.power(jnp.float32(0.999), step_float)
    update = ADAM_RATE * (moment_new / fix_one) / (jnp.sqrt(second_new / fix_two) + 1e-08)
    return (param - update, moment_new, second_new)


def shards(
    hidden_in,
    cotangent,
    lengths,
    token_order,
    own_map,
    w_query,
    w_key,
    w_value,
    w_out,
    w_up,
    w_down,
    gains,
    biases,
    up_bias,
    vector_moment,
    vector_second,
    bias_moment,
    bias_second,
    step_count,
    stat_left,
    stat_right,
    root_left,
    root_right,
    master,
):
    head_count = lax.axis_size("head")
    seq_size = lax.axis_size("seq")
    head_index = lax.axis_index("head")
    group_index = lax.axis_index("seq")
    tok_count = hidden_in.shape[0]
    width = hidden_in.shape[1]
    panel_width = w_query.shape[1]
    ff_width = w_up.shape[1]
    seq_count = lengths.shape[0]
    heads = panel_width // HDIM
    parts = seq_size // heads
    runs = token_order.shape[0] // RUN
    aligned = seq_count == 2
    tile = 1024 if aligned else RUN
    setup = (parts, tile, seq_count, aligned, runs)
    tables = stream_tables(token_order, lengths, head_count, seq_size, tile, group_index % parts)
    own_block = head_index * seq_size + group_index
    order_here = lax.dynamic_slice_in_dim(token_order, own_block * tok_count, tok_count, 0)
    valid_here = order_here < tables[3][seq_count - 1]
    inputs_f32 = hidden_in.astype(jnp.float32)

    inputs_grp, qkv_panel = start_gathers(
        hidden_in, jnp.concatenate([w_query, w_key, w_value], axis=1), head_count, seq_size, 7
    )
    inputs_grp = inputs_grp.reshape(head_count * tok_count, width)
    qkv_panel = qkv_panel.reshape(width, 3 * panel_width)
    o_panel = lax.all_gather(w_out, "seq", axis=1, tiled=True)
    up_panel = lax.all_gather(w_up, "seq", axis=0, tiled=True)
    down_panel = lax.all_gather(w_down, "seq", axis=1, tiled=True)

    def own_columns(row):
        return lax.dynamic_slice_in_dim(row, head_index * panel_width, panel_width, 0)

    qkv_bias = jnp.concatenate(
        [own_columns(biases[0]), jnp.zeros((panel_width,), jnp.float32), own_columns(biases[1])]
    )
    qkv_grp = (
        jnp.dot(inputs_grp, qkv_panel, preferred_element_type=jnp.float32) + qkv_bias
    ).astype(jnp.bfloat16)
    qkv_head = spread(qkv_grp, 3, heads, parts, seq_size, 0)
    qkv_head = qkv_head.reshape(3, runs, RUN, HDIM)
    attended_part, attended_exact, log_total = attend_forward(qkv_head, tables, setup)
    rows_grp = head_count * tok_count
    attended_grp = collect(
        attended_part.reshape(1, seq_size, rows_grp, HDIM), heads, parts, 1
    )
    branch_out = group_sums(jnp.dot(attended_grp, o_panel, preferred_element_type=jnp.float32))
    z_one = inputs_f32 + branch_out + biases[2]
    h_one, normed_one, recip_one = normalize(z_one, gains[0], biases[3])
    h_low = h_one.astype(jnp.bfloat16)
    h_grp, act, pre_act, ff_out = feed(
        h_low, up_panel, down_panel, up_bias.reshape(1, ff_width), True, head_count, 5
    )
    z_two = h_one + ff_out + biases[4]
    layer_f32, normed_two, recip_two = normalize(z_two, gains[1], biases[5])
    layer_out = layer_f32.astype(jnp.bfloat16)
    grad_y = cotangent.astype(jnp.float32) * valid_here[:, None].astype(jnp.float32)
    dz_two, dgain_two, dshift_two = normalize_back(grad_y, normed_two, recip_two, gains[1])
    dbias_down = jnp.sum(dz_two, axis=0)
    dz_two_grp, dpre, dh_part = feed(
        dz_two.astype(jnp.bfloat16), up_panel, down_panel, pre_act, False, head_count, 6
    )
    h_grp, act, dz_two_grp, dpre = (
        array.reshape(rows_grp, array.shape[2]) for array in (h_grp, act, dz_two_grp, dpre)
    )
    up_bias_part = jnp.sum(dpre.astype(jnp.float32), axis=0)
    dh_one = dz_two + dh_part
    dz_one, dgain_one, dshift_one = normalize_back(dh_one, normed_one, recip_one, gains[0])
    dbias_out = jnp.sum(dz_one, axis=0)
    dz_one_grp = group_rows(dz_one.astype(jnp.bfloat16))
    dattended = jnp.dot(dz_one_grp, o_panel.T, preferred_element_type=jnp.float32).astype(
        jnp.bfloat16
    )
    dattended_head = spread(dattended, 1, heads, parts, seq_size, 2).reshape(runs, RUN, HDIM)
    dqkv_part = attend_backward(
        qkv_head, dattended_head, attended_exact, log_total, tables, setup
    )
    dqkv_grp = collect(dqkv_part.reshape(3, seq_size, rows_grp, HDIM), heads, parts, 3)
    input_grad = dz_one + group_sums(
        jnp.dot(dqkv_grp, qkv_panel.T, preferred_element_type=jnp.float32)
    )
    bias_qkv = jnp.sum(dqkv_grp.astype(jnp.float32), axis=0)
    zero_width = jnp.zeros((width,), jnp.float32)
    dbias_query = lax.dynamic_update_slice_in_dim(
        zero_width, bias_qkv[:panel_width], head_index * panel_width, 0
    )
    dbias_value = lax.dynamic_update_slice_in_dim(
        zero_width, bias_qkv[2 * panel_width :], head_index * panel_width, 0
    )
    local_vectors = jnp.stack(
        (
            dbias_query,
            dbias_value,
            dbias_out,
            dshift_one,
            dbias_down,
            dshift_two,
            dgain_one,
            dgain_two,
        )
    )
    packed = jnp.concatenate([local_vectors.reshape(-1), up_bias_part])
    packed_all = lax.all_gather(packed, ("head", "seq"))
    vector_grad = jnp.sum(packed_all[:, : 8 * width], axis=0).reshape(8, width)
    up_bias_grad = jnp.sum(
        lax.dynamic_slice_in_dim(packed_all[:, 8 * width :], head_index * seq_size, seq_size, 0),
        axis=0,
    )
    left_index, right_index = block_operands(own_map[0], width, panel_width, ff_width)
    low_grads = owned_grads(
        left_index,
        right_index,
        (inputs_grp, attended_grp, h_grp, act),
        (dqkv_grp, dz_one_grp, dpre, dz_two_grp),
        seq_size,
        4,
    )
    block_grads = low_grads.astype(jnp.float32)
    stat_left_new = 0.5 * stat_left + 0.5 * jnp.einsum(
        "bij,bkj->bik", low_grads, low_grads, preferred_element_type=jnp.float32
    )
    stat_right_new = 0.5 * stat_right + 0.5 * jnp.einsum(
        "bji,bjk->bik", low_grads, low_grads, preferred_element_type=jnp.float32
    )
    left_mix = jnp.einsum(
        "bij,bjk->bik",
        root_left.astype(jnp.bfloat16),
        low_grads,
        preferred_element_type=jnp.float32,
    )
    direction = jnp.einsum(
        "bij,bjk->bik",
        left_mix.astype(jnp.bfloat16),
        root_right.astype(jnp.bfloat16),
        preferred_element_type=jnp.float32,
    )
    master_new = master - SHAMPOO_RATE * direction
    step_float = step_count[0].astype(jnp.float32)
    vector_params = jnp.concatenate([biases, gains], axis=0)
    vector_new, vector_moment_new, vector_second_new = adam_step(
        vector_params, vector_grad, vector_moment, vector_second, step_float
    )
    up_bias_new, bias_moment_new, bias_second_new = adam_step(
        up_bias, up_bias_grad, bias_moment, bias_second, step_float
    )
    return (
        layer_out,
        input_grad,
        block_grads,
        stat_left_new,
        stat_right_new,
        master_new,
        vector_new[0:6],
        vector_new[6:8],
        up_bias_new,
        vector_grad,
        vector_moment_new,
        vector_second_new,
        up_bias_grad,
        bias_moment_new,
        bias_second_new,
    )


def solution(mesh):
    rows = P(("head", "seq"), None)
    blocks = P(("head", "seq"), None, None)
    in_specs = (
        rows,
        rows,
        P(),
        P(),
        P("head", None),
        P("seq", "head"),
        P("seq", "head"),
        P("seq", "head"),
        P("head", "seq"),
        P("seq", "head"),
        P("head", "seq"),
        P(),
        P(),
        P("head"),
        P(),
        P(),
        P("head"),
        P("head"),
        P(),
        blocks,
        blocks,
        blocks,
        blocks,
        blocks,
    )
    out_specs = (
        rows,
        rows,
        blocks,
        blocks,
        blocks,
        blocks,
        P(),
        P(),
        P("head"),
        P(),
        P(),
        P(),
        P("head"),
        P("head"),
        P("head"),
    )
    return jax.shard_map(shards, mesh=mesh, in_specs=in_specs, out_specs=out_specs, check_vma=False)
```

```python
import functools
import math

import jax
import jax.numpy as jnp
from jax import lax
from jax.experimental import pallas as pl
from jax.experimental.pallas import tpu as pltpu
from jax.sharding import PartitionSpec as P


HDIM = 128
BLOCK = 256
RUN = 256

NEG_LARGE = -1e30
NORM_EPS = 1e-12
ADAM_RATE = 0.4
SHAMPOO_RATE = 0.15
MESH = pl.DeviceIdType.MESH
VMEM_MOST = 60 * 1024 * 1024

ANY = pl.BlockSpec(memory_space=pl.ANY)
IN_SMEM = pl.BlockSpec(memory_space=pltpu.SMEM)
IN_VMEM = pl.BlockSpec(memory_space=pltpu.VMEM)


def busy(microseconds):
    return pl.CostEstimate(
        flops=microseconds * 800_000_000, bytes_accessed=1_000_000, transcendentals=0
    )


def seq_barrier(me, heads, parts):
    own_head, own_part = me // parts, me % parts
    barrier = pltpu.get_barrier_semaphore()
    for step in range(1, heads):
        pl.semaphore_signal(
            barrier,
            inc=1,
            device_id={"seq": (own_head + step) % heads * parts + own_part},
            device_id_type=MESH,
        )
    for step in range(1, parts):
        pl.semaphore_signal(
            barrier,
            inc=1,
            device_id={"seq": own_head * parts + (own_part + step) % parts},
            device_id_type=MESH,
        )
    pl.semaphore_wait(barrier, heads - 1 + parts - 1)


def spread_kernel(
    fields, heads, parts, x_ref, y_ref, own_sem, send_sem, recv_sem, pass_sem, take_sem
):
    me = lax.axis_index("seq")
    own_head, own_part = me // parts, me % parts
    seq_barrier(me, heads, parts)

    def columns(field, head):
        return pl.ds(pl.multiple_of((field * heads + head) * HDIM, HDIM), HDIM)

    sends = []
    for step in range(1, heads):
        head = (own_head + step) % heads
        for field in range(fields):
            copy = pltpu.make_async_remote_copy(
                src_ref=x_ref.at[:, columns(field, head)],
                dst_ref=y_ref.at[field, me],
                send_sem=send_sem.at[step - 1, field],
                recv_sem=recv_sem.at[step - 1, field],
                device_id={"seq": head * parts + own_part},
                device_id_type=MESH,
            )
            copy.start()
            sends.append(copy)
    owns = []
    for field in range(fields):
        copy = pltpu.make_async_copy(
            x_ref.at[:, columns(field, own_head)], y_ref.at[field, me], own_sem.at[field]
        )
        copy.start()
        owns.append(copy)
    passes = []

    def pass_on(step, field, source):
        origin = (own_head - step + heads) % heads * parts + own_part
        for other in range(1, parts):
            copy = pltpu.make_async_remote_copy(
                src_ref=source,
                dst_ref=y_ref.at[field, origin],
                send_sem=pass_sem.at[other - 1, step, field],
                recv_sem=take_sem.at[other - 1, step, field],
                device_id={"seq": own_head * parts + (own_part + other) % parts},
                device_id_type=MESH,
            )
            copy.start()
            passes.append(copy)

    for field in range(fields):
        pass_on(0, field, x_ref.at[:, columns(field, own_head)])
    for step in range(1, heads):
        origin = (own_head - step + heads) % heads * parts + own_part
        for field in range(fields):
            sends[(step - 1) * fields + field].wait_recv()
            pass_on(step, field, y_ref.at[field, origin])
    for copy in owns:
        copy.wait()
    for copy in sends:
        copy.wait_send()
    for copy in passes:
        copy.wait()


def spread(x_rows, fields, heads, parts, seq_size, collective_id):
    rows = x_rows.shape[0]
    return pl.pallas_call(
        functools.partial(spread_kernel, fields, heads, parts),
        out_shape=jax.ShapeDtypeStruct((fields, seq_size, rows, HDIM), x_rows.dtype),
        in_specs=[IN_VMEM],
        out_specs=ANY,
        scratch_shapes=[
            pltpu.SemaphoreType.DMA((fields,)),
            pltpu.SemaphoreType.DMA((max(heads - 1, 1), fields)),
            pltpu.SemaphoreType.DMA((max(heads - 1, 1), fields)),
            pltpu.SemaphoreType.DMA((max(parts - 1, 1), heads, fields)),
            pltpu.SemaphoreType.DMA((max(parts - 1, 1), heads, fields)),
        ],
        compiler_params=pltpu.CompilerParams(
            collective_id=collective_id, has_side_effects=True, vmem_limit_bytes=24 * 1024 * 1024
        ),
        cost_estimate=busy(fields * 24),
        name="spread",
    )(x_rows)


def collect_kernel(
    fields,
    heads,
    parts,
    x_ref,
    y_ref,
    own,
    got,
    ready,
    own_sem,
    pass_sem,
    take_sem,
    send_sem,
    recv_sem,
    keep_sem,
):
    me = lax.axis_index("seq")
    own_head, own_part = me // parts, me % parts
    seq_barrier(me, heads, parts)
    order = list(range(1, heads)) + [0]

    def home(step, part):
        return (own_head + step) % heads * parts + part

    passes, owns = {}, {}
    for step in order:
        for field in range(fields):
            for other in range(1, parts):
                part = (own_part + other) % parts
                copy = pltpu.make_async_remote_copy(
                    src_ref=x_ref.at[field, home(step, part)],
                    dst_ref=got.at[other - 1, step, field],
                    send_sem=pass_sem.at[other - 1, step, field],
                    recv_sem=take_sem.at[other - 1, step, field],
                    device_id={"seq": own_head * parts + part},
                    device_id_type=MESH,
                )
                copy.start()
                passes[step, field, other] = copy
            copy = pltpu.make_async_copy(
                x_ref.at[field, home(step, own_part)], own.at[step, field], own_sem.at[step, field]
            )
            copy.start()
            owns[step, field] = copy

    sends = []
    for step in order:
        for field in range(fields):
            owns[step, field].wait()
            for other in range(1, parts):
                passes[step, field, other].wait_recv()
            total = own[step, field].astype(jnp.float32)
            for other in range(1, parts):
                total = total + got[other - 1, step, field].astype(jnp.float32)
            ready[step, field] = total.astype(ready.dtype)
            columns = pl.ds(pl.multiple_of((field * heads + own_head) * HDIM, HDIM), HDIM)
            if step == 0:
                copy = pltpu.make_async_copy(
                    ready.at[step, field], y_ref.at[:, columns], keep_sem.at[field]
                )
            else:
                copy = pltpu.make_async_remote_copy(
                    src_ref=ready.at[step, field],
                    dst_ref=y_ref.at[:, columns],
                    send_sem=send_sem.at[step - 1, field],
                    recv_sem=recv_sem.at[step - 1, field],
                    device_id={"seq": home(step, own_part)},
                    device_id_type=MESH,
                )
            copy.start()
            sends.append(copy)
    for copy in sends:
        copy.wait()
    for copy in passes.values():
        copy.wait_send()


def collect(x_parts, heads, parts, collective_id):
    fields, _, rows, _ = x_parts.shape
    kind = x_parts.dtype
    few = max(parts - 1, 1)
    return pl.pallas_call(
        functools.partial(collect_kernel, fields, heads, parts),
        out_shape=jax.ShapeDtypeStruct((rows, fields * heads * HDIM), kind),
        in_specs=[ANY],
        out_specs=ANY,
        scratch_shapes=[
            pltpu.VMEM((heads, fields, rows, HDIM), kind),
            pltpu.VMEM((few, heads, fields, rows, HDIM), kind),
            pltpu.VMEM((heads, fields, rows, HDIM), kind),
            pltpu.SemaphoreType.DMA((heads, fields)),
            pltpu.SemaphoreType.DMA((few, heads, fields)),
            pltpu.SemaphoreType.DMA((few, heads, fields)),
            pltpu.SemaphoreType.DMA((max(heads - 1, 1), fields)),
            pltpu.SemaphoreType.DMA((max(heads - 1, 1), fields)),
            pltpu.SemaphoreType.DMA((fields,)),
        ],
        compiler_params=pltpu.CompilerParams(
            collective_id=collective_id, has_side_effects=True, vmem_limit_bytes=VMEM_MOST
        ),
        cost_estimate=busy(fields * 24),
        name="collect",
    )(x_parts)


def allowed_tile(ends_ref, seq_count, key_low, query_low, shape):
    key_pos = key_low + lax.broadcasted_iota(jnp.int32, shape, 0)
    query_pos = query_low + lax.broadcasted_iota(jnp.int32, shape, 1)
    key_seg = jnp.zeros(shape, jnp.int32)
    query_seg = jnp.zeros(shape, jnp.int32)
    for index in range(seq_count):
        key_seg += (key_pos >= ends_ref[index]).astype(jnp.int32)
        query_seg += (query_pos >= ends_ref[index]).astype(jnp.int32)
    last = ends_ref[seq_count - 1]
    key_seg = jnp.where(key_pos < last, key_seg, seq_count + key_pos)
    query_seg = jnp.where(query_pos < last, query_seg, seq_count + query_pos)
    return key_seg == query_seg


def nt(left, right):
    return lax.dot_general(
        left, right, (((1,), (1,)), ((), ())), preferred_element_type=jnp.float32
    )


def nn(left, right):
    return lax.dot_general(
        left, right, (((1,), (0,)), ((), ())), preferred_element_type=jnp.float32
    )


def forward_kernel(
    setup,
    where_ref,
    low_ref,
    high_ref,
    ends_ref,
    part_ref,
    qkv_ref,
    out_ref,
    exact_ref,
    log_ref,
    q_buf,
    k_buf,
    v_buf,
    vt_buf,
    sem,
):
    parts, tile, seq_count, aligned, runs = setup
    turn = pl.program_id(0)
    part = part_ref[0]
    scale2 = math.log2(math.e) / math.sqrt(HDIM)

    @pl.when(turn == 0)
    def _():
        def fetch(field, run, buf, slot):
            return pltpu.make_async_copy(
                qkv_ref.at[field, where_ref[run]],
                buf.at[pl.ds(pl.multiple_of(slot * RUN, RUN), RUN), :],
                sem.at[field],
            )

        def start(run, carry):
            fetch(1, run, k_buf, run).start()
            fetch(2, run, v_buf, run).start()
            return carry

        def start_own(index, carry):
            fetch(0, index * parts + part, q_buf, index).start()
            return carry

        def finish(run, carry):
            fetch(1, run, k_buf, run).wait()
            fetch(2, run, v_buf, run).wait()
            return carry

        def finish_own(index, carry):
            fetch(0, index * parts + part, q_buf, index).wait()
            return carry

        lax.fori_loop(0, runs, start, 0)
        lax.fori_loop(0, runs // parts, start_own, 0)
        out_ref[...] = jnp.zeros_like(out_ref)
        lax.fori_loop(0, runs, finish, 0)
        lax.fori_loop(0, runs // parts, finish_own, 0)
        if aligned:

            def turn_tile(index, carry):
                low = pl.multiple_of(index * RUN, RUN)
                vt_buf[:, pl.ds(low, RUN)] = v_buf[pl.ds(low, RUN), :].T
                return carry

            lax.fori_loop(0, runs, turn_tile, 0)

    run = turn * parts + part
    place = where_ref[run]
    queries = q_buf[pl.ds(pl.multiple_of(turn * RUN, RUN), RUN), :]

    def attend():
        def key_step(index, carry):
            top, total, acc = carry
            low = pl.multiple_of(index * tile, tile)
            scores = nt(k_buf[pl.ds(low, tile), :], queries)
            if not aligned:
                allowed = allowed_tile(ends_ref, seq_count, low, run * RUN, scores.shape)
                scores = jnp.where(allowed, scores, NEG_LARGE)
            new_top = jnp.maximum(top, jnp.max(scores, axis=0, keepdims=True))
            prob = jnp.exp2((scores - new_top) * scale2)
            if not aligned:
                prob = jnp.where(allowed, prob, 0.0)
            fade = jnp.exp2((top - new_top) * scale2)
            total = total * fade + jnp.sum(prob, axis=0, keepdims=True)
            if aligned:
                turned = vt_buf[:, pl.ds(low, tile)]
            else:
                turned = v_buf[pl.ds(low, tile), :].T
            acc = acc * fade + nn(turned, prob.astype(jnp.bfloat16))
            return new_top, total, acc

        top, total, acc = lax.fori_loop(
            low_ref[run],
            high_ref[run],
            key_step,
            (
                jnp.full((1, RUN), NEG_LARGE, jnp.float32),
                jnp.zeros((1, RUN), jnp.float32),
                jnp.zeros((HDIM, RUN), jnp.float32),
            ),
        )
        result = (acc / total).T
        exact_ref[0] = result
        out_ref[place] = result.astype(out_ref.dtype)
        log_ref[0] = top * scale2 + jnp.log2(total)

    if aligned:
        is_valid = run * RUN < ends_ref[seq_count - 1]
        pl.when(is_valid)(attend)

        @pl.when(jnp.logical_not(is_valid))
        def _():
            values = v_buf[pl.ds(pl.multiple_of(run * RUN, RUN), RUN), :]
            exact_ref[0] = values.astype(jnp.float32)
            out_ref[place] = values
            log_ref[0] = jnp.zeros((1, RUN), jnp.float32)
    else:
        attend()


def attend_forward(qkv, tables, setup):
    parts, _, _, aligned, runs = setup
    own = runs // parts
    rows = runs * RUN
    return pl.pallas_call(
        functools.partial(forward_kernel, setup),
        grid=(own,),
        out_shape=(
            jax.ShapeDtypeStruct((runs, RUN, HDIM), jnp.bfloat16),
            jax.ShapeDtypeStruct((own, RUN, HDIM), jnp.float32),
            jax.ShapeDtypeStruct((own, 1, RUN), jnp.float32),
        ),
        in_specs=[IN_SMEM] * 5 + [ANY],
        out_specs=(
            pl.BlockSpec((runs, RUN, HDIM), lambda i: (0, 0, 0), pipeline_mode=pl.Buffered(1)),
            pl.BlockSpec((1, RUN, HDIM), lambda i: (i, 0, 0)),
            pl.BlockSpec((1, 1, RUN), lambda i: (i, 0, 0)),
        ),
        scratch_shapes=[
            pltpu.VMEM((own * RUN, HDIM), jnp.bfloat16),
            pltpu.VMEM((rows, HDIM), jnp.bfloat16),
            pltpu.VMEM((rows, HDIM), jnp.bfloat16),
            pltpu.VMEM((HDIM, rows if aligned else RUN), jnp.bfloat16),
            pltpu.SemaphoreType.DMA((3,)),
        ],
        compiler_params=pltpu.CompilerParams(
            dimension_semantics=("arbitrary",), vmem_limit_bytes=VMEM_MOST
        ),
        cost_estimate=busy(36),
        name="attend_forward",
    )(*tables, qkv)


def backward_kernel(
    setup,
    where_ref,
    low_ref,
    high_ref,
    ends_ref,
    part_ref,
    qkv_ref,
    grad_ref,
    exact_ref,
    log_ref,
    out_ref,
    q_buf,
    k_buf,
    v_buf,
    kt_buf,
    g_buf,
    dk_acc,
    dv_acc,
    stage,
    sem,
    out_sem,
):
    parts, tile, seq_count, aligned, runs = setup
    own = runs // parts
    turn = pl.program_id(0)
    part = part_ref[0]
    scale = 1.0 / math.sqrt(HDIM)
    scale2 = math.log2(math.e) * scale

    @pl.when(turn == 0)
    def _():
        def fetch(source, index, buf, slot, lane):
            return pltpu.make_async_copy(
                source.at[index],
                buf.at[pl.ds(pl.multiple_of(slot * RUN, RUN), RUN), :],
                sem.at[lane],
            )

        def pair(run):
            place = where_ref[run]
            return (
                fetch(qkv_ref.at[1], place, k_buf, run, 1),
                fetch(qkv_ref.at[2], place, v_buf, run, 2),
            )

        def own_pair(index):
            place = where_ref[index * parts + part]
            return (
                fetch(qkv_ref.at[0], place, q_buf, index, 0),
                fetch(grad_ref, place, g_buf, index, 3),
            )

        def start(run, carry):
            for copy in pair(run):
                copy.start()
            return carry

        def start_own(index, carry):
            for copy in own_pair(index):
                copy.start()
            return carry

        def finish(run, carry):
            for copy in pair(run):
                copy.wait()
            return carry

        def finish_own(index, carry):
            for copy in own_pair(index):
                copy.wait()
            return carry

        lax.fori_loop(0, runs, start, 0)
        lax.fori_loop(0, own, start_own, 0)
        dk_acc[...] = jnp.zeros_like(dk_acc)
        dv_acc[...] = jnp.zeros_like(dv_acc)
        lax.fori_loop(0, runs, finish, 0)
        lax.fori_loop(0, own, finish_own, 0)
        if aligned:

            def turn_tile(index, carry):
                low = pl.multiple_of(index * RUN, RUN)
                kt_buf[:, pl.ds(low, RUN)] = k_buf[pl.ds(low, RUN), :].T
                return carry

            lax.fori_loop(0, runs, turn_tile, 0)

    run = turn * parts + part
    low_row = pl.multiple_of(turn * RUN, RUN)

    def attend():
        queries = q_buf[pl.ds(low_row, RUN), :]
        grads = g_buf[pl.ds(low_row, RUN), :]
        delta = jnp.sum((grads.astype(jnp.float32) * exact_ref[0]).T, axis=0, keepdims=True)
        log_total = log_ref[0]

        def key_step(index, acc):
            low = pl.multiple_of(index * tile, tile)
            keys = k_buf[pl.ds(low, tile), :]
            values = v_buf[pl.ds(low, tile), :]
            scores = nt(keys, queries)
            prob = jnp.exp2(scores * scale2 - log_total)
            if not aligned:
                allowed = allowed_tile(ends_ref, seq_count, low, run * RUN, scores.shape)
                prob = jnp.where(allowed, prob, 0.0)
            prob_grad = nt(values, grads)
            dv_acc[pl.ds(low, tile), :] += nn(prob.astype(jnp.bfloat16), grads)
            score_grad = (prob * (prob_grad - delta)).astype(jnp.bfloat16)
            dk_acc[pl.ds(low, tile), :] += nn(score_grad, queries)
            turned = kt_buf[:, pl.ds(low, tile)] if aligned else keys.T
            return acc + nn(turned, score_grad)

        acc = lax.fori_loop(
            low_ref[run], high_ref[run], key_step, jnp.zeros((HDIM, RUN), jnp.float32)
        )
        q_buf[pl.ds(low_row, RUN), :] = (acc.T * scale).astype(jnp.bfloat16)

    if aligned:
        is_valid = run * RUN < ends_ref[seq_count - 1]
        pl.when(is_valid)(attend)

        @pl.when(jnp.logical_not(is_valid))
        def _():
            q_buf[pl.ds(low_row, RUN), :] = jnp.zeros((RUN, HDIM), jnp.bfloat16)
    else:
        attend()

    @pl.when(turn == own - 1)
    def _():
        def key_copies(run_index, slot):
            place = where_ref[run_index]
            return (
                pltpu.make_async_copy(stage.at[slot, 0], out_ref.at[1, place], out_sem.at[slot, 0]),
                pltpu.make_async_copy(stage.at[slot, 1], out_ref.at[2, place], out_sem.at[slot, 1]),
            )

        v_buf[pl.ds(0, RUN), :] = jnp.zeros((RUN, HDIM), jnp.bfloat16)

        def query_copy(run_index):
            mine = run_index % parts == part
            place = where_ref[run_index]
            index = jnp.where(mine, run_index // parts, 0)
            return mine, (
                pltpu.make_async_copy(
                    q_buf.at[pl.ds(pl.multiple_of(index * RUN, RUN), RUN), :],
                    out_ref.at[0, place],
                    sem.at[0],
                ),
                pltpu.make_async_copy(
                    v_buf.at[pl.ds(0, RUN), :], out_ref.at[0, place], sem.at[0]
                ),
            )

        def start_query(run_index, carry):
            mine, (copy, blank) = query_copy(run_index)
            pl.when(mine)(copy.start)
            pl.when(jnp.logical_not(mine))(blank.start)
            return carry

        def finish_query(run_index, carry):
            _, (copy, blank) = query_copy(run_index)
            blank.wait()
            return carry

        lax.fori_loop(0, runs, start_query, 0)

        def write(run_index, carry):
            slot = run_index % 2

            @pl.when(run_index >= 2)
            def _():
                for copy in key_copies(run_index - 2, slot):
                    copy.wait()

            low = pl.multiple_of(run_index * RUN, RUN)
            stage[slot, 0] = (dk_acc[pl.ds(low, RUN), :] * scale).astype(jnp.bfloat16)
            stage[slot, 1] = dv_acc[pl.ds(low, RUN), :].astype(jnp.bfloat16)
            for copy in key_copies(run_index, slot):
                copy.start()
            return carry

        lax.fori_loop(0, runs, write, 0)
        for back in (2, 1):
            for copy in key_copies(runs - back, (runs - back) % 2):
                copy.wait()
        lax.fori_loop(0, runs, finish_query, 0)


def attend_backward(qkv, grads, exact, log_total, tables, setup):
    parts, _, _, aligned, runs = setup
    own = runs // parts
    rows = runs * RUN
    return pl.pallas_call(
        functools.partial(backward_kernel, setup),
        grid=(own,),
        out_shape=jax.ShapeDtypeStruct((3, runs, RUN, HDIM), jnp.bfloat16),
        in_specs=[IN_SMEM] * 5
        + [
            ANY,
            ANY,
            pl.BlockSpec((1, RUN, HDIM), lambda i: (i, 0, 0)),
            pl.BlockSpec((1, 1, RUN), lambda i: (i, 0, 0)),
        ],
        out_specs=ANY,
        scratch_shapes=[
            pltpu.VMEM((own * RUN, HDIM), jnp.bfloat16),
            pltpu.VMEM((rows, HDIM), jnp.bfloat16),
            pltpu.VMEM((rows, HDIM), jnp.bfloat16),
            pltpu.VMEM((HDIM, rows if aligned else RUN), jnp.bfloat16),
            pltpu.VMEM((own * RUN, HDIM), jnp.bfloat16),
            pltpu.VMEM((rows, HDIM), jnp.float32),
            pltpu.VMEM((rows, HDIM), jnp.float32),
            pltpu.VMEM((2, 2, RUN, HDIM), jnp.bfloat16),
            pltpu.SemaphoreType.DMA((4,)),
            pltpu.SemaphoreType.DMA((2, 2)),
        ],
        compiler_params=pltpu.CompilerParams(
            dimension_semantics=("arbitrary",), vmem_limit_bytes=VMEM_MOST
        ),
        cost_estimate=busy(50),
        name="attend_backward",
    )(*tables, qkv, grads, exact, log_total)


def stream_tables(token_order, lengths, head_count, seq_size, tile, part):
    runs = token_order.shape[0] // RUN
    stream = (token_order.reshape(head_count, seq_size, RUN)[:, :, 0] // RUN).T.reshape(-1)
    places = jnp.arange(runs, dtype=jnp.int32)
    where = jnp.sum(jnp.where(stream[None, :] == places[:, None], places[None, :], 0), axis=1)
    ends = jnp.cumsum(lengths)
    starts = ends - lengths
    first = places * RUN
    last = first + RUN - 1

    def bound(position, of_seq, of_pad):
        inside = (position[:, None] >= starts[None, :]) & (position[:, None] < ends[None, :])
        found = jnp.sum(jnp.where(inside, of_seq[None, :], 0), axis=1)
        return jnp.where(position < ends[-1], found, of_pad)

    low = bound(first, starts, first) // tile
    high = (bound(last, ends, last + 1) + tile - 1) // tile
    return (
        where.astype(jnp.int32),
        low.astype(jnp.int32),
        high.astype(jnp.int32),
        ends.astype(jnp.int32),
        part.reshape(1).astype(jnp.int32),
    )


PAIR = 2
DEPTH = 6
LAG = 2


def grads_kernel(spec, left_ref, right_ref, *refs):
    chips, slots, left_strips, right_strips = spec
    lefts, refs = refs[: len(left_strips)], refs[len(left_strips) :]
    rights, refs = refs[: len(right_strips)], refs[len(right_strips) :]
    (
        out_ref,
        left_buf,
        right_buf,
        strip_buf,
        pair_out,
        pair_in,
        line_out,
        line_in,
        last_in,
        own_sum,
        load_sem,
        pair_send,
        pair_recv,
        line_send,
        line_recv,
        last_recv,
        pair_free,
        line_free,
    ) = refs
    me = lax.axis_index("seq")
    chip, core = me // PAIR, me % PAIR
    sibling = chip * PAIR + (1 - core)
    neighbours = ((chip + 1) * PAIR + core, (chip - 1) * PAIR + core)
    has_next = (chip < chips - 1, chip > 0)

    barrier = pltpu.get_barrier_semaphore()
    pl.semaphore_signal(barrier, inc=1, device_id={"seq": sibling}, device_id_type=MESH)
    for way in range(2):

        @pl.when(has_next[way])
        def _():
            pl.semaphore_signal(
                barrier, inc=1, device_id={"seq": neighbours[way]}, device_id_type=MESH
            )

    ends = (chip == 0).astype(jnp.int32) + (chip == chips - 1).astype(jnp.int32)
    pl.semaphore_wait(barrier, 3 - ends)

    def strip(source, index):
        return source.at[:, pl.ds(pl.multiple_of(index * BLOCK, BLOCK), BLOCK)]

    low = 0
    for source, count in zip(rights, right_strips):

        def load_right(index, carry, source=source, low=low):
            pltpu.make_async_copy(
                strip(source, index), right_buf.at[low + index], load_sem.at[2]
            ).start()
            return carry

        lax.fori_loop(0, count, load_right, 0)
        low += count
    rows = left_buf.shape[2]
    low = 0
    for source, count in zip(lefts, left_strips):

        def fetch(index, slot, source=source):
            return pltpu.make_async_copy(strip(source, index), strip_buf.at[slot], load_sem.at[slot])

        def turn_strip(index, carry, count=count, low=low, fetch=fetch):
            slot = index % 2

            @pl.when(index + 1 < count)
            def _():
                fetch(index + 1, 1 - slot).start()

            fetch(index, slot).wait()
            for part in range(rows // BLOCK):
                span = pl.ds(part * BLOCK, BLOCK)
                left_buf[low + index, :, span] = strip_buf[slot, span, :].T
            return carry

        fetch(0, 0).start()
        lax.fori_loop(0, count, turn_strip, 0)
        low += count
    low = 0
    for source, count in zip(rights, right_strips):

        def wait_right(index, carry, source=source, low=low):
            pltpu.make_async_copy(
                strip(source, index), right_buf.at[low + index], load_sem.at[2]
            ).wait()
            return carry

        lax.fori_loop(0, count, wait_right, 0)
        low += count

    def product(owner_chip, owner_core, k):
        slot = (owner_chip * PAIR + owner_core) * slots + k
        return nn(left_buf[left_ref[slot]], right_buf[right_ref[slot]])

    counts = ((chips - 1 - chip) * slots, chip * slots, slots)

    def owner(stream, step):
        if stream == 0:
            return chips - 1 - step // slots
        if stream == 1:
            return step // slots
        return chip

    def pair_copy(stream, step):
        slot = step % DEPTH
        return pltpu.make_async_remote_copy(
            src_ref=pair_out.at[stream, slot],
            dst_ref=pair_in.at[stream, slot],
            send_sem=pair_send.at[stream, slot],
            recv_sem=pair_recv.at[stream, slot],
            device_id={"seq": sibling},
            device_id_type=MESH,
        )

    def line_copy(stream, step):
        slot = step % DEPTH
        return pltpu.make_async_remote_copy(
            src_ref=line_out.at[stream, slot],
            dst_ref=line_in.at[stream, slot],
            send_sem=line_send.at[stream, slot],
            recv_sem=line_recv.at[stream, slot],
            device_id={"seq": neighbours[stream]},
            device_id_type=MESH,
        )

    def last_copy(stream, step):
        slot, k = step % DEPTH, step % slots
        return pltpu.make_async_remote_copy(
            src_ref=line_out.at[stream, slot],
            dst_ref=last_in.at[stream, k],
            send_sem=line_send.at[stream, slot],
            recv_sem=last_recv.at[stream, k],
            device_id={"seq": neighbours[stream]},
            device_id_type=MESH,
        )

    def give(stream, step):
        slot = step % DEPTH

        @pl.when(step >= DEPTH)
        def _():
            pair_copy(stream, step).wait_send()
            pl.semaphore_wait(pair_free.at[stream], 1)

        pair_out[stream, slot] = product(owner(stream, step), 1 - core, step % slots).astype(
            jnp.bfloat16
        )
        pair_copy(stream, step).start()

    def take(stream, step):
        slot = step % DEPTH
        total = product(owner(stream, step), core, step % slots)
        pair_copy(stream, step).wait_recv()
        total = total + pair_in[stream, slot].astype(jnp.float32)

        @pl.when(step + DEPTH < counts[stream])
        def _():
            pl.semaphore_signal(
                pair_free.at[stream], inc=1, device_id={"seq": sibling}, device_id_type=MESH
            )

        return total

    def forward(stream, step):
        slot = step % DEPTH
        target = chip + 1 if stream == 0 else chip - 1
        ends_there = owner(stream, step) == target
        has_source = has_next[1 - stream]
        total = take(stream, step)

        @pl.when(step >= DEPTH)
        def _():
            line_copy(stream, step).wait_send()

        @pl.when(has_source)
        def _():
            line_copy(stream, step).wait_recv()
            line_out[stream, slot] = (total + line_in[stream, slot].astype(jnp.float32)).astype(
                jnp.bfloat16
            )

            @pl.when(step + DEPTH < counts[stream])
            def _():
                pl.semaphore_signal(
                    line_free.at[stream],
                    inc=1,
                    device_id={"seq": neighbours[1 - stream]},
                    device_id_type=MESH,
                )

        @pl.when(jnp.logical_not(has_source))
        def _():
            line_out[stream, slot] = total.astype(jnp.bfloat16)

        @pl.when(ends_there)
        def _():
            last_copy(stream, step).start()

        @pl.when(jnp.logical_not(ends_there))
        def _():
            @pl.when(step >= DEPTH)
            def _():
                pl.semaphore_wait(line_free.at[stream], 1)

            line_copy(stream, step).start()

    def keep(step):
        own_sum[step] = take(2, step).astype(jnp.bfloat16)

    for stream in range(2):
        pl.when(counts[stream] > 0)(functools.partial(give, stream, 0))
    give(2, 0)

    delays = (chip * LAG, (chips - 1 - chip) * LAG, slots)

    def body(turn, carry):
        for stream in range(3):
            step = turn - delays[stream] + 1

            @pl.when((step > 0) & (step < counts[stream]))
            def _():
                give(stream, step)

        for stream in range(3):
            step = turn - delays[stream]

            @pl.when((step >= 0) & (step < counts[stream]))
            def _():
                if stream < 2:
                    forward(stream, step)
                else:
                    keep(step)

        return carry

    lax.fori_loop(0, (chips - 1) * slots + (chips - 1) * LAG, body, 0)

    def finish(k, carry):
        out_ref[k] = own_sum[k]
        for stream in range(2):

            @pl.when(has_next[1 - stream])
            def _():
                last_copy(stream, k).wait_recv()
                out_ref[k] = (
                    out_ref[k].astype(jnp.float32) + last_in[stream, k].astype(jnp.float32)
                ).astype(jnp.bfloat16)

        return carry

    lax.fori_loop(0, slots, finish, 0)
    for slot in range(DEPTH):
        for stream in range(2):

            @pl.when(counts[stream] > 0)
            def _():
                line_copy(stream, slot).wait_send()
                pair_copy(stream, slot).wait_send()

        pair_copy(2, slot).wait_send()


def owned_grads(left_index, right_index, lefts, rights, seq_size, collective_id):
    rows = lefts[0].shape[0]
    left_strips = tuple(array.shape[1] // BLOCK for array in lefts)
    right_strips = tuple(array.shape[1] // BLOCK for array in rights)
    chips = seq_size // PAIR
    slots = left_index.shape[0] // seq_size
    kind = jnp.bfloat16
    block = (BLOCK, BLOCK)
    return pl.pallas_call(
        functools.partial(grads_kernel, (chips, slots, left_strips, right_strips)),
        out_shape=jax.ShapeDtypeStruct((slots,) + block, kind),
        in_specs=[IN_SMEM] * 2 + [ANY] * (len(lefts) + len(rights)),
        out_specs=IN_VMEM,
        scratch_shapes=[
            pltpu.VMEM((sum(left_strips), BLOCK, rows), kind),
            pltpu.VMEM((sum(right_strips), rows, BLOCK), kind),
            pltpu.VMEM((2, rows, BLOCK), kind),
            pltpu.VMEM((3, DEPTH) + block, kind),
            pltpu.VMEM((3, DEPTH) + block, kind),
            pltpu.VMEM((2, DEPTH) + block, kind),
            pltpu.VMEM((2, DEPTH) + block, kind),
            pltpu.VMEM((2, slots) + block, kind),
            pltpu.VMEM((slots,) + block, kind),
            pltpu.SemaphoreType.DMA((3,)),
            pltpu.SemaphoreType.DMA((3, DEPTH)),
            pltpu.SemaphoreType.DMA((3, DEPTH)),
            pltpu.SemaphoreType.DMA((2, DEPTH)),
            pltpu.SemaphoreType.DMA((2, DEPTH)),
            pltpu.SemaphoreType.DMA((2, slots)),
            pltpu.SemaphoreType.REGULAR((3,)),
            pltpu.SemaphoreType.REGULAR((2,)),
        ],
        compiler_params=pltpu.CompilerParams(
            collective_id=collective_id, has_side_effects=True, vmem_limit_bytes=VMEM_MOST
        ),
        cost_estimate=busy(240),
        name="owned_grads",
    )(left_index, right_index, *lefts, *rights)


def block_operands(own_map, width, panel_width, ff_width):
    deep, narrow, wide = width // BLOCK, panel_width // BLOCK, ff_width // BLOCK
    left = jnp.zeros_like(own_map)
    right = jnp.zeros_like(own_map)
    first, left_low, right_low = 0, 0, 0
    panels = [(deep, narrow, 0, 0), (deep, narrow, 0, narrow), (deep, narrow, 0, 2 * narrow)]
    panels.append((narrow, deep, deep, 3 * narrow))
    panels.append((deep, wide, deep + narrow, 3 * narrow + deep))
    panels.append((wide, deep, 2 * deep + narrow, 3 * narrow + deep + wide))
    for high, broad, left_low, right_low in panels:
        inside = (own_map >= first) & (own_map < first + high * broad)
        within = own_map - first
        left = jnp.where(inside, left_low + within // broad, left)
        right = jnp.where(inside, right_low + within % broad, right)
        first += high * broad
    return left.astype(jnp.int32), right.astype(jnp.int32)


def group_peer(me, count, slot, way):
    far, near = slot // 2, slot % 2
    half = count // 2
    return (me // 2 + way * far + half) % half * 2 + (me % 2 + near) % 2


def group_barrier(me, count):
    barrier = pltpu.get_barrier_semaphore()
    for slot in range(1, count):
        pl.semaphore_signal(
            barrier, inc=1, device_id={"head": group_peer(me, count, slot, 1)}, device_id_type=MESH
        )
    pl.semaphore_wait(barrier, count - 1)


GELU_SCALE = 0.7978845608028654
GELU_CUBIC = 0.044715
WIDE = 512


def gelu(u):
    return 0.5 * u * (1.0 + jnp.tanh(GELU_SCALE * (u + GELU_CUBIC * (u * u * u))))


def gelu_slope(u):
    square = u * u
    bend = jnp.tanh(GELU_SCALE * (u + GELU_CUBIC * (square * u)))
    inner = GELU_SCALE * (1.0 + 3.0 * GELU_CUBIC * square)
    return 0.5 * (1.0 + bend) + 0.5 * u * (1.0 - bend * bend) * inner


def feed_kernel(is_forward, count, x_ref, up_ref, down_ref, side_ref, *refs):
    if is_forward:
        rows_ref, mid_ref, pre_ref, sum_ref = refs[:4]
        refs = refs[4:]
    else:
        rows_ref, mid_ref, sum_ref = refs[:3]
        refs = refs[3:]
    (
        land,
        up_buf,
        down_buf,
        mid_buf,
        pre_buf,
        part_buf,
        got,
        load_sem,
        send_sem,
        recv_sem,
        back_sem,
        got_sem,
        out_sem,
    ) = refs
    me = lax.axis_index("head")
    width, ff_width = up_buf.shape
    loads = [
        pltpu.make_async_copy(up_ref, up_buf, load_sem.at[0]),
        pltpu.make_async_copy(down_ref, down_buf, load_sem.at[1]),
    ]
    if not is_forward:
        loads.append(pltpu.make_async_copy(side_ref, pre_buf, load_sem.at[2]))
    for copy in loads:
        copy.start()
    group_barrier(me, count)

    def push(slot):
        return pltpu.make_async_remote_copy(
            src_ref=x_ref,
            dst_ref=land.at[slot],
            send_sem=send_sem.at[slot],
            recv_sem=recv_sem.at[slot],
            device_id={"head": group_peer(me, count, slot, 1)},
            device_id_type=MESH,
        )

    def give_back(slot):
        return pltpu.make_async_remote_copy(
            src_ref=part_buf.at[slot],
            dst_ref=got.at[slot],
            send_sem=back_sem.at[slot],
            recv_sem=got_sem.at[slot],
            device_id={"head": group_peer(me, count, slot, -1)},
            device_id_type=MESH,
        )

    def outs(slot):
        copies = [
            pltpu.make_async_copy(land.at[slot], rows_ref.at[slot], out_sem.at[0, slot]),
            pltpu.make_async_copy(mid_buf.at[slot], mid_ref.at[slot], out_sem.at[1, slot]),
        ]
        if is_forward:
            copies.append(
                pltpu.make_async_copy(pre_buf.at[slot], pre_ref.at[slot], out_sem.at[2, slot])
            )
        return copies

    for slot in range(1, count):
        push(slot).start()
    land[0] = x_ref[...]
    for copy in loads:
        copy.wait()

    def work(slot, carry):
        @pl.when(slot > 0)
        def _():
            push(slot).wait_recv()

        def hidden(index, inner):
            span = pl.ds(pl.multiple_of(index * WIDE, WIDE), WIDE)
            if is_forward:
                pre = nn(land[slot], up_buf[:, span]) + side_ref[:, span]
                pre_buf[slot, :, span] = pre.astype(jnp.bfloat16)
                mid_buf[slot, :, span] = gelu(pre).astype(jnp.bfloat16)
            else:
                grad = nt(land[slot], down_buf[span, :])
                slope = gelu_slope(pre_buf[slot, :, span].astype(jnp.float32))
                mid_buf[slot, :, span] = (grad * slope).astype(jnp.bfloat16)
            return inner

        def result(index, inner):
            span = pl.ds(pl.multiple_of(index * WIDE, WIDE), WIDE)
            if is_forward:
                part = nn(mid_buf[slot], down_buf[:, span])
            else:
                part = nt(mid_buf[slot], up_buf[span, :])

            @pl.when(slot == 0)
            def _():
                sum_ref[:, span] = part

            @pl.when(slot > 0)
            def _():
                part_buf[slot, :, span] = part.astype(jnp.bfloat16)

            return inner

        lax.fori_loop(0, ff_width // WIDE, hidden, 0)
        for copy in outs(slot):
            copy.start()
        lax.fori_loop(0, width // WIDE, result, 0)

        @pl.when(slot > 0)
        def _():
            give_back(slot).start()

        return carry

    lax.fori_loop(0, count, work, 0)

    def add(slot, carry):
        give_back(slot).wait_recv()
        sum_ref[...] += got[slot].astype(jnp.float32)
        return carry

    lax.fori_loop(1, count, add, 0)
    for slot in range(count):
        for copy in outs(slot):
            copy.wait()
        if slot > 0:
            push(slot).wait_send()
            give_back(slot).wait_send()


def feed(x_rows, up_panel, down_panel, side, is_forward, count, collective_id):
    if count == 4:
        return square_feed(x_rows, up_panel, down_panel, side, is_forward, collective_id)
    rows, width = x_rows.shape
    ff_width = up_panel.shape[1]
    kind = jnp.bfloat16
    by_width = jax.ShapeDtypeStruct((count, rows, width), kind)
    by_ff = jax.ShapeDtypeStruct((count, rows, ff_width), kind)
    total = jax.ShapeDtypeStruct((rows, width), jnp.float32)
    out_shape = (by_width, by_ff, by_ff, total) if is_forward else (by_width, by_ff, total)
    return pl.pallas_call(
        functools.partial(feed_kernel, is_forward, count),
        out_shape=out_shape,
        in_specs=[IN_VMEM, ANY, ANY, IN_VMEM if is_forward else ANY],
        out_specs=(ANY,) * (len(out_shape) - 1) + (IN_VMEM,),
        scratch_shapes=[
            pltpu.VMEM((count, rows, width), kind),
            pltpu.VMEM(up_panel.shape, kind),
            pltpu.VMEM(down_panel.shape, kind),
            pltpu.VMEM((count, rows, ff_width), kind),
            pltpu.VMEM((count, rows, ff_width), kind),
            pltpu.VMEM((count, rows, width), kind),
            pltpu.VMEM((count, rows, width), kind),
            pltpu.SemaphoreType.DMA((3,)),
            pltpu.SemaphoreType.DMA((count,)),
            pltpu.SemaphoreType.DMA((count,)),
            pltpu.SemaphoreType.DMA((count,)),
            pltpu.SemaphoreType.DMA((count,)),
            pltpu.SemaphoreType.DMA((3, count)),
        ],
        compiler_params=pltpu.CompilerParams(
            collective_id=collective_id, has_side_effects=True, vmem_limit_bytes=VMEM_MOST
        ),
        cost_estimate=busy(90),
        name="feed_forward" if is_forward else "feed_backward",
    )(x_rows, up_panel, down_panel, side)


def square_places(me):
    far, near = me // 2, me % 2
    return far * 2 + 1 - near, (1 - far) * 2 + near


def square_barrier(me):
    barrier = pltpu.get_barrier_semaphore()
    for peer in square_places(me):
        pl.semaphore_signal(barrier, inc=1, device_id={"head": peer}, device_id_type=MESH)
    pl.semaphore_wait(barrier, 2)


def square_copy(source, target, sems, index, peer):
    return pltpu.make_async_remote_copy(
        src_ref=source,
        dst_ref=target,
        send_sem=sems.at[0, index],
        recv_sem=sems.at[1, index],
        device_id={"head": peer},
        device_id_type=MESH,
    )


def square_gather(me, rows, x_ref, land, at_target, at_self, sems):
    one, two = square_places(me)
    low, high = pl.ds(0, rows // 2), pl.ds(rows // 2, rows // 2)
    return (
        square_copy(x_ref.at[low], land.at[at_target[0], low], sems, 0, one),
        square_copy(x_ref.at[high], land.at[at_target[0], high], sems, 1, one),
        square_copy(x_ref.at[high], land.at[at_target[1], high], sems, 2, two),
        square_copy(x_ref.at[low], land.at[at_target[1], low], sems, 3, two),
        square_copy(land.at[at_self[0], low], land.at[at_target[2], low], sems, 4, two),
        square_copy(land.at[at_self[1], high], land.at[at_target[3], high], sems, 5, one),
    )


def square_sums(me, rows, part_buf, relay, got, sems):
    one, two = square_places(me)
    low, high = pl.ds(0, rows // 2), pl.ds(rows // 2, rows // 2)
    return (
        square_copy(part_buf.at[3, low], relay.at[0], sems, 0, one),
        square_copy(part_buf.at[3, high], relay.at[1], sems, 1, two),
        square_copy(part_buf.at[1, low], got.at[0, low], sems, 2, one),
        square_copy(part_buf.at[1, high], got.at[0, high], sems, 3, one),
        square_copy(part_buf.at[2, high], got.at[1, high], sems, 4, two),
        square_copy(part_buf.at[2, low], got.at[1, low], sems, 5, two),
    )


def square_finish(rows, sums, part_buf, relay, got, sum_ref):
    low, high = pl.ds(0, rows // 2), pl.ds(rows // 2, rows // 2)

    def join(slot, span, index):
        total = part_buf[slot, span, :].astype(jnp.float32) + relay[index].astype(jnp.float32)
        part_buf[slot, span, :] = total.astype(jnp.bfloat16)

    sums[1].wait_recv()
    join(1, high, 1)
    sums[3].start()
    sums[0].wait_recv()
    join(2, low, 0)
    sums[5].start()
    for index in (2, 4, 3, 5):
        sums[index].wait_recv()
    sum_ref[...] += got[0].astype(jnp.float32) + got[1].astype(jnp.float32)
    for copy in sums:
        copy.wait_send()


def square_rows_kernel(x_ref, rows_ref, own_sem, sems):
    me = lax.axis_index("head")
    one, two = square_places(me)
    own = pltpu.make_async_copy(x_ref, rows_ref.at[me], own_sem)
    own.start()
    square_barrier(me)
    copies = square_gather(
        me, x_ref.shape[0], x_ref, rows_ref, (me, me, one, two), (one, two), sems
    )
    for index in (0, 2, 1, 3):
        copies[index].start()
    copies[0].wait_recv()
    copies[4].start()
    copies[2].wait_recv()
    copies[5].start()
    for index in (1, 3, 4, 5):
        copies[index].wait_recv()
    for copy in copies:
        copy.wait_send()
    own.wait()


def square_rows(x_rows, collective_id):
    return pl.pallas_call(
        square_rows_kernel,
        out_shape=jax.ShapeDtypeStruct((4,) + x_rows.shape, x_rows.dtype),
        in_specs=[IN_VMEM],
        out_specs=ANY,
        scratch_shapes=[pltpu.SemaphoreType.DMA, pltpu.SemaphoreType.DMA((2, 6))],
        compiler_params=pltpu.CompilerParams(
            collective_id=collective_id, has_side_effects=True, vmem_limit_bytes=8 * 1024 * 1024
        ),
        cost_estimate=busy(36),
        name="square_rows",
    )(x_rows)


def square_project_kernel(x_ref, w_ref, sum_ref, part_buf, relay, got, sems):
    me = lax.axis_index("head")
    one, two = square_places(me)
    rows, width = sum_ref.shape
    square_barrier(me)
    sums = square_sums(me, rows, part_buf, relay, got, sems)

    def work(slot, origin):
        def result(index, carry):
            span = pl.ds(pl.multiple_of(index * WIDE, WIDE), WIDE)
            part = nn(x_ref[origin], w_ref[:, span])
            if slot == 0:
                sum_ref[:, span] = part
            else:
                part_buf[slot, :, span] = part.astype(jnp.bfloat16)
            return carry

        lax.fori_loop(0, width // WIDE, result, 0)

    work(3, 3 - me)
    sums[0].start()
    sums[1].start()
    work(1, one)
    sums[2].start()
    work(2, two)
    sums[4].start()
    work(0, me)
    square_finish(rows, sums, part_buf, relay, got, sum_ref)


def square_project(x_rows, weights, collective_id):
    _, rows, _ = x_rows.shape
    width = weights.shape[1]
    kind = jnp.bfloat16
    return pl.pallas_call(
        square_project_kernel,
        out_shape=jax.ShapeDtypeStruct((rows, width), jnp.float32),
        in_specs=[IN_VMEM, IN_VMEM],
        out_specs=IN_VMEM,
        scratch_shapes=[
            pltpu.VMEM((4, rows, width), kind),
            pltpu.VMEM((2, rows // 2, width), kind),
            pltpu.VMEM((2, rows, width), kind),
            pltpu.SemaphoreType.DMA((2, 6)),
        ],
        compiler_params=pltpu.CompilerParams(
            collective_id=collective_id, has_side_effects=True, vmem_limit_bytes=24 * 1024 * 1024
        ),
        cost_estimate=busy(45),
        name="square_project",
    )(x_rows, weights)


def square_feed_kernel(is_forward, x_ref, up_ref, down_ref, side_ref, *refs):
    if is_forward:
        rows_ref, mid_ref, pre_ref, sum_ref = refs[:4]
        refs = refs[4:]
    else:
        rows_ref, mid_ref, sum_ref = refs[:3]
        refs = refs[3:]
    land, up_buf, down_buf, mid_buf, pre_buf, part_buf, relay, got, load_sem, in_sems, sum_sems, out_sem = refs
    me = lax.axis_index("head")
    rows = x_ref.shape[0]
    width, ff_width = up_buf.shape
    loads = [
        pltpu.make_async_copy(up_ref, up_buf, load_sem.at[0]),
        pltpu.make_async_copy(down_ref, down_buf, load_sem.at[1]),
    ]
    if not is_forward:
        loads.append(pltpu.make_async_copy(side_ref, pre_buf, load_sem.at[2]))
    for copy in loads:
        copy.start()
    square_barrier(me)
    gathers = square_gather(me, rows, x_ref, land, (1, 2, 3, 3), (1, 2), in_sems)
    sums = square_sums(me, rows, part_buf, relay, got, sum_sems)

    def outs(slot):
        copies = [
            pltpu.make_async_copy(land.at[slot], rows_ref.at[slot], out_sem.at[0, slot]),
            pltpu.make_async_copy(mid_buf.at[slot], mid_ref.at[slot], out_sem.at[1, slot]),
        ]
        if is_forward:
            copies.append(
                pltpu.make_async_copy(pre_buf.at[slot], pre_ref.at[slot], out_sem.at[2, slot])
            )
        return copies

    def work(slot):
        def hidden(index, inner):
            span = pl.ds(pl.multiple_of(index * WIDE, WIDE), WIDE)
            if is_forward:
                pre = nn(land[slot], up_buf[:, span]) + side_ref[:, span]
                pre_buf[slot, :, span] = pre.astype(jnp.bfloat16)
                mid_buf[slot, :, span] = gelu(pre).astype(jnp.bfloat16)
            else:
                grad = nt(land[slot], down_buf[span, :])
                slope = gelu_slope(pre_buf[slot, :, span].astype(jnp.float32))
                mid_buf[slot, :, span] = (grad * slope).astype(jnp.bfloat16)
            return inner

        def result(index, inner):
            span = pl.ds(pl.multiple_of(index * WIDE, WIDE), WIDE)
            if is_forward:
                part = nn(mid_buf[slot], down_buf[:, span])
            else:
                part = nt(mid_buf[slot], up_buf[span, :])
            if slot == 0:
                sum_ref[:, span] = part
            else:
                part_buf[slot, :, span] = part.astype(jnp.bfloat16)
            return inner

        lax.fori_loop(0, ff_width // WIDE, hidden, 0)
        for copy in outs(slot):
            copy.start()
        lax.fori_loop(0, width // WIDE, result, 0)

    for index in (0, 2, 1, 3):
        gathers[index].start()
    land[0] = x_ref[...]
    for copy in loads:
        copy.wait()
    work(0)
    gathers[0].wait_recv()
    gathers[4].start()
    gathers[2].wait_recv()
    gathers[5].start()
    gathers[1].wait_recv()
    work(1)
    sums[2].start()
    gathers[3].wait_recv()
    work(2)
    sums[4].start()
    gathers[4].wait_recv()
    gathers[5].wait_recv()
    work(3)
    sums[0].start()
    sums[1].start()
    square_finish(rows, sums, part_buf, relay, got, sum_ref)
    for copy in gathers:
        copy.wait_send()
    for slot in range(4):
        for copy in outs(slot):
            copy.wait()


def square_feed(x_rows, up_panel, down_panel, side, is_forward, collective_id):
    rows, width = x_rows.shape
    ff_width = up_panel.shape[1]
    kind = jnp.bfloat16
    by_width = jax.ShapeDtypeStruct((4, rows, width), kind)
    by_ff = jax.ShapeDtypeStruct((4, rows, ff_width), kind)
    total = jax.ShapeDtypeStruct((rows, width), jnp.float32)
    out_shape = (by_width, by_ff, by_ff, total) if is_forward else (by_width, by_ff, total)
    return pl.pallas_call(
        functools.partial(square_feed_kernel, is_forward),
        out_shape=out_shape,
        in_specs=[IN_VMEM, ANY, ANY, IN_VMEM if is_forward else ANY],
        out_specs=(ANY,) * (len(out_shape) - 1) + (IN_VMEM,),
        scratch_shapes=[
            pltpu.VMEM((4, rows, width), kind),
            pltpu.VMEM(up_panel.shape, kind),
            pltpu.VMEM(down_panel.shape, kind),
            pltpu.VMEM((4, rows, ff_width), kind),
            pltpu.VMEM((4, rows, ff_width), kind),
            pltpu.VMEM((4, rows, width), kind),
            pltpu.VMEM((2, rows // 2, width), kind),
            pltpu.VMEM((2, rows, width), kind),
            pltpu.SemaphoreType.DMA((3,)),
            pltpu.SemaphoreType.DMA((2, 6)),
            pltpu.SemaphoreType.DMA((2, 6)),
            pltpu.SemaphoreType.DMA((3, 4)),
        ],
        compiler_params=pltpu.CompilerParams(
            collective_id=collective_id, has_side_effects=True, vmem_limit_bytes=VMEM_MOST
        ),
        cost_estimate=busy(80),
        name="square_forward" if is_forward else "square_backward",
    )(x_rows, up_panel, down_panel, side)


def start_kernel(count, chips, x_ref, w_ref, rows_ref, panel_ref, own_sem, row_sems, line_sems, pair_sems):
    me, place = lax.axis_index("head"), lax.axis_index("seq")
    chip, core = place // PAIR, place % PAIR
    sibling = chip * PAIR + (1 - core)
    neighbours = ((chip + 1) * PAIR + core, (chip - 1) * PAIR + core)
    has_next = (chip < chips - 1, chip > 0)
    owns = [
        pltpu.make_async_copy(x_ref, rows_ref.at[me], own_sem.at[0]),
        pltpu.make_async_copy(w_ref, panel_ref.at[place], own_sem.at[1]),
    ]
    for copy in owns:
        copy.start()

    barrier = pltpu.get_barrier_semaphore()
    for slot in range(1, count):
        pl.semaphore_signal(
            barrier, inc=1, device_id={"head": group_peer(me, count, slot, 1)}, device_id_type=MESH
        )
    pl.semaphore_signal(barrier, inc=1, device_id={"seq": sibling}, device_id_type=MESH)
    for way in range(2):

        @pl.when(has_next[way])
        def _():
            pl.semaphore_signal(
                barrier, inc=1, device_id={"seq": neighbours[way]}, device_id_type=MESH
            )

    ends = (chip == 0).astype(jnp.int32) + (chip == chips - 1).astype(jnp.int32)
    pl.semaphore_wait(barrier, count - 1 + 3 - ends)

    pushes = []
    for slot in range(1, count):
        pushes.append(
            pltpu.make_async_remote_copy(
                src_ref=x_ref,
                dst_ref=rows_ref.at[me],
                send_sem=row_sems.at[0, slot],
                recv_sem=row_sems.at[1, slot],
                device_id={"head": group_peer(me, count, slot, 1)},
                device_id_type=MESH,
            )
        )

    def relay(way, step):
        origin = chip - step if way == 0 else chip + step
        block = panel_ref.at[origin * PAIR + core]
        return pltpu.make_async_remote_copy(
            src_ref=w_ref if step == 0 else block,
            dst_ref=block,
            send_sem=line_sems.at[0, way, step],
            recv_sem=line_sems.at[1, way, step],
            device_id={"seq": neighbours[way]},
            device_id_type=MESH,
        )

    def share(way, step):
        origin = chip - 1 - step if way == 0 else chip + 1 + step
        if way == 2:
            origin = chip
        block = panel_ref.at[origin * PAIR + core]
        return pltpu.make_async_remote_copy(
            src_ref=w_ref if way == 2 else block,
            dst_ref=block,
            send_sem=pair_sems.at[0, way, step],
            recv_sem=pair_sems.at[1, way, step],
            device_id={"seq": sibling},
            device_id_type=MESH,
        )

    def sends(way, step):
        behind = chip >= step if way == 0 else chip + step <= chips - 1
        return has_next[way] & behind

    def receives(way, step):
        return chip - 1 - step >= 0 if way == 0 else chip + 1 + step <= chips - 1

    for way in range(2):
        pl.when(sends(way, 0))(relay(way, 0).start)
    for copy in pushes:
        copy.start()
    share(2, 0).start()
    for step in range(chips - 1):
        for way in range(2):

            @pl.when(receives(way, step))
            def _():
                relay(way, step).wait_recv()
                if step + 1 < chips - 1:
                    pl.when(sends(way, step + 1))(relay(way, step + 1).start)
                share(way, step).start()

    for copy in owns + pushes:
        copy.wait()
    share(2, 0).wait()
    for step in range(chips - 1):
        for way in range(2):
            pl.when(sends(way, step))(relay(way, step).wait_send)
            pl.when(receives(way, step))(share(way, step).wait)


def start_gathers(x_rows, w_rows, head_count, seq_size, collective_id):
    chips = seq_size // PAIR
    return pl.pallas_call(
        functools.partial(start_kernel, head_count, chips),
        out_shape=(
            jax.ShapeDtypeStruct((head_count,) + x_rows.shape, x_rows.dtype),
            jax.ShapeDtypeStruct((seq_size,) + w_rows.shape, w_rows.dtype),
        ),
        in_specs=[IN_VMEM, IN_VMEM],
        out_specs=(ANY, ANY),
        scratch_shapes=[
            pltpu.SemaphoreType.DMA((2,)),
            pltpu.SemaphoreType.DMA((2, head_count)),
            pltpu.SemaphoreType.DMA((2, 2, chips)),
            pltpu.SemaphoreType.DMA((2, 3, chips)),
        ],
        compiler_params=pltpu.CompilerParams(
            collective_id=collective_id, has_side_effects=True, vmem_limit_bytes=16 * 1024 * 1024
        ),
        cost_estimate=busy(60),
        name="start_gathers",
    )(x_rows, w_rows)


def normalize(z_rows, gain, shift):
    average = jnp.mean(z_rows, axis=-1, keepdims=True)
    centered = z_rows - average
    variance = jnp.mean(centered * centered, axis=-1, keepdims=True)
    recip = lax.rsqrt(variance + NORM_EPS)
    normed = centered * recip
    return (normed * gain + shift, normed, recip)


def normalize_back(grad_rows, normed, recip, gain):
    scaled = grad_rows * gain
    dz_rows = recip * (
        scaled
        - jnp.mean(scaled, axis=-1, keepdims=True)
        - normed * jnp.mean(scaled * normed, axis=-1, keepdims=True)
    )
    return (dz_rows, jnp.sum(grad_rows * normed, axis=0), jnp.sum(grad_rows, axis=0))


def group_rows(rows_low):
    return lax.all_gather(rows_low, "head", axis=0, tiled=True)


def group_sums(partial_value):
    return lax.psum_scatter(
        partial_value.astype(jnp.bfloat16), "head", scatter_dimension=0, tiled=True
    ).astype(jnp.float32)


def adam_step(param, grad, moment, second, step_float):
    moment_new = 0.9 * moment + 0.1 * grad
    second_new = 0.999 * second + 0.001 * grad * grad
    fix_one = 1.0 - jnp.power(jnp.float32(0.9), step_float)
    fix_two = 1.0 - jnp.power(jnp.float32(0.999), step_float)
    update = ADAM_RATE * (moment_new / fix_one) / (jnp.sqrt(second_new / fix_two) + 1e-08)
    return (param - update, moment_new, second_new)


def shards(
    hidden_in,
    cotangent,
    lengths,
    token_order,
    own_map,
    w_query,
    w_key,
    w_value,
    w_out,
    w_up,
    w_down,
    gains,
    biases,
    up_bias,
    vector_moment,
    vector_second,
    bias_moment,
    bias_second,
    step_count,
    stat_left,
    stat_right,
    root_left,
    root_right,
    master,
):
    head_count = lax.axis_size("head")
    seq_size = lax.axis_size("seq")
    head_index = lax.axis_index("head")
    group_index = lax.axis_index("seq")
    tok_count = hidden_in.shape[0]
    width = hidden_in.shape[1]
    panel_width = w_query.shape[1]
    ff_width = w_up.shape[1]
    seq_count = lengths.shape[0]
    heads = panel_width // HDIM
    parts = seq_size // heads
    runs = token_order.shape[0] // RUN
    aligned = seq_count == 2
    tile = 1024 if aligned else RUN
    setup = (parts, tile, seq_count, aligned, runs)
    tables = stream_tables(token_order, lengths, head_count, seq_size, tile, group_index % parts)
    own_block = head_index * seq_size + group_index
    order_here = lax.dynamic_slice_in_dim(token_order, own_block * tok_count, tok_count, 0)
    valid_here = order_here < tables[3][seq_count - 1]
    inputs_f32 = hidden_in.astype(jnp.float32)

    inputs_grp, qkv_panel = start_gathers(
        hidden_in, jnp.concatenate([w_query, w_key, w_value], axis=1), head_count, seq_size, 7
    )
    inputs_grp = inputs_grp.reshape(head_count * tok_count, width)
    qkv_panel = qkv_panel.reshape(width, 3 * panel_width)
    o_panel = lax.all_gather(w_out, "seq", axis=1, tiled=True)
    up_panel = lax.all_gather(w_up, "seq", axis=0, tiled=True)
    down_panel = lax.all_gather(w_down, "seq", axis=1, tiled=True)

    def own_columns(row):
        return lax.dynamic_slice_in_dim(row, head_index * panel_width, panel_width, 0)

    qkv_bias = jnp.concatenate(
        [own_columns(biases[0]), jnp.zeros((panel_width,), jnp.float32), own_columns(biases[1])]
    )
    qkv_grp = (
        jnp.dot(inputs_grp, qkv_panel, preferred_element_type=jnp.float32) + qkv_bias
    ).astype(jnp.bfloat16)
    qkv_head = spread(qkv_grp, 3, heads, parts, seq_size, 0)
    qkv_head = qkv_head.reshape(3, runs, RUN, HDIM)
    attended_part, attended_exact, log_total = attend_forward(qkv_head, tables, setup)
    rows_grp = head_count * tok_count
    attended_grp = collect(
        attended_part.reshape(1, seq_size, rows_grp, HDIM), heads, parts, 1
    )
    if head_count == 4:
        branch_out = square_project(
            attended_grp.reshape(head_count, tok_count, panel_width), o_panel, 8
        )
    else:
        branch_out = group_sums(
            jnp.dot(attended_grp, o_panel, preferred_element_type=jnp.float32)
        )
    z_one = inputs_f32 + branch_out + biases[2]
    h_one, normed_one, recip_one = normalize(z_one, gains[0], biases[3])
    h_low = h_one.astype(jnp.bfloat16)
    h_grp, act, pre_act, ff_out = feed(
        h_low, up_panel, down_panel, up_bias.reshape(1, ff_width), True, head_count, 5
    )
    z_two = h_one + ff_out + biases[4]
    layer_f32, normed_two, recip_two = normalize(z_two, gains[1], biases[5])
    layer_out = layer_f32.astype(jnp.bfloat16)
    grad_y = cotangent.astype(jnp.float32) * valid_here[:, None].astype(jnp.float32)
    dz_two, dgain_two, dshift_two = normalize_back(grad_y, normed_two, recip_two, gains[1])
    dbias_down = jnp.sum(dz_two, axis=0)
    dz_two_grp, dpre, dh_part = feed(
        dz_two.astype(jnp.bfloat16), up_panel, down_panel, pre_act, False, head_count, 6
    )
    h_grp, act, dz_two_grp, dpre = (
        array.reshape(rows_grp, array.shape[2]) for array in (h_grp, act, dz_two_grp, dpre)
    )
    up_bias_part = jnp.sum(dpre.astype(jnp.float32), axis=0)
    dh_one = dz_two + dh_part
    dz_one, dgain_one, dshift_one = normalize_back(dh_one, normed_one, recip_one, gains[0])
    dbias_out = jnp.sum(dz_one, axis=0)
    dz_one_low = dz_one.astype(jnp.bfloat16)
    if head_count == 4:
        dz_one_grp = square_rows(dz_one_low, 9).reshape(rows_grp, width)
    else:
        dz_one_grp = group_rows(dz_one_low)
    dattended = jnp.dot(dz_one_grp, o_panel.T, preferred_element_type=jnp.float32).astype(
        jnp.bfloat16
    )
    dattended_head = spread(dattended, 1, heads, parts, seq_size, 2).reshape(runs, RUN, HDIM)
    dqkv_part = attend_backward(
        qkv_head, dattended_head, attended_exact, log_total, tables, setup
    )
    dqkv_grp = collect(dqkv_part.reshape(3, seq_size, rows_grp, HDIM), heads, parts, 3)
    input_grad = dz_one + group_sums(
        jnp.dot(dqkv_grp, qkv_panel.T, preferred_element_type=jnp.float32)
    )
    bias_qkv = jnp.sum(dqkv_grp.astype(jnp.float32), axis=0)
    zero_width = jnp.zeros((width,), jnp.float32)
    dbias_query = lax.dynamic_update_slice_in_dim(
        zero_width, bias_qkv[:panel_width], head_index * panel_width, 0
    )
    dbias_value = lax.dynamic_update_slice_in_dim(
        zero_width, bias_qkv[2 * panel_width :], head_index * panel_width, 0
    )
    local_vectors = jnp.stack(
        (
            dbias_query,
            dbias_value,
            dbias_out,
            dshift_one,
            dbias_down,
            dshift_two,
            dgain_one,
            dgain_two,
        )
    )
    packed = jnp.concatenate([local_vectors.reshape(-1), up_bias_part])
    packed_all = lax.all_gather(packed, ("head", "seq"))
    vector_grad = jnp.sum(packed_all[:, : 8 * width], axis=0).reshape(8, width)
    up_bias_grad = jnp.sum(
        lax.dynamic_slice_in_dim(packed_all[:, 8 * width :], head_index * seq_size, seq_size, 0),
        axis=0,
    )
    left_index, right_index = block_operands(own_map[0], width, panel_width, ff_width)
    low_grads = owned_grads(
        left_index,
        right_index,
        (inputs_grp, attended_grp, h_grp, act),
        (dqkv_grp, dz_one_grp, dpre, dz_two_grp),
        seq_size,
        4,
    )
    block_grads = low_grads.astype(jnp.float32)
    stat_left_new = 0.5 * stat_left + 0.5 * jnp.einsum(
        "bij,bkj->bik", low_grads, low_grads, preferred_element_type=jnp.float32
    )
    stat_right_new = 0.5 * stat_right + 0.5 * jnp.einsum(
        "bji,bjk->bik", low_grads, low_grads, preferred_element_type=jnp.float32
    )
    left_mix = jnp.einsum(
        "bij,bjk->bik",
        root_left.astype(jnp.bfloat16),
        low_grads,
        preferred_element_type=jnp.float32,
    )
    direction = jnp.einsum(
        "bij,bjk->bik",
        left_mix.astype(jnp.bfloat16),
        root_right.astype(jnp.bfloat16),
        preferred_element_type=jnp.float32,
    )
    master_new = master - SHAMPOO_RATE * direction
    step_float = step_count[0].astype(jnp.float32)
    vector_params = jnp.concatenate([biases, gains], axis=0)
    vector_new, vector_moment_new, vector_second_new = adam_step(
        vector_params, vector_grad, vector_moment, vector_second, step_float
    )
    up_bias_new, bias_moment_new, bias_second_new = adam_step(
        up_bias, up_bias_grad, bias_moment, bias_second, step_float
    )
    return (
        layer_out,
        input_grad,
        block_grads,
        stat_left_new,
        stat_right_new,
        master_new,
        vector_new[0:6],
        vector_new[6:8],
        up_bias_new,
        vector_grad,
        vector_moment_new,
        vector_second_new,
        up_bias_grad,
        bias_moment_new,
        bias_second_new,
    )


def solution(mesh):
    rows = P(("head", "seq"), None)
    blocks = P(("head", "seq"), None, None)
    in_specs = (
        rows,
        rows,
        P(),
        P(),
        P("head", None),
        P("seq", "head"),
        P("seq", "head"),
        P("seq", "head"),
        P("head", "seq"),
        P("seq", "head"),
        P("head", "seq"),
        P(),
        P(),
        P("head"),
        P(),
        P(),
        P("head"),
        P("head"),
        P(),
        blocks,
        blocks,
        blocks,
        blocks,
        blocks,
    )
    out_specs = (
        rows,
        rows,
        blocks,
        blocks,
        blocks,
        blocks,
        P(),
        P(),
        P("head"),
        P(),
        P(),
        P(),
        P("head"),
        P("head"),
        P("head"),
    )
    return jax.shard_map(shards, mesh=mesh, in_specs=in_specs, out_specs=out_specs, check_vma=False)
```

```python
import functools
import math

import jax
import jax.numpy as jnp
from jax import lax
from jax.experimental import pallas as pl
from jax.experimental.pallas import tpu as pltpu
from jax.sharding import PartitionSpec as P


HDIM = 128
BLOCK = 256
RUN = 256

NEG_LARGE = -1e30
NORM_EPS = 1e-12
ADAM_RATE = 0.4
SHAMPOO_RATE = 0.15
MESH = pl.DeviceIdType.MESH
VMEM_MOST = 60 * 1024 * 1024

ANY = pl.BlockSpec(memory_space=pl.ANY)
IN_SMEM = pl.BlockSpec(memory_space=pltpu.SMEM)
IN_VMEM = pl.BlockSpec(memory_space=pltpu.VMEM)


def busy(microseconds):
    return pl.CostEstimate(
        flops=microseconds * 800_000_000, bytes_accessed=1_000_000, transcendentals=0
    )


def seq_barrier(me, heads, parts):
    own_head, own_part = me // parts, me % parts
    barrier = pltpu.get_barrier_semaphore()
    for step in range(1, heads):
        pl.semaphore_signal(
            barrier,
            inc=1,
            device_id={"seq": (own_head + step) % heads * parts + own_part},
            device_id_type=MESH,
        )
    for step in range(1, parts):
        pl.semaphore_signal(
            barrier,
            inc=1,
            device_id={"seq": own_head * parts + (own_part + step) % parts},
            device_id_type=MESH,
        )
    pl.semaphore_wait(barrier, heads - 1 + parts - 1)


def spread_kernel(
    fields, heads, parts, x_ref, y_ref, own_sem, send_sem, recv_sem, pass_sem, take_sem
):
    me = lax.axis_index("seq")
    own_head, own_part = me // parts, me % parts
    seq_barrier(me, heads, parts)

    def columns(field, head):
        return pl.ds(pl.multiple_of((field * heads + head) * HDIM, HDIM), HDIM)

    sends = []
    for step in range(1, heads):
        head = (own_head + step) % heads
        for field in range(fields):
            copy = pltpu.make_async_remote_copy(
                src_ref=x_ref.at[:, columns(field, head)],
                dst_ref=y_ref.at[field, me],
                send_sem=send_sem.at[step - 1, field],
                recv_sem=recv_sem.at[step - 1, field],
                device_id={"seq": head * parts + own_part},
                device_id_type=MESH,
            )
            copy.start()
            sends.append(copy)
    owns = []
    for field in range(fields):
        copy = pltpu.make_async_copy(
            x_ref.at[:, columns(field, own_head)], y_ref.at[field, me], own_sem.at[field]
        )
        copy.start()
        owns.append(copy)
    passes = []

    def pass_on(step, field, source):
        origin = (own_head - step + heads) % heads * parts + own_part
        for other in range(1, parts):
            copy = pltpu.make_async_remote_copy(
                src_ref=source,
                dst_ref=y_ref.at[field, origin],
                send_sem=pass_sem.at[other - 1, step, field],
                recv_sem=take_sem.at[other - 1, step, field],
                device_id={"seq": own_head * parts + (own_part + other) % parts},
                device_id_type=MESH,
            )
            copy.start()
            passes.append(copy)

    for field in range(fields):
        pass_on(0, field, x_ref.at[:, columns(field, own_head)])
    for step in range(1, heads):
        origin = (own_head - step + heads) % heads * parts + own_part
        for field in range(fields):
            sends[(step - 1) * fields + field].wait_recv()
            pass_on(step, field, y_ref.at[field, origin])
    for copy in owns:
        copy.wait()
    for copy in sends:
        copy.wait_send()
    for copy in passes:
        copy.wait()


def spread(x_rows, fields, heads, parts, seq_size, collective_id):
    rows = x_rows.shape[0]
    return pl.pallas_call(
        functools.partial(spread_kernel, fields, heads, parts),
        out_shape=jax.ShapeDtypeStruct((fields, seq_size, rows, HDIM), x_rows.dtype),
        in_specs=[IN_VMEM],
        out_specs=ANY,
        scratch_shapes=[
            pltpu.SemaphoreType.DMA((fields,)),
            pltpu.SemaphoreType.DMA((max(heads - 1, 1), fields)),
            pltpu.SemaphoreType.DMA((max(heads - 1, 1), fields)),
            pltpu.SemaphoreType.DMA((max(parts - 1, 1), heads, fields)),
            pltpu.SemaphoreType.DMA((max(parts - 1, 1), heads, fields)),
        ],
        compiler_params=pltpu.CompilerParams(
            collective_id=collective_id, has_side_effects=True, vmem_limit_bytes=24 * 1024 * 1024
        ),
        cost_estimate=busy(fields * 24),
        name="spread",
    )(x_rows)


def collect_kernel(
    fields,
    heads,
    parts,
    x_ref,
    y_ref,
    own,
    got,
    ready,
    own_sem,
    pass_sem,
    take_sem,
    send_sem,
    recv_sem,
    keep_sem,
):
    me = lax.axis_index("seq")
    own_head, own_part = me // parts, me % parts
    seq_barrier(me, heads, parts)
    order = list(range(1, heads)) + [0]

    def home(step, part):
        return (own_head + step) % heads * parts + part

    passes, owns = {}, {}
    for step in order:
        for field in range(fields):
            for other in range(1, parts):
                part = (own_part + other) % parts
                copy = pltpu.make_async_remote_copy(
                    src_ref=x_ref.at[field, home(step, part)],
                    dst_ref=got.at[other - 1, step, field],
                    send_sem=pass_sem.at[other - 1, step, field],
                    recv_sem=take_sem.at[other - 1, step, field],
                    device_id={"seq": own_head * parts + part},
                    device_id_type=MESH,
                )
                copy.start()
                passes[step, field, other] = copy
            copy = pltpu.make_async_copy(
                x_ref.at[field, home(step, own_part)], own.at[step, field], own_sem.at[step, field]
            )
            copy.start()
            owns[step, field] = copy

    sends = []
    for step in order:
        for field in range(fields):
            owns[step, field].wait()
            for other in range(1, parts):
                passes[step, field, other].wait_recv()
            total = own[step, field].astype(jnp.float32)
            for other in range(1, parts):
                total = total + got[other - 1, step, field].astype(jnp.float32)
            ready[step, field] = total.astype(ready.dtype)
            columns = pl.ds(pl.multiple_of((field * heads + own_head) * HDIM, HDIM), HDIM)
            if step == 0:
                copy = pltpu.make_async_copy(
                    ready.at[step, field], y_ref.at[:, columns], keep_sem.at[field]
                )
            else:
                copy = pltpu.make_async_remote_copy(
                    src_ref=ready.at[step, field],
                    dst_ref=y_ref.at[:, columns],
                    send_sem=send_sem.at[step - 1, field],
                    recv_sem=recv_sem.at[step - 1, field],
                    device_id={"seq": home(step, own_part)},
                    device_id_type=MESH,
                )
            copy.start()
            sends.append(copy)
    for copy in sends:
        copy.wait()
    for copy in passes.values():
        copy.wait_send()


def collect(x_parts, heads, parts, collective_id):
    fields, _, rows, _ = x_parts.shape
    kind = x_parts.dtype
    few = max(parts - 1, 1)
    return pl.pallas_call(
        functools.partial(collect_kernel, fields, heads, parts),
        out_shape=jax.ShapeDtypeStruct((rows, fields * heads * HDIM), kind),
        in_specs=[ANY],
        out_specs=ANY,
        scratch_shapes=[
            pltpu.VMEM((heads, fields, rows, HDIM), kind),
            pltpu.VMEM((few, heads, fields, rows, HDIM), kind),
            pltpu.VMEM((heads, fields, rows, HDIM), kind),
            pltpu.SemaphoreType.DMA((heads, fields)),
            pltpu.SemaphoreType.DMA((few, heads, fields)),
            pltpu.SemaphoreType.DMA((few, heads, fields)),
            pltpu.SemaphoreType.DMA((max(heads - 1, 1), fields)),
            pltpu.SemaphoreType.DMA((max(heads - 1, 1), fields)),
            pltpu.SemaphoreType.DMA((fields,)),
        ],
        compiler_params=pltpu.CompilerParams(
            collective_id=collective_id, has_side_effects=True, vmem_limit_bytes=VMEM_MOST
        ),
        cost_estimate=busy(fields * 24),
        name="collect",
    )(x_parts)


def allowed_tile(ends_ref, seq_count, key_low, query_low, shape):
    key_pos = key_low + lax.broadcasted_iota(jnp.int32, shape, 0)
    query_pos = query_low + lax.broadcasted_iota(jnp.int32, shape, 1)
    key_seg = jnp.zeros(shape, jnp.int32)
    query_seg = jnp.zeros(shape, jnp.int32)
    for index in range(seq_count):
        key_seg += (key_pos >= ends_ref[index]).astype(jnp.int32)
        query_seg += (query_pos >= ends_ref[index]).astype(jnp.int32)
    last = ends_ref[seq_count - 1]
    key_seg = jnp.where(key_pos < last, key_seg, seq_count + key_pos)
    query_seg = jnp.where(query_pos < last, query_seg, seq_count + query_pos)
    return key_seg == query_seg


def nt(left, right):
    return lax.dot_general(
        left, right, (((1,), (1,)), ((), ())), preferred_element_type=jnp.float32
    )


def nn(left, right):
    return lax.dot_general(
        left, right, (((1,), (0,)), ((), ())), preferred_element_type=jnp.float32
    )


def forward_kernel(
    setup,
    where_ref,
    low_ref,
    high_ref,
    ends_ref,
    part_ref,
    qkv_ref,
    out_ref,
    exact_ref,
    log_ref,
    q_buf,
    k_buf,
    v_buf,
    vt_buf,
    sem,
):
    parts, tile, seq_count, aligned, runs = setup
    turn = pl.program_id(0)
    part = part_ref[0]
    scale2 = math.log2(math.e) / math.sqrt(HDIM)

    @pl.when(turn == 0)
    def _():
        def fetch(field, run, buf, slot):
            return pltpu.make_async_copy(
                qkv_ref.at[field, where_ref[run]],
                buf.at[pl.ds(pl.multiple_of(slot * RUN, RUN), RUN), :],
                sem.at[field],
            )

        def start(run, carry):
            fetch(1, run, k_buf, run).start()
            fetch(2, run, v_buf, run).start()
            return carry

        def start_own(index, carry):
            fetch(0, index * parts + part, q_buf, index).start()
            return carry

        def finish(run, carry):
            fetch(1, run, k_buf, run).wait()
            fetch(2, run, v_buf, run).wait()
            return carry

        def finish_own(index, carry):
            fetch(0, index * parts + part, q_buf, index).wait()
            return carry

        lax.fori_loop(0, runs, start, 0)
        lax.fori_loop(0, runs // parts, start_own, 0)
        out_ref[...] = jnp.zeros_like(out_ref)
        lax.fori_loop(0, runs, finish, 0)
        lax.fori_loop(0, runs // parts, finish_own, 0)
        if aligned:

            def turn_tile(index, carry):
                low = pl.multiple_of(index * RUN, RUN)
                vt_buf[:, pl.ds(low, RUN)] = v_buf[pl.ds(low, RUN), :].T
                return carry

            lax.fori_loop(0, runs, turn_tile, 0)

    run = turn * parts + part
    place = where_ref[run]
    queries = q_buf[pl.ds(pl.multiple_of(turn * RUN, RUN), RUN), :]

    def attend():
        def key_step(index, carry):
            top, total, acc = carry
            low = pl.multiple_of(index * tile, tile)
            scores = nt(k_buf[pl.ds(low, tile), :], queries)
            if not aligned:
                allowed = allowed_tile(ends_ref, seq_count, low, run * RUN, scores.shape)
                scores = jnp.where(allowed, scores, NEG_LARGE)
            new_top = jnp.maximum(top, jnp.max(scores, axis=0, keepdims=True))
            prob = jnp.exp2((scores - new_top) * scale2)
            if not aligned:
                prob = jnp.where(allowed, prob, 0.0)
            fade = jnp.exp2((top - new_top) * scale2)
            total = total * fade + jnp.sum(prob, axis=0, keepdims=True)
            if aligned:
                turned = vt_buf[:, pl.ds(low, tile)]
            else:
                turned = v_buf[pl.ds(low, tile), :].T
            acc = acc * fade + nn(turned, prob.astype(jnp.bfloat16))
            return new_top, total, acc

        top, total, acc = lax.fori_loop(
            low_ref[run],
            high_ref[run],
            key_step,
            (
                jnp.full((1, RUN), NEG_LARGE, jnp.float32),
                jnp.zeros((1, RUN), jnp.float32),
                jnp.zeros((HDIM, RUN), jnp.float32),
            ),
        )
        result = (acc / total).T
        exact_ref[0] = result
        out_ref[place] = result.astype(out_ref.dtype)
        log_ref[0] = top * scale2 + jnp.log2(total)

    if aligned:
        is_valid = run * RUN < ends_ref[seq_count - 1]
        pl.when(is_valid)(attend)

        @pl.when(jnp.logical_not(is_valid))
        def _():
            values = v_buf[pl.ds(pl.multiple_of(run * RUN, RUN), RUN), :]
            exact_ref[0] = values.astype(jnp.float32)
            out_ref[place] = values
            log_ref[0] = jnp.zeros((1, RUN), jnp.float32)
    else:
        attend()


def attend_forward(qkv, tables, setup):
    parts, _, _, aligned, runs = setup
    own = runs // parts
    rows = runs * RUN
    return pl.pallas_call(
        functools.partial(forward_kernel, setup),
        grid=(own,),
        out_shape=(
            jax.ShapeDtypeStruct((runs, RUN, HDIM), jnp.bfloat16),
            jax.ShapeDtypeStruct((own, RUN, HDIM), jnp.float32),
            jax.ShapeDtypeStruct((own, 1, RUN), jnp.float32),
        ),
        in_specs=[IN_SMEM] * 5 + [ANY],
        out_specs=(
            pl.BlockSpec((runs, RUN, HDIM), lambda i: (0, 0, 0), pipeline_mode=pl.Buffered(1)),
            pl.BlockSpec((1, RUN, HDIM), lambda i: (i, 0, 0)),
            pl.BlockSpec((1, 1, RUN), lambda i: (i, 0, 0)),
        ),
        scratch_shapes=[
            pltpu.VMEM((own * RUN, HDIM), jnp.bfloat16),
            pltpu.VMEM((rows, HDIM), jnp.bfloat16),
            pltpu.VMEM((rows, HDIM), jnp.bfloat16),
            pltpu.VMEM((HDIM, rows if aligned else RUN), jnp.bfloat16),
            pltpu.SemaphoreType.DMA((3,)),
        ],
        compiler_params=pltpu.CompilerParams(
            dimension_semantics=("arbitrary",), vmem_limit_bytes=VMEM_MOST
        ),
        cost_estimate=busy(36),
        name="attend_forward",
    )(*tables, qkv)


def backward_kernel(
    setup,
    where_ref,
    low_ref,
    high_ref,
    ends_ref,
    part_ref,
    qkv_ref,
    grad_ref,
    exact_ref,
    log_ref,
    out_ref,
    q_buf,
    k_buf,
    v_buf,
    kt_buf,
    g_buf,
    dk_acc,
    dv_acc,
    stage,
    sem,
    out_sem,
):
    parts, tile, seq_count, aligned, runs = setup
    own = runs // parts
    turn = pl.program_id(0)
    part = part_ref[0]
    scale = 1.0 / math.sqrt(HDIM)
    scale2 = math.log2(math.e) * scale

    @pl.when(turn == 0)
    def _():
        def fetch(source, index, buf, slot, lane):
            return pltpu.make_async_copy(
                source.at[index],
                buf.at[pl.ds(pl.multiple_of(slot * RUN, RUN), RUN), :],
                sem.at[lane],
            )

        def pair(run):
            place = where_ref[run]
            return (
                fetch(qkv_ref.at[1], place, k_buf, run, 1),
                fetch(qkv_ref.at[2], place, v_buf, run, 2),
            )

        def own_pair(index):
            place = where_ref[index * parts + part]
            return (
                fetch(qkv_ref.at[0], place, q_buf, index, 0),
                fetch(grad_ref, place, g_buf, index, 3),
            )

        def start(run, carry):
            for copy in pair(run):
                copy.start()
            return carry

        def start_own(index, carry):
            for copy in own_pair(index):
                copy.start()
            return carry

        def finish(run, carry):
            for copy in pair(run):
                copy.wait()
            return carry

        def finish_own(index, carry):
            for copy in own_pair(index):
                copy.wait()
            return carry

        lax.fori_loop(0, runs, start, 0)
        lax.fori_loop(0, own, start_own, 0)
        dk_acc[...] = jnp.zeros_like(dk_acc)
        dv_acc[...] = jnp.zeros_like(dv_acc)
        lax.fori_loop(0, runs, finish, 0)
        lax.fori_loop(0, own, finish_own, 0)
        if aligned:

            def turn_tile(index, carry):
                low = pl.multiple_of(index * RUN, RUN)
                kt_buf[:, pl.ds(low, RUN)] = k_buf[pl.ds(low, RUN), :].T
                return carry

            lax.fori_loop(0, runs, turn_tile, 0)

    run = turn * parts + part
    low_row = pl.multiple_of(turn * RUN, RUN)

    def attend():
        queries = q_buf[pl.ds(low_row, RUN), :]
        grads = g_buf[pl.ds(low_row, RUN), :]
        delta = jnp.sum((grads.astype(jnp.float32) * exact_ref[0]).T, axis=0, keepdims=True)
        log_total = log_ref[0]

        def key_step(index, acc):
            low = pl.multiple_of(index * tile, tile)
            keys = k_buf[pl.ds(low, tile), :]
            values = v_buf[pl.ds(low, tile), :]
            scores = nt(keys, queries)
            prob = jnp.exp2(scores * scale2 - log_total)
            if not aligned:
                allowed = allowed_tile(ends_ref, seq_count, low, run * RUN, scores.shape)
                prob = jnp.where(allowed, prob, 0.0)
            prob_grad = nt(values, grads)
            dv_acc[pl.ds(low, tile), :] += nn(prob.astype(jnp.bfloat16), grads)
            score_grad = (prob * (prob_grad - delta)).astype(jnp.bfloat16)
            dk_acc[pl.ds(low, tile), :] += nn(score_grad, queries)
            turned = kt_buf[:, pl.ds(low, tile)] if aligned else keys.T
            return acc + nn(turned, score_grad)

        acc = lax.fori_loop(
            low_ref[run], high_ref[run], key_step, jnp.zeros((HDIM, RUN), jnp.float32)
        )
        q_buf[pl.ds(low_row, RUN), :] = (acc.T * scale).astype(jnp.bfloat16)

    if aligned:
        is_valid = run * RUN < ends_ref[seq_count - 1]
        pl.when(is_valid)(attend)

        @pl.when(jnp.logical_not(is_valid))
        def _():
            q_buf[pl.ds(low_row, RUN), :] = jnp.zeros((RUN, HDIM), jnp.bfloat16)
    else:
        attend()

    @pl.when(turn == own - 1)
    def _():
        def key_copies(run_index, slot):
            place = where_ref[run_index]
            return (
                pltpu.make_async_copy(stage.at[slot, 0], out_ref.at[1, place], out_sem.at[slot, 0]),
                pltpu.make_async_copy(stage.at[slot, 1], out_ref.at[2, place], out_sem.at[slot, 1]),
            )

        v_buf[pl.ds(0, RUN), :] = jnp.zeros((RUN, HDIM), jnp.bfloat16)

        def query_copy(run_index):
            mine = run_index % parts == part
            place = where_ref[run_index]
            index = jnp.where(mine, run_index // parts, 0)
            return mine, (
                pltpu.make_async_copy(
                    q_buf.at[pl.ds(pl.multiple_of(index * RUN, RUN), RUN), :],
                    out_ref.at[0, place],
                    sem.at[0],
                ),
                pltpu.make_async_copy(
                    v_buf.at[pl.ds(0, RUN), :], out_ref.at[0, place], sem.at[0]
                ),
            )

        def start_query(run_index, carry):
            mine, (copy, blank) = query_copy(run_index)
            pl.when(mine)(copy.start)
            pl.when(jnp.logical_not(mine))(blank.start)
            return carry

        def finish_query(run_index, carry):
            _, (copy, blank) = query_copy(run_index)
            blank.wait()
            return carry

        lax.fori_loop(0, runs, start_query, 0)

        def write(run_index, carry):
            slot = run_index % 2

            @pl.when(run_index >= 2)
            def _():
                for copy in key_copies(run_index - 2, slot):
                    copy.wait()

            low = pl.multiple_of(run_index * RUN, RUN)
            stage[slot, 0] = (dk_acc[pl.ds(low, RUN), :] * scale).astype(jnp.bfloat16)
            stage[slot, 1] = dv_acc[pl.ds(low, RUN), :].astype(jnp.bfloat16)
            for copy in key_copies(run_index, slot):
                copy.start()
            return carry

        lax.fori_loop(0, runs, write, 0)
        for back in (2, 1):
            for copy in key_copies(runs - back, (runs - back) % 2):
                copy.wait()
        lax.fori_loop(0, runs, finish_query, 0)


def attend_backward(qkv, grads, exact, log_total, tables, setup):
    parts, _, _, aligned, runs = setup
    own = runs // parts
    rows = runs * RUN
    return pl.pallas_call(
        functools.partial(backward_kernel, setup),
        grid=(own,),
        out_shape=jax.ShapeDtypeStruct((3, runs, RUN, HDIM), jnp.bfloat16),
        in_specs=[IN_SMEM] * 5
        + [
            ANY,
            ANY,
            pl.BlockSpec((1, RUN, HDIM), lambda i: (i, 0, 0)),
            pl.BlockSpec((1, 1, RUN), lambda i: (i, 0, 0)),
        ],
        out_specs=ANY,
        scratch_shapes=[
            pltpu.VMEM((own * RUN, HDIM), jnp.bfloat16),
            pltpu.VMEM((rows, HDIM), jnp.bfloat16),
            pltpu.VMEM((rows, HDIM), jnp.bfloat16),
            pltpu.VMEM((HDIM, rows if aligned else RUN), jnp.bfloat16),
            pltpu.VMEM((own * RUN, HDIM), jnp.bfloat16),
            pltpu.VMEM((rows, HDIM), jnp.float32),
            pltpu.VMEM((rows, HDIM), jnp.float32),
            pltpu.VMEM((2, 2, RUN, HDIM), jnp.bfloat16),
            pltpu.SemaphoreType.DMA((4,)),
            pltpu.SemaphoreType.DMA((2, 2)),
        ],
        compiler_params=pltpu.CompilerParams(
            dimension_semantics=("arbitrary",), vmem_limit_bytes=VMEM_MOST
        ),
        cost_estimate=busy(50),
        name="attend_backward",
    )(*tables, qkv, grads, exact, log_total)


def stream_tables(token_order, lengths, head_count, seq_size, tile, part):
    runs = token_order.shape[0] // RUN
    stream = (token_order.reshape(head_count, seq_size, RUN)[:, :, 0] // RUN).T.reshape(-1)
    places = jnp.arange(runs, dtype=jnp.int32)
    where = jnp.sum(jnp.where(stream[None, :] == places[:, None], places[None, :], 0), axis=1)
    ends = jnp.cumsum(lengths)
    starts = ends - lengths
    first = places * RUN
    last = first + RUN - 1

    def bound(position, of_seq, of_pad):
        inside = (position[:, None] >= starts[None, :]) & (position[:, None] < ends[None, :])
        found = jnp.sum(jnp.where(inside, of_seq[None, :], 0), axis=1)
        return jnp.where(position < ends[-1], found, of_pad)

    low = bound(first, starts, first) // tile
    high = (bound(last, ends, last + 1) + tile - 1) // tile
    return (
        where.astype(jnp.int32),
        low.astype(jnp.int32),
        high.astype(jnp.int32),
        ends.astype(jnp.int32),
        part.reshape(1).astype(jnp.int32),
    )


PAIR = 2
DEPTH = 6
LAG = 2


def grads_kernel(spec, left_ref, right_ref, *refs):
    chips, slots, left_strips, right_strips = spec
    lefts, refs = refs[: len(left_strips)], refs[len(left_strips) :]
    rights, refs = refs[: len(right_strips)], refs[len(right_strips) :]
    (
        out_ref,
        left_buf,
        right_buf,
        strip_buf,
        pair_out,
        pair_in,
        line_out,
        line_in,
        last_in,
        own_sum,
        load_sem,
        pair_send,
        pair_recv,
        line_send,
        line_recv,
        last_recv,
        pair_free,
        line_free,
    ) = refs
    me = lax.axis_index("seq")
    chip, core = me // PAIR, me % PAIR
    sibling = chip * PAIR + (1 - core)
    neighbours = ((chip + 1) * PAIR + core, (chip - 1) * PAIR + core)
    has_next = (chip < chips - 1, chip > 0)

    barrier = pltpu.get_barrier_semaphore()
    pl.semaphore_signal(barrier, inc=1, device_id={"seq": sibling}, device_id_type=MESH)
    for way in range(2):

        @pl.when(has_next[way])
        def _():
            pl.semaphore_signal(
                barrier, inc=1, device_id={"seq": neighbours[way]}, device_id_type=MESH
            )

    ends = (chip == 0).astype(jnp.int32) + (chip == chips - 1).astype(jnp.int32)
    pl.semaphore_wait(barrier, 3 - ends)

    def strip(source, index):
        return source.at[:, pl.ds(pl.multiple_of(index * BLOCK, BLOCK), BLOCK)]

    low = 0
    for source, count in zip(rights, right_strips):

        def load_right(index, carry, source=source, low=low):
            pltpu.make_async_copy(
                strip(source, index), right_buf.at[low + index], load_sem.at[2]
            ).start()
            return carry

        lax.fori_loop(0, count, load_right, 0)
        low += count
    rows = left_buf.shape[2]
    low = 0
    for source, count in zip(lefts, left_strips):

        def fetch(index, slot, source=source):
            return pltpu.make_async_copy(strip(source, index), strip_buf.at[slot], load_sem.at[slot])

        def turn_strip(index, carry, count=count, low=low, fetch=fetch):
            slot = index % 2

            @pl.when(index + 1 < count)
            def _():
                fetch(index + 1, 1 - slot).start()

            fetch(index, slot).wait()
            for part in range(rows // BLOCK):
                span = pl.ds(part * BLOCK, BLOCK)
                left_buf[low + index, :, span] = strip_buf[slot, span, :].T
            return carry

        fetch(0, 0).start()
        lax.fori_loop(0, count, turn_strip, 0)
        low += count
    low = 0
    for source, count in zip(rights, right_strips):

        def wait_right(index, carry, source=source, low=low):
            pltpu.make_async_copy(
                strip(source, index), right_buf.at[low + index], load_sem.at[2]
            ).wait()
            return carry

        lax.fori_loop(0, count, wait_right, 0)
        low += count

    def product(owner_chip, owner_core, k):
        slot = (owner_chip * PAIR + owner_core) * slots + k
        return nn(left_buf[left_ref[slot]], right_buf[right_ref[slot]])

    counts = ((chips - 1 - chip) * slots, chip * slots, slots)

    def owner(stream, step):
        if stream == 0:
            return chips - 1 - step // slots
        if stream == 1:
            return step // slots
        return chip

    def pair_copy(stream, step):
        slot = step % DEPTH
        return pltpu.make_async_remote_copy(
            src_ref=pair_out.at[stream, slot],
            dst_ref=pair_in.at[stream, slot],
            send_sem=pair_send.at[stream, slot],
            recv_sem=pair_recv.at[stream, slot],
            device_id={"seq": sibling},
            device_id_type=MESH,
        )

    def line_copy(stream, step):
        slot = step % DEPTH
        return pltpu.make_async_remote_copy(
            src_ref=line_out.at[stream, slot],
            dst_ref=line_in.at[stream, slot],
            send_sem=line_send.at[stream, slot],
            recv_sem=line_recv.at[stream, slot],
            device_id={"seq": neighbours[stream]},
            device_id_type=MESH,
        )

    def last_copy(stream, step):
        slot, k = step % DEPTH, step % slots
        return pltpu.make_async_remote_copy(
            src_ref=line_out.at[stream, slot],
            dst_ref=last_in.at[stream, k],
            send_sem=line_send.at[stream, slot],
            recv_sem=last_recv.at[stream, k],
            device_id={"seq": neighbours[stream]},
            device_id_type=MESH,
        )

    def give(stream, step):
        slot = step % DEPTH

        @pl.when(step >= DEPTH)
        def _():
            pair_copy(stream, step).wait_send()
            pl.semaphore_wait(pair_free.at[stream], 1)

        pair_out[stream, slot] = product(owner(stream, step), 1 - core, step % slots).astype(
            jnp.bfloat16
        )
        pair_copy(stream, step).start()

    def take(stream, step):
        slot = step % DEPTH
        total = product(owner(stream, step), core, step % slots)
        pair_copy(stream, step).wait_recv()
        total = total + pair_in[stream, slot].astype(jnp.float32)

        @pl.when(step + DEPTH < counts[stream])
        def _():
            pl.semaphore_signal(
                pair_free.at[stream], inc=1, device_id={"seq": sibling}, device_id_type=MESH
            )

        return total

    def forward(stream, step):
        slot = step % DEPTH
        target = chip + 1 if stream == 0 else chip - 1
        ends_there = owner(stream, step) == target
        has_source = has_next[1 - stream]
        total = take(stream, step)

        @pl.when(step >= DEPTH)
        def _():
            line_copy(stream, step).wait_send()

        @pl.when(has_source)
        def _():
            line_copy(stream, step).wait_recv()
            line_out[stream, slot] = (total + line_in[stream, slot].astype(jnp.float32)).astype(
                jnp.bfloat16
            )

            @pl.when(step + DEPTH < counts[stream])
            def _():
                pl.semaphore_signal(
                    line_free.at[stream],
                    inc=1,
                    device_id={"seq": neighbours[1 - stream]},
                    device_id_type=MESH,
                )

        @pl.when(jnp.logical_not(has_source))
        def _():
            line_out[stream, slot] = total.astype(jnp.bfloat16)

        @pl.when(ends_there)
        def _():
            last_copy(stream, step).start()

        @pl.when(jnp.logical_not(ends_there))
        def _():
            @pl.when(step >= DEPTH)
            def _():
                pl.semaphore_wait(line_free.at[stream], 1)

            line_copy(stream, step).start()

    def keep(step):
        own_sum[step] = take(2, step).astype(jnp.bfloat16)

    for stream in range(2):
        pl.when(counts[stream] > 0)(functools.partial(give, stream, 0))
    give(2, 0)

    delays = (chip * LAG, (chips - 1 - chip) * LAG, slots)

    def body(turn, carry):
        for stream in range(3):
            step = turn - delays[stream] + 1

            @pl.when((step > 0) & (step < counts[stream]))
            def _():
                give(stream, step)

        for stream in range(3):
            step = turn - delays[stream]

            @pl.when((step >= 0) & (step < counts[stream]))
            def _():
                if stream < 2:
                    forward(stream, step)
                else:
                    keep(step)

        return carry

    lax.fori_loop(0, (chips - 1) * slots + (chips - 1) * LAG, body, 0)

    def finish(k, carry):
        out_ref[k] = own_sum[k]
        for stream in range(2):

            @pl.when(has_next[1 - stream])
            def _():
                last_copy(stream, k).wait_recv()
                out_ref[k] = (
                    out_ref[k].astype(jnp.float32) + last_in[stream, k].astype(jnp.float32)
                ).astype(jnp.bfloat16)

        return carry

    lax.fori_loop(0, slots, finish, 0)
    for slot in range(DEPTH):
        for stream in range(2):

            @pl.when(counts[stream] > 0)
            def _():
                line_copy(stream, slot).wait_send()
                pair_copy(stream, slot).wait_send()

        pair_copy(2, slot).wait_send()


def owned_grads(left_index, right_index, lefts, rights, seq_size, collective_id):
    rows = lefts[0].shape[0]
    left_strips = tuple(array.shape[1] // BLOCK for array in lefts)
    right_strips = tuple(array.shape[1] // BLOCK for array in rights)
    chips = seq_size // PAIR
    slots = left_index.shape[0] // seq_size
    kind = jnp.bfloat16
    block = (BLOCK, BLOCK)
    return pl.pallas_call(
        functools.partial(grads_kernel, (chips, slots, left_strips, right_strips)),
        out_shape=jax.ShapeDtypeStruct((slots,) + block, kind),
        in_specs=[IN_SMEM] * 2 + [ANY] * (len(lefts) + len(rights)),
        out_specs=IN_VMEM,
        scratch_shapes=[
            pltpu.VMEM((sum(left_strips), BLOCK, rows), kind),
            pltpu.VMEM((sum(right_strips), rows, BLOCK), kind),
            pltpu.VMEM((2, rows, BLOCK), kind),
            pltpu.VMEM((3, DEPTH) + block, kind),
            pltpu.VMEM((3, DEPTH) + block, kind),
            pltpu.VMEM((2, DEPTH) + block, kind),
            pltpu.VMEM((2, DEPTH) + block, kind),
            pltpu.VMEM((2, slots) + block, kind),
            pltpu.VMEM((slots,) + block, kind),
            pltpu.SemaphoreType.DMA((3,)),
            pltpu.SemaphoreType.DMA((3, DEPTH)),
            pltpu.SemaphoreType.DMA((3, DEPTH)),
            pltpu.SemaphoreType.DMA((2, DEPTH)),
            pltpu.SemaphoreType.DMA((2, DEPTH)),
            pltpu.SemaphoreType.DMA((2, slots)),
            pltpu.SemaphoreType.REGULAR((3,)),
            pltpu.SemaphoreType.REGULAR((2,)),
        ],
        compiler_params=pltpu.CompilerParams(
            collective_id=collective_id, has_side_effects=True, vmem_limit_bytes=VMEM_MOST
        ),
        cost_estimate=busy(240),
        name="owned_grads",
    )(left_index, right_index, *lefts, *rights)


def block_operands(own_map, width, panel_width, ff_width):
    deep, narrow, wide = width // BLOCK, panel_width // BLOCK, ff_width // BLOCK
    left = jnp.zeros_like(own_map)
    right = jnp.zeros_like(own_map)
    first, left_low, right_low = 0, 0, 0
    panels = [(deep, narrow, 0, 0), (deep, narrow, 0, narrow), (deep, narrow, 0, 2 * narrow)]
    panels.append((narrow, deep, deep, 3 * narrow))
    panels.append((deep, wide, deep + narrow, 3 * narrow + deep))
    panels.append((wide, deep, 2 * deep + narrow, 3 * narrow + deep + wide))
    for high, broad, left_low, right_low in panels:
        inside = (own_map >= first) & (own_map < first + high * broad)
        within = own_map - first
        left = jnp.where(inside, left_low + within // broad, left)
        right = jnp.where(inside, right_low + within % broad, right)
        first += high * broad
    return left.astype(jnp.int32), right.astype(jnp.int32)


def group_peer(me, count, slot, way):
    far, near = slot // 2, slot % 2
    half = count // 2
    return (me // 2 + way * far + half) % half * 2 + (me % 2 + near) % 2


def group_barrier(me, count):
    barrier = pltpu.get_barrier_semaphore()
    for slot in range(1, count):
        pl.semaphore_signal(
            barrier, inc=1, device_id={"head": group_peer(me, count, slot, 1)}, device_id_type=MESH
        )
    pl.semaphore_wait(barrier, count - 1)


GELU_SCALE = 0.7978845608028654
GELU_CUBIC = 0.044715
WIDE = 512


def gelu(u):
    return 0.5 * u * (1.0 + jnp.tanh(GELU_SCALE * (u + GELU_CUBIC * (u * u * u))))


def gelu_slope(u):
    square = u * u
    bend = jnp.tanh(GELU_SCALE * (u + GELU_CUBIC * (square * u)))
    inner = GELU_SCALE * (1.0 + 3.0 * GELU_CUBIC * square)
    return 0.5 * (1.0 + bend) + 0.5 * u * (1.0 - bend * bend) * inner


def feed_kernel(is_forward, count, x_ref, up_ref, down_ref, side_ref, *refs):
    if is_forward:
        rows_ref, mid_ref, pre_ref, sum_ref = refs[:4]
        refs = refs[4:]
    else:
        rows_ref, mid_ref, sum_ref = refs[:3]
        refs = refs[3:]
    (
        land,
        up_buf,
        down_buf,
        mid_buf,
        pre_buf,
        part_buf,
        got,
        load_sem,
        send_sem,
        recv_sem,
        back_sem,
        got_sem,
        out_sem,
    ) = refs
    me = lax.axis_index("head")
    width, ff_width = up_buf.shape
    loads = [
        pltpu.make_async_copy(up_ref, up_buf, load_sem.at[0]),
        pltpu.make_async_copy(down_ref, down_buf, load_sem.at[1]),
    ]
    if not is_forward:
        loads.append(pltpu.make_async_copy(side_ref, pre_buf, load_sem.at[2]))
    for copy in loads:
        copy.start()
    group_barrier(me, count)

    def push(slot):
        return pltpu.make_async_remote_copy(
            src_ref=x_ref,
            dst_ref=land.at[slot],
            send_sem=send_sem.at[slot],
            recv_sem=recv_sem.at[slot],
            device_id={"head": group_peer(me, count, slot, 1)},
            device_id_type=MESH,
        )

    def give_back(slot):
        return pltpu.make_async_remote_copy(
            src_ref=part_buf.at[slot],
            dst_ref=got.at[slot],
            send_sem=back_sem.at[slot],
            recv_sem=got_sem.at[slot],
            device_id={"head": group_peer(me, count, slot, -1)},
            device_id_type=MESH,
        )

    def outs(slot):
        copies = [
            pltpu.make_async_copy(land.at[slot], rows_ref.at[slot], out_sem.at[0, slot]),
            pltpu.make_async_copy(mid_buf.at[slot], mid_ref.at[slot], out_sem.at[1, slot]),
        ]
        if is_forward:
            copies.append(
                pltpu.make_async_copy(pre_buf.at[slot], pre_ref.at[slot], out_sem.at[2, slot])
            )
        return copies

    for slot in range(1, count):
        push(slot).start()
    land[0] = x_ref[...]
    for copy in loads:
        copy.wait()

    def work(slot, carry):
        @pl.when(slot > 0)
        def _():
            push(slot).wait_recv()

        def hidden(index, inner):
            span = pl.ds(pl.multiple_of(index * WIDE, WIDE), WIDE)
            if is_forward:
                pre = nn(land[slot], up_buf[:, span]) + side_ref[:, span]
                pre_buf[slot, :, span] = pre.astype(jnp.bfloat16)
                mid_buf[slot, :, span] = gelu(pre).astype(jnp.bfloat16)
            else:
                grad = nt(land[slot], down_buf[span, :])
                slope = gelu_slope(pre_buf[slot, :, span].astype(jnp.float32))
                mid_buf[slot, :, span] = (grad * slope).astype(jnp.bfloat16)
            return inner

        def result(index, inner):
            span = pl.ds(pl.multiple_of(index * WIDE, WIDE), WIDE)
            if is_forward:
                part = nn(mid_buf[slot], down_buf[:, span])
            else:
                part = nt(mid_buf[slot], up_buf[span, :])

            @pl.when(slot == 0)
            def _():
                sum_ref[:, span] = part

            @pl.when(slot > 0)
            def _():
                part_buf[slot, :, span] = part.astype(jnp.bfloat16)

            return inner

        lax.fori_loop(0, ff_width // WIDE, hidden, 0)
        for copy in outs(slot):
            copy.start()
        lax.fori_loop(0, width // WIDE, result, 0)

        @pl.when(slot > 0)
        def _():
            give_back(slot).start()

        return carry

    lax.fori_loop(0, count, work, 0)

    def add(slot, carry):
        give_back(slot).wait_recv()
        sum_ref[...] += got[slot].astype(jnp.float32)
        return carry

    lax.fori_loop(1, count, add, 0)
    for slot in range(count):
        for copy in outs(slot):
            copy.wait()
        if slot > 0:
            push(slot).wait_send()
            give_back(slot).wait_send()


def feed(x_rows, up_panel, down_panel, side, is_forward, count, collective_id):
    if count == 4:
        return square_feed(x_rows, up_panel, down_panel, side, is_forward, collective_id)
    rows, width = x_rows.shape
    ff_width = up_panel.shape[1]
    kind = jnp.bfloat16
    by_width = jax.ShapeDtypeStruct((count, rows, width), kind)
    by_ff = jax.ShapeDtypeStruct((count, rows, ff_width), kind)
    total = jax.ShapeDtypeStruct((rows, width), jnp.float32)
    out_shape = (by_width, by_ff, by_ff, total) if is_forward else (by_width, by_ff, total)
    return pl.pallas_call(
        functools.partial(feed_kernel, is_forward, count),
        out_shape=out_shape,
        in_specs=[IN_VMEM, ANY, ANY, IN_VMEM if is_forward else ANY],
        out_specs=(ANY,) * (len(out_shape) - 1) + (IN_VMEM,),
        scratch_shapes=[
            pltpu.VMEM((count, rows, width), kind),
            pltpu.VMEM(up_panel.shape, kind),
            pltpu.VMEM(down_panel.shape, kind),
            pltpu.VMEM((count, rows, ff_width), kind),
            pltpu.VMEM((count, rows, ff_width), kind),
            pltpu.VMEM((count, rows, width), kind),
            pltpu.VMEM((count, rows, width), kind),
            pltpu.SemaphoreType.DMA((3,)),
            pltpu.SemaphoreType.DMA((count,)),
            pltpu.SemaphoreType.DMA((count,)),
            pltpu.SemaphoreType.DMA((count,)),
            pltpu.SemaphoreType.DMA((count,)),
            pltpu.SemaphoreType.DMA((3, count)),
        ],
        compiler_params=pltpu.CompilerParams(
            collective_id=collective_id, has_side_effects=True, vmem_limit_bytes=VMEM_MOST
        ),
        cost_estimate=busy(90),
        name="feed_forward" if is_forward else "feed_backward",
    )(x_rows, up_panel, down_panel, side)


def square_places(me):
    far, near = me // 2, me % 2
    return far * 2 + 1 - near, (1 - far) * 2 + near


def square_barrier(me):
    barrier = pltpu.get_barrier_semaphore()
    for peer in square_places(me):
        pl.semaphore_signal(barrier, inc=1, device_id={"head": peer}, device_id_type=MESH)
    pl.semaphore_wait(barrier, 2)


def square_copy(source, target, sems, index, peer):
    return pltpu.make_async_remote_copy(
        src_ref=source,
        dst_ref=target,
        send_sem=sems.at[0, index],
        recv_sem=sems.at[1, index],
        device_id={"head": peer},
        device_id_type=MESH,
    )


def square_gather(me, rows, x_ref, land, at_target, at_self, sems):
    one, two = square_places(me)
    low, high = pl.ds(0, rows // 2), pl.ds(rows // 2, rows // 2)
    return (
        square_copy(x_ref.at[low], land.at[at_target[0], low], sems, 0, one),
        square_copy(x_ref.at[high], land.at[at_target[0], high], sems, 1, one),
        square_copy(x_ref.at[high], land.at[at_target[1], high], sems, 2, two),
        square_copy(x_ref.at[low], land.at[at_target[1], low], sems, 3, two),
        square_copy(land.at[at_self[0], low], land.at[at_target[2], low], sems, 4, two),
        square_copy(land.at[at_self[1], high], land.at[at_target[3], high], sems, 5, one),
    )


def square_sums(me, rows, part_buf, relay, got, sems):
    one, two = square_places(me)
    low, high = pl.ds(0, rows // 2), pl.ds(rows // 2, rows // 2)
    return (
        square_copy(part_buf.at[3, low], relay.at[0], sems, 0, one),
        square_copy(part_buf.at[3, high], relay.at[1], sems, 1, two),
        square_copy(part_buf.at[1, low], got.at[0, low], sems, 2, one),
        square_copy(part_buf.at[1, high], got.at[0, high], sems, 3, one),
        square_copy(part_buf.at[2, high], got.at[1, high], sems, 4, two),
        square_copy(part_buf.at[2, low], got.at[1, low], sems, 5, two),
    )


def square_finish(rows, sums, part_buf, relay, got, sum_ref):
    low, high = pl.ds(0, rows // 2), pl.ds(rows // 2, rows // 2)

    def join(slot, span, index):
        total = part_buf[slot, span, :].astype(jnp.float32) + relay[index].astype(jnp.float32)
        part_buf[slot, span, :] = total.astype(jnp.bfloat16)

    sums[1].wait_recv()
    join(1, high, 1)
    sums[3].start()
    sums[0].wait_recv()
    join(2, low, 0)
    sums[5].start()
    for index in (2, 4, 3, 5):
        sums[index].wait_recv()
    sum_ref[...] += got[0].astype(jnp.float32) + got[1].astype(jnp.float32)
    for copy in sums:
        copy.wait_send()


def square_rows_kernel(x_ref, rows_ref, own_sem, sems):
    me = lax.axis_index("head")
    one, two = square_places(me)
    own = pltpu.make_async_copy(x_ref, rows_ref.at[me], own_sem)
    own.start()
    square_barrier(me)
    copies = square_gather(
        me, x_ref.shape[0], x_ref, rows_ref, (me, me, one, two), (one, two), sems
    )
    for index in (0, 2, 1, 3):
        copies[index].start()
    copies[0].wait_recv()
    copies[4].start()
    copies[2].wait_recv()
    copies[5].start()
    for index in (1, 3, 4, 5):
        copies[index].wait_recv()
    for copy in copies:
        copy.wait_send()
    own.wait()


def square_rows(x_rows, collective_id):
    return pl.pallas_call(
        square_rows_kernel,
        out_shape=jax.ShapeDtypeStruct((4,) + x_rows.shape, x_rows.dtype),
        in_specs=[IN_VMEM],
        out_specs=ANY,
        scratch_shapes=[pltpu.SemaphoreType.DMA, pltpu.SemaphoreType.DMA((2, 6))],
        compiler_params=pltpu.CompilerParams(
            collective_id=collective_id, has_side_effects=True, vmem_limit_bytes=8 * 1024 * 1024
        ),
        cost_estimate=busy(36),
        name="square_rows",
    )(x_rows)


def square_project_kernel(by_slot, x_ref, w_ref, sum_ref, part_buf, relay, got, sems):
    me = lax.axis_index("head")
    one, two = square_places(me)
    rows, width = sum_ref.shape
    square_barrier(me)
    sums = square_sums(me, rows, part_buf, relay, got, sems)

    def work(slot, origin):
        place = slot if by_slot else origin

        def result(index, carry):
            span = pl.ds(pl.multiple_of(index * WIDE, WIDE), WIDE)
            part = nn(x_ref[place], w_ref[:, span])
            if slot == 0:
                sum_ref[:, span] = part
            else:
                part_buf[slot, :, span] = part.astype(jnp.bfloat16)
            return carry

        lax.fori_loop(0, width // WIDE, result, 0)

    work(3, 3 - me)
    sums[0].start()
    sums[1].start()
    work(1, one)
    sums[2].start()
    work(2, two)
    sums[4].start()
    work(0, me)
    square_finish(rows, sums, part_buf, relay, got, sum_ref)


def square_project(x_rows, weights, by_slot, collective_id):
    _, rows, _ = x_rows.shape
    width = weights.shape[1]
    kind = jnp.bfloat16
    return pl.pallas_call(
        functools.partial(square_project_kernel, by_slot),
        out_shape=jax.ShapeDtypeStruct((rows, width), jnp.float32),
        in_specs=[IN_VMEM, IN_VMEM],
        out_specs=IN_VMEM,
        scratch_shapes=[
            pltpu.VMEM((4, rows, width), kind),
            pltpu.VMEM((2, rows // 2, width), kind),
            pltpu.VMEM((2, rows, width), kind),
            pltpu.SemaphoreType.DMA((2, 6)),
        ],
        compiler_params=pltpu.CompilerParams(
            collective_id=collective_id, has_side_effects=True, vmem_limit_bytes=40 * 1024 * 1024
        ),
        cost_estimate=busy(45),
        name="square_project",
    )(x_rows, weights)


def square_hidden_kernel(x_ref, up_ref, bias_ref, rows_ref, mid_ref, pre_ref, land, mid_buf, pre_buf, in_sems, out_sem):
    me = lax.axis_index("head")
    rows = x_ref.shape[0]
    ff_width = up_ref.shape[1]
    square_barrier(me)
    gathers = square_gather(me, rows, x_ref, land, (1, 2, 3, 3), (1, 2), in_sems)

    def outs(slot):
        return (
            pltpu.make_async_copy(land.at[slot], rows_ref.at[slot], out_sem.at[0, slot]),
            pltpu.make_async_copy(mid_buf.at[slot], mid_ref.at[slot], out_sem.at[1, slot]),
            pltpu.make_async_copy(pre_buf.at[slot], pre_ref.at[slot], out_sem.at[2, slot]),
        )

    def work(slot):
        def hidden(index, inner):
            span = pl.ds(pl.multiple_of(index * WIDE, WIDE), WIDE)
            pre = nn(land[slot], up_ref[:, span]) + bias_ref[:, span]
            pre_buf[slot, :, span] = pre.astype(jnp.bfloat16)
            mid_buf[slot, :, span] = gelu(pre).astype(jnp.bfloat16)
            return inner

        lax.fori_loop(0, ff_width // WIDE, hidden, 0)
        for copy in outs(slot):
            copy.start()

    for index in (0, 2, 1, 3):
        gathers[index].start()
    land[0] = x_ref[...]
    work(0)
    gathers[0].wait_recv()
    gathers[4].start()
    gathers[2].wait_recv()
    gathers[5].start()
    gathers[1].wait_recv()
    work(1)
    gathers[3].wait_recv()
    work(2)
    gathers[4].wait_recv()
    gathers[5].wait_recv()
    work(3)
    for copy in gathers:
        copy.wait_send()
    for slot in range(4):
        for copy in outs(slot):
            copy.wait()


def square_hidden(x_rows, up_panel, bias, collective_id):
    rows, width = x_rows.shape
    ff_width = up_panel.shape[1]
    kind = jnp.bfloat16
    by_width = jax.ShapeDtypeStruct((4, rows, width), kind)
    by_ff = jax.ShapeDtypeStruct((4, rows, ff_width), kind)
    return pl.pallas_call(
        square_hidden_kernel,
        out_shape=(by_width, by_ff, by_ff),
        in_specs=[IN_VMEM] * 3,
        out_specs=(ANY,) * 3,
        scratch_shapes=[
            pltpu.VMEM((4, rows, width), kind),
            pltpu.VMEM((4, rows, ff_width), kind),
            pltpu.VMEM((4, rows, ff_width), kind),
            pltpu.SemaphoreType.DMA((2, 6)),
            pltpu.SemaphoreType.DMA((3, 4)),
        ],
        compiler_params=pltpu.CompilerParams(
            collective_id=collective_id, has_side_effects=True, vmem_limit_bytes=40 * 1024 * 1024
        ),
        cost_estimate=busy(45),
        name="square_hidden",
    )(x_rows, up_panel, bias)


def square_feed_kernel(is_forward, x_ref, up_ref, down_ref, side_ref, *refs):
    if is_forward:
        rows_ref, mid_ref, pre_ref, sum_ref = refs[:4]
        refs = refs[4:]
    else:
        rows_ref, mid_ref, sum_ref = refs[:3]
        refs = refs[3:]
    land, up_buf, down_buf, mid_buf, pre_buf, part_buf, relay, got, load_sem, in_sems, sum_sems, out_sem = refs
    me = lax.axis_index("head")
    rows = x_ref.shape[0]
    width, ff_width = up_buf.shape
    loads = [
        pltpu.make_async_copy(up_ref, up_buf, load_sem.at[0]),
        pltpu.make_async_copy(down_ref, down_buf, load_sem.at[1]),
    ]
    if not is_forward:
        loads.append(pltpu.make_async_copy(side_ref, pre_buf, load_sem.at[2]))
    for copy in loads:
        copy.start()
    square_barrier(me)
    gathers = square_gather(me, rows, x_ref, land, (1, 2, 3, 3), (1, 2), in_sems)
    sums = square_sums(me, rows, part_buf, relay, got, sum_sems)

    def outs(slot):
        copies = [
            pltpu.make_async_copy(land.at[slot], rows_ref.at[slot], out_sem.at[0, slot]),
            pltpu.make_async_copy(mid_buf.at[slot], mid_ref.at[slot], out_sem.at[1, slot]),
        ]
        if is_forward:
            copies.append(
                pltpu.make_async_copy(pre_buf.at[slot], pre_ref.at[slot], out_sem.at[2, slot])
            )
        return copies

    def work(slot):
        def hidden(index, inner):
            span = pl.ds(pl.multiple_of(index * WIDE, WIDE), WIDE)
            if is_forward:
                pre = nn(land[slot], up_buf[:, span]) + side_ref[:, span]
                pre_buf[slot, :, span] = pre.astype(jnp.bfloat16)
                mid_buf[slot, :, span] = gelu(pre).astype(jnp.bfloat16)
            else:
                grad = nt(land[slot], down_buf[span, :])
                slope = gelu_slope(pre_buf[slot, :, span].astype(jnp.float32))
                mid_buf[slot, :, span] = (grad * slope).astype(jnp.bfloat16)
            return inner

        def result(index, inner):
            span = pl.ds(pl.multiple_of(index * WIDE, WIDE), WIDE)
            if is_forward:
                part = nn(mid_buf[slot], down_buf[:, span])
            else:
                part = nt(mid_buf[slot], up_buf[span, :])
            if slot == 0:
                sum_ref[:, span] = part
            else:
                part_buf[slot, :, span] = part.astype(jnp.bfloat16)
            return inner

        lax.fori_loop(0, ff_width // WIDE, hidden, 0)
        for copy in outs(slot):
            copy.start()
        lax.fori_loop(0, width // WIDE, result, 0)

    for index in (0, 2, 1, 3):
        gathers[index].start()
    land[0] = x_ref[...]
    for copy in loads:
        copy.wait()
    work(0)
    gathers[0].wait_recv()
    gathers[4].start()
    gathers[2].wait_recv()
    gathers[5].start()
    gathers[1].wait_recv()
    work(1)
    sums[2].start()
    gathers[3].wait_recv()
    work(2)
    sums[4].start()
    gathers[4].wait_recv()
    gathers[5].wait_recv()
    work(3)
    sums[0].start()
    sums[1].start()
    square_finish(rows, sums, part_buf, relay, got, sum_ref)
    for copy in gathers:
        copy.wait_send()
    for slot in range(4):
        for copy in outs(slot):
            copy.wait()


def square_feed(x_rows, up_panel, down_panel, side, is_forward, collective_id):
    rows, width = x_rows.shape
    ff_width = up_panel.shape[1]
    kind = jnp.bfloat16
    by_width = jax.ShapeDtypeStruct((4, rows, width), kind)
    by_ff = jax.ShapeDtypeStruct((4, rows, ff_width), kind)
    total = jax.ShapeDtypeStruct((rows, width), jnp.float32)
    out_shape = (by_width, by_ff, by_ff, total) if is_forward else (by_width, by_ff, total)
    return pl.pallas_call(
        functools.partial(square_feed_kernel, is_forward),
        out_shape=out_shape,
        in_specs=[IN_VMEM, ANY, ANY, IN_VMEM if is_forward else ANY],
        out_specs=(ANY,) * (len(out_shape) - 1) + (IN_VMEM,),
        scratch_shapes=[
            pltpu.VMEM((4, rows, width), kind),
            pltpu.VMEM(up_panel.shape, kind),
            pltpu.VMEM(down_panel.shape, kind),
            pltpu.VMEM((4, rows, ff_width), kind),
            pltpu.VMEM((4, rows, ff_width), kind),
            pltpu.VMEM((4, rows, width), kind),
            pltpu.VMEM((2, rows // 2, width), kind),
            pltpu.VMEM((2, rows, width), kind),
            pltpu.SemaphoreType.DMA((3,)),
            pltpu.SemaphoreType.DMA((2, 6)),
            pltpu.SemaphoreType.DMA((2, 6)),
            pltpu.SemaphoreType.DMA((3, 4)),
        ],
        compiler_params=pltpu.CompilerParams(
            collective_id=collective_id, has_side_effects=True, vmem_limit_bytes=VMEM_MOST
        ),
        cost_estimate=busy(80),
        name="square_forward" if is_forward else "square_backward",
    )(x_rows, up_panel, down_panel, side)


def start_kernel(count, chips, x_ref, w_ref, rows_ref, panel_ref, own_sem, row_sems, line_sems, pair_sems):
    me, place = lax.axis_index("head"), lax.axis_index("seq")
    chip, core = place // PAIR, place % PAIR
    sibling = chip * PAIR + (1 - core)
    neighbours = ((chip + 1) * PAIR + core, (chip - 1) * PAIR + core)
    has_next = (chip < chips - 1, chip > 0)
    owns = [
        pltpu.make_async_copy(x_ref, rows_ref.at[me], own_sem.at[0]),
        pltpu.make_async_copy(w_ref, panel_ref.at[place], own_sem.at[1]),
    ]
    for copy in owns:
        copy.start()

    barrier = pltpu.get_barrier_semaphore()
    for slot in range(1, count):
        pl.semaphore_signal(
            barrier, inc=1, device_id={"head": group_peer(me, count, slot, 1)}, device_id_type=MESH
        )
    pl.semaphore_signal(barrier, inc=1, device_id={"seq": sibling}, device_id_type=MESH)
    for way in range(2):

        @pl.when(has_next[way])
        def _():
            pl.semaphore_signal(
                barrier, inc=1, device_id={"seq": neighbours[way]}, device_id_type=MESH
            )

    ends = (chip == 0).astype(jnp.int32) + (chip == chips - 1).astype(jnp.int32)
    pl.semaphore_wait(barrier, count - 1 + 3 - ends)

    pushes = []
    for slot in range(1, count):
        pushes.append(
            pltpu.make_async_remote_copy(
                src_ref=x_ref,
                dst_ref=rows_ref.at[me],
                send_sem=row_sems.at[0, slot],
                recv_sem=row_sems.at[1, slot],
                device_id={"head": group_peer(me, count, slot, 1)},
                device_id_type=MESH,
            )
        )

    def relay(way, step):
        origin = chip - step if way == 0 else chip + step
        block = panel_ref.at[origin * PAIR + core]
        return pltpu.make_async_remote_copy(
            src_ref=w_ref if step == 0 else block,
            dst_ref=block,
            send_sem=line_sems.at[0, way, step],
            recv_sem=line_sems.at[1, way, step],
            device_id={"seq": neighbours[way]},
            device_id_type=MESH,
        )

    def share(way, step):
        origin = chip - 1 - step if way == 0 else chip + 1 + step
        if way == 2:
            origin = chip
        block = panel_ref.at[origin * PAIR + core]
        return pltpu.make_async_remote_copy(
            src_ref=w_ref if way == 2 else block,
            dst_ref=block,
            send_sem=pair_sems.at[0, way, step],
            recv_sem=pair_sems.at[1, way, step],
            device_id={"seq": sibling},
            device_id_type=MESH,
        )

    def sends(way, step):
        behind = chip >= step if way == 0 else chip + step <= chips - 1
        return has_next[way] & behind

    def receives(way, step):
        return chip - 1 - step >= 0 if way == 0 else chip + 1 + step <= chips - 1

    for way in range(2):
        pl.when(sends(way, 0))(relay(way, 0).start)
    for copy in pushes:
        copy.start()
    share(2, 0).start()
    for step in range(chips - 1):
        for way in range(2):

            @pl.when(receives(way, step))
            def _():
                relay(way, step).wait_recv()
                if step + 1 < chips - 1:
                    pl.when(sends(way, step + 1))(relay(way, step + 1).start)
                share(way, step).start()

    for copy in owns + pushes:
        copy.wait()
    share(2, 0).wait()
    for step in range(chips - 1):
        for way in range(2):
            pl.when(sends(way, step))(relay(way, step).wait_send)
            pl.when(receives(way, step))(share(way, step).wait)


def start_gathers(x_rows, w_rows, head_count, seq_size, collective_id):
    chips = seq_size // PAIR
    return pl.pallas_call(
        functools.partial(start_kernel, head_count, chips),
        out_shape=(
            jax.ShapeDtypeStruct((head_count,) + x_rows.shape, x_rows.dtype),
            jax.ShapeDtypeStruct((seq_size,) + w_rows.shape, w_rows.dtype),
        ),
        in_specs=[IN_VMEM, IN_VMEM],
        out_specs=(ANY, ANY),
        scratch_shapes=[
            pltpu.SemaphoreType.DMA((2,)),
            pltpu.SemaphoreType.DMA((2, head_count)),
            pltpu.SemaphoreType.DMA((2, 2, chips)),
            pltpu.SemaphoreType.DMA((2, 3, chips)),
        ],
        compiler_params=pltpu.CompilerParams(
            collective_id=collective_id, has_side_effects=True, vmem_limit_bytes=16 * 1024 * 1024
        ),
        cost_estimate=busy(60),
        name="start_gathers",
    )(x_rows, w_rows)


def normalize(z_rows, gain, shift):
    average = jnp.mean(z_rows, axis=-1, keepdims=True)
    centered = z_rows - average
    variance = jnp.mean(centered * centered, axis=-1, keepdims=True)
    recip = lax.rsqrt(variance + NORM_EPS)
    normed = centered * recip
    return (normed * gain + shift, normed, recip)


def normalize_back(grad_rows, normed, recip, gain):
    scaled = grad_rows * gain
    dz_rows = recip * (
        scaled
        - jnp.mean(scaled, axis=-1, keepdims=True)
        - normed * jnp.mean(scaled * normed, axis=-1, keepdims=True)
    )
    return (dz_rows, jnp.sum(grad_rows * normed, axis=0), jnp.sum(grad_rows, axis=0))


def group_rows(rows_low):
    return lax.all_gather(rows_low, "head", axis=0, tiled=True)


def group_sums(partial_value):
    return lax.psum_scatter(
        partial_value.astype(jnp.bfloat16), "head", scatter_dimension=0, tiled=True
    ).astype(jnp.float32)


def adam_step(param, grad, moment, second, step_float):
    moment_new = 0.9 * moment + 0.1 * grad
    second_new = 0.999 * second + 0.001 * grad * grad
    fix_one = 1.0 - jnp.power(jnp.float32(0.9), step_float)
    fix_two = 1.0 - jnp.power(jnp.float32(0.999), step_float)
    update = ADAM_RATE * (moment_new / fix_one) / (jnp.sqrt(second_new / fix_two) + 1e-08)
    return (param - update, moment_new, second_new)


def shards(
    hidden_in,
    cotangent,
    lengths,
    token_order,
    own_map,
    w_query,
    w_key,
    w_value,
    w_out,
    w_up,
    w_down,
    gains,
    biases,
    up_bias,
    vector_moment,
    vector_second,
    bias_moment,
    bias_second,
    step_count,
    stat_left,
    stat_right,
    root_left,
    root_right,
    master,
):
    head_count = lax.axis_size("head")
    seq_size = lax.axis_size("seq")
    head_index = lax.axis_index("head")
    group_index = lax.axis_index("seq")
    tok_count = hidden_in.shape[0]
    width = hidden_in.shape[1]
    panel_width = w_query.shape[1]
    ff_width = w_up.shape[1]
    seq_count = lengths.shape[0]
    heads = panel_width // HDIM
    parts = seq_size // heads
    runs = token_order.shape[0] // RUN
    aligned = seq_count == 2
    tile = 1024 if aligned else RUN
    setup = (parts, tile, seq_count, aligned, runs)
    tables = stream_tables(token_order, lengths, head_count, seq_size, tile, group_index % parts)
    own_block = head_index * seq_size + group_index
    order_here = lax.dynamic_slice_in_dim(token_order, own_block * tok_count, tok_count, 0)
    valid_here = order_here < tables[3][seq_count - 1]
    inputs_f32 = hidden_in.astype(jnp.float32)

    inputs_grp, qkv_panel = start_gathers(
        hidden_in, jnp.concatenate([w_query, w_key, w_value], axis=1), head_count, seq_size, 7
    )
    inputs_grp = inputs_grp.reshape(head_count * tok_count, width)
    qkv_panel = qkv_panel.reshape(width, 3 * panel_width)
    o_panel = lax.all_gather(w_out, "seq", axis=1, tiled=True)
    up_panel = lax.all_gather(w_up, "seq", axis=0, tiled=True)
    down_panel = lax.all_gather(w_down, "seq", axis=1, tiled=True)

    def own_columns(row):
        return lax.dynamic_slice_in_dim(row, head_index * panel_width, panel_width, 0)

    qkv_bias = jnp.concatenate(
        [own_columns(biases[0]), jnp.zeros((panel_width,), jnp.float32), own_columns(biases[1])]
    )
    qkv_grp = (
        jnp.dot(inputs_grp, qkv_panel, preferred_element_type=jnp.float32) + qkv_bias
    ).astype(jnp.bfloat16)
    qkv_head = spread(qkv_grp, 3, heads, parts, seq_size, 0)
    qkv_head = qkv_head.reshape(3, runs, RUN, HDIM)
    attended_part, attended_exact, log_total = attend_forward(qkv_head, tables, setup)
    rows_grp = head_count * tok_count
    attended_grp = collect(
        attended_part.reshape(1, seq_size, rows_grp, HDIM), heads, parts, 1
    )
    if head_count == 4:
        branch_out = square_project(
            attended_grp.reshape(head_count, tok_count, panel_width), o_panel, False, 8
        )
    else:
        branch_out = group_sums(
            jnp.dot(attended_grp, o_panel, preferred_element_type=jnp.float32)
        )
    z_one = inputs_f32 + branch_out + biases[2]
    h_one, normed_one, recip_one = normalize(z_one, gains[0], biases[3])
    h_low = h_one.astype(jnp.bfloat16)
    hidden_bias = up_bias.reshape(1, ff_width)
    if head_count == 4:
        h_grp, act, pre_act = square_hidden(h_low, up_panel, hidden_bias, 5)
        ff_out = square_project(act, down_panel, True, 10)
    else:
        h_grp, act, pre_act, ff_out = feed(
            h_low, up_panel, down_panel, hidden_bias, True, head_count, 5
        )
    z_two = h_one + ff_out + biases[4]
    layer_f32, normed_two, recip_two = normalize(z_two, gains[1], biases[5])
    layer_out = layer_f32.astype(jnp.bfloat16)
    grad_y = cotangent.astype(jnp.float32) * valid_here[:, None].astype(jnp.float32)
    dz_two, dgain_two, dshift_two = normalize_back(grad_y, normed_two, recip_two, gains[1])
    dbias_down = jnp.sum(dz_two, axis=0)
    dz_two_grp, dpre, dh_part = feed(
        dz_two.astype(jnp.bfloat16), up_panel, down_panel, pre_act, False, head_count, 6
    )
    h_grp, act, dz_two_grp, dpre = (
        array.reshape(rows_grp, array.shape[2]) for array in (h_grp, act, dz_two_grp, dpre)
    )
    up_bias_part = jnp.sum(dpre.astype(jnp.float32), axis=0)
    dh_one = dz_two + dh_part
    dz_one, dgain_one, dshift_one = normalize_back(dh_one, normed_one, recip_one, gains[0])
    dbias_out = jnp.sum(dz_one, axis=0)
    dz_one_low = dz_one.astype(jnp.bfloat16)
    if head_count == 4:
        dz_one_grp = square_rows(dz_one_low, 9).reshape(rows_grp, width)
    else:
        dz_one_grp = group_rows(dz_one_low)
    dattended = jnp.dot(dz_one_grp, o_panel.T, preferred_element_type=jnp.float32).astype(
        jnp.bfloat16
    )
    dattended_head = spread(dattended, 1, heads, parts, seq_size, 2).reshape(runs, RUN, HDIM)
    dqkv_part = attend_backward(
        qkv_head, dattended_head, attended_exact, log_total, tables, setup
    )
    dqkv_grp = collect(dqkv_part.reshape(3, seq_size, rows_grp, HDIM), heads, parts, 3)
    input_grad = dz_one + group_sums(
        jnp.dot(dqkv_grp, qkv_panel.T, preferred_element_type=jnp.float32)
    )
    bias_qkv = jnp.sum(dqkv_grp.astype(jnp.float32), axis=0)
    zero_width = jnp.zeros((width,), jnp.float32)
    dbias_query = lax.dynamic_update_slice_in_dim(
        zero_width, bias_qkv[:panel_width], head_index * panel_width, 0
    )
    dbias_value = lax.dynamic_update_slice_in_dim(
        zero_width, bias_qkv[2 * panel_width :], head_index * panel_width, 0
    )
    local_vectors = jnp.stack(
        (
            dbias_query,
            dbias_value,
            dbias_out,
            dshift_one,
            dbias_down,
            dshift_two,
            dgain_one,
            dgain_two,
        )
    )
    packed = jnp.concatenate([local_vectors.reshape(-1), up_bias_part])
    packed_all = lax.all_gather(packed, ("head", "seq"))
    vector_grad = jnp.sum(packed_all[:, : 8 * width], axis=0).reshape(8, width)
    up_bias_grad = jnp.sum(
        lax.dynamic_slice_in_dim(packed_all[:, 8 * width :], head_index * seq_size, seq_size, 0),
        axis=0,
    )
    left_index, right_index = block_operands(own_map[0], width, panel_width, ff_width)
    low_grads = owned_grads(
        left_index,
        right_index,
        (inputs_grp, attended_grp, h_grp, act),
        (dqkv_grp, dz_one_grp, dpre, dz_two_grp),
        seq_size,
        4,
    )
    block_grads = low_grads.astype(jnp.float32)
    stat_left_new = 0.5 * stat_left + 0.5 * jnp.einsum(
        "bij,bkj->bik", low_grads, low_grads, preferred_element_type=jnp.float32
    )
    stat_right_new = 0.5 * stat_right + 0.5 * jnp.einsum(
        "bji,bjk->bik", low_grads, low_grads, preferred_element_type=jnp.float32
    )
    left_mix = jnp.einsum(
        "bij,bjk->bik",
        root_left.astype(jnp.bfloat16),
        low_grads,
        preferred_element_type=jnp.float32,
    )
    direction = jnp.einsum(
        "bij,bjk->bik",
        left_mix.astype(jnp.bfloat16),
        root_right.astype(jnp.bfloat16),
        preferred_element_type=jnp.float32,
    )
    master_new = master - SHAMPOO_RATE * direction
    step_float = step_count[0].astype(jnp.float32)
    vector_params = jnp.concatenate([biases, gains], axis=0)
    vector_new, vector_moment_new, vector_second_new = adam_step(
        vector_params, vector_grad, vector_moment, vector_second, step_float
    )
    up_bias_new, bias_moment_new, bias_second_new = adam_step(
        up_bias, up_bias_grad, bias_moment, bias_second, step_float
    )
    return (
        layer_out,
        input_grad,
        block_grads,
        stat_left_new,
        stat_right_new,
        master_new,
        vector_new[0:6],
        vector_new[6:8],
        up_bias_new,
        vector_grad,
        vector_moment_new,
        vector_second_new,
        up_bias_grad,
        bias_moment_new,
        bias_second_new,
    )


def solution(mesh):
    rows = P(("head", "seq"), None)
    blocks = P(("head", "seq"), None, None)
    in_specs = (
        rows,
        rows,
        P(),
        P(),
        P("head", None),
        P("seq", "head"),
        P("seq", "head"),
        P("seq", "head"),
        P("head", "seq"),
        P("seq", "head"),
        P("head", "seq"),
        P(),
        P(),
        P("head"),
        P(),
        P(),
        P("head"),
        P("head"),
        P(),
        blocks,
        blocks,
        blocks,
        blocks,
        blocks,
    )
    out_specs = (
        rows,
        rows,
        blocks,
        blocks,
        blocks,
        blocks,
        P(),
        P(),
        P("head"),
        P(),
        P(),
        P(),
        P("head"),
        P("head"),
        P("head"),
    )
    return jax.shard_map(shards, mesh=mesh, in_specs=in_specs, out_specs=out_specs, check_vma=False)
```
